32 devices in a mesh: dp: 8 (over z, core), fsdp: 4 (over y, x).
Axes of the slice: x: 2, y: 2, z: 4, core: 2. Of those that a mesh axis runs over, the one named last changes fastest.
Arguments:
- tokens: bfloat16 [32, 512, 1024], P(('dp', 'fsdp')), may hold values from -6 to 6
- images: bfloat16 [64, 588, 1024], P(('dp', 'fsdp')), may hold values from -6 to 6
- segment_ids: int32 [32, 512], P(('dp', 'fsdp')), may hold values from 0 to 3, never falling along the last dimension, each value on 1 to 256 neighbouring positions
- image_map: int32 [32, 4], P(('dp', 'fsdp')), may hold values from 0 to 1
- out_grad: bfloat16 [32, 512, 1024], P(('dp', 'fsdp')), may hold values from -6 to 6
- norm_self: bfloat16 [1024], P(('dp', 'fsdp')), may hold values from 0.5 to 1.5
- attn_query: bfloat16 [1024, 1024], P(('dp', 'fsdp')), may hold values from -0.1875 to 0.1875
- attn_key: bfloat16 [1024, 1024], P(('dp', 'fsdp')), may hold values from -0.1875 to 0.1875
- attn_value: bfloat16 [1024, 1024], P(('dp', 'fsdp')), may hold values from -0.1875 to 0.1875
- attn_out: bfloat16 [1024, 1024], P(('dp', 'fsdp')), may hold values from -0.75 to 0.75
- norm_cross: bfloat16 [1024], P(('dp', 'fsdp')), may hold values from 0.5 to 1.5
- cross_query: bfloat16 [1024, 1024], P(('dp', 'fsdp')), may hold values from -0.1875 to 0.1875
- cross_key: bfloat16 [1024, 1024], P(('dp', 'fsdp')), may hold values from -0.1875 to 0.1875
- cross_value: bfloat16 [1024, 1024], P(('dp', 'fsdp')), may hold values from -0.1875 to 0.1875
- cross_out: bfloat16 [1024, 1024], P(('dp', 'fsdp')), may hold values from -0.75 to 0.75
- norm_ffn: bfloat16 [1024], P(('dp', 'fsdp')), may hold values from 0.5 to 1.5
- ffn_up: bfloat16 [1024, 4096], P(('dp', 'fsdp')), may hold values from -0.1875 to 0.1875
- ffn_down: bfloat16 [4096, 1024], P(('dp', 'fsdp')), may hold values from -0.09375 to 0.09375
Outputs:
- output: bfloat16 [32, 512, 1024], P(('dp', 'fsdp'))
- grad_tokens: bfloat16 [32, 512, 1024], P(('dp', 'fsdp'))
- grad_images: bfloat16 [64, 588, 1024], P(('dp', 'fsdp'))
- grad_norm_self: float32 [1024], P(('dp', 'fsdp'))
- grad_attn_query: float32 [1024, 1024], P(('dp', 'fsdp'))
- grad_attn_key: float32 [1024, 1024], P(('dp', 'fsdp'))
- grad_attn_value: float32 [1024, 1024], P(('dp', 'fsdp'))
- grad_attn_out: float32 [1024, 1024], P(('dp', 'fsdp'))
- grad_norm_cross: float32 [1024], P(('dp', 'fsdp'))
- grad_cross_query: float32 [1024, 1024], P(('dp', 'fsdp'))
- grad_cross_key: float32 [1024, 1024], P(('dp', 'fsdp'))
- grad_cross_value: float32 [1024, 1024], P(('dp', 'fsdp'))
- grad_cross_out: float32 [1024, 1024], P(('dp', 'fsdp'))
- grad_norm_ffn: float32 [1024], P(('dp', 'fsdp'))
- grad_ffn_up: float32 [1024, 4096], P(('dp', 'fsdp'))
- grad_ffn_down: float32 [4096, 1024], P(('dp', 'fsdp'))
The draws below stay inside these ranges and needn't reach their ends.
Inputs may be any that keep to these rules, and one draw needn't show every extreme that they name: `segment_ids`: Non-decreasing along each row; each of a row's 4 pages holds 1 to 256 tokens, one exactly 256. `image_map`: A local index among the row's own images.
All inputs are finite; a program needn't handle non-finite values.
Results may differ from the reference program's by a relative error of at most 0.02.
Values may be sent and summed in bfloat16 or wider, within the bound.
A program may use at most 256 MiB of HBM per device.

```python
import math
import jax
import jax.numpy as jnp
import numpy as np
from jax import lax

D = 1024
FF = 4096
HEADS = 16
IMG_TOK = 588
SEQ = 512
SEGS = 4
IMG_DEV = 2
ROWS = 32
IMAGES = 64


def place_ends(values, own_key, least, high):
    longest = values.shape.index(max(values.shape))
    spots = []
    for shift in (0, 1):
        where = [jax.random.randint(jax.random.fold_in(own_key, axis), (), 0, length) for axis, length in enumerate(values.shape)]
        where[longest] = (where[longest] + shift) % values.shape[longest]
        spots.append(tuple(where))
    return values.at[spots[0]].set(least).at[spots[1]].set(high)


def level_of(stream_key, extent, pieces, low, top_value):
    loudness, own = 1.0, jax.random.fold_in(stream_key, 6)
    for dim, parts in pieces:
        steps = jnp.exp(jax.random.uniform(jax.random.fold_in(own, dim), (parts,), jnp.float32, low / len(pieces), top_value / len(pieces)))
        loudness = loudness * jnp.repeat(steps, extent[dim] // parts).reshape([-1 if axis == dim else 1 for axis in range(len(extent))])
    return loudness


def split_up(count, total, reach, slope):
    loads = [(1 << 20) // math.isqrt(standing ** slope) + 1 for standing in range(2, count + 1)]
    rest, given = total - reach - (count - 1), [1] * (count - 1)
    while rest > 0:
        movable = [i for i in range(count - 1) if given[i] < reach]
        mass, budget = sum([loads[i] for i in movable]), rest
        for i in movable:
            extra = min(reach - given[i], max(1, budget * loads[i] // mass), rest)
            given[i] = given[i] + extra
            rest = rest - extra
    return np.array([reach] + given)


def ragged_sizes(key, number_of, total, limit, skew):
    if number_of == 2:
        one = jax.random.randint(key, (), max(1, total - limit), min(limit, total - 1) + 1)
        return jnp.stack([one, total - one])
    tallies = jnp.asarray(split_up(number_of, total, limit, skew), jnp.int32)
    pairs = (number_of - 1) // 2
    giver, receiver = tallies[1:1 + 2 * pairs:2], tallies[2:2 + 2 * pairs:2]
    room = jnp.minimum(giver - 1, limit - receiver)
    shifted = jax.random.randint(jax.random.fold_in(key, 1), (pairs,), 0, 1 << 20) % (room + 1)
    tallies = tallies.at[1:1 + 2 * pairs:2].set(giver - shifted).at[2:2 + 2 * pairs:2].set(receiver + shifted)
    return tallies[jax.random.permutation(jax.random.fold_in(key, 2), number_of)]


def noise(own_key, shape, scale, most, pieces=(), held_as=jnp.bfloat16):
    values = scale * jax.random.normal(own_key, shape, jnp.float32)
    if pieces:
        values = values * level_of(own_key, shape, pieces, -0.22, 0.18)
    return jnp.clip(values, -most, most).astype(held_as)


def setup_inputs(seed: int = 0) -> dict:
    seeds = jax.random.split(jax.random.key(seed), 19)
    tokens = noise(seeds[0], (ROWS, SEQ, D), 1.0, 6.0, ((0, 32),))
    images = noise(seeds[1], (IMAGES, IMG_TOK, D), 1.0, 6.0, ((0, 32),))
    segment_ids = jax.vmap(lambda own: jnp.searchsorted(jnp.cumsum(ragged_sizes(own, SEGS, SEQ, SEQ // 2, 0)), jnp.arange(SEQ), side="right"))(jax.random.split(seeds[2], ROWS)).reshape((ROWS, SEQ)).astype(jnp.int32)
    image_map = place_ends(jax.random.randint(seeds[3], (ROWS, SEGS), 0, IMG_DEV), jax.random.fold_in(seeds[3], 1), 0, IMG_DEV - 1).astype(jnp.int32)
    out_grad = noise(seeds[4], (ROWS, SEQ, D), 1.0, 6.0, ((0, 32),))
    norm_self = jnp.clip(1.0 + 0.1 * jax.random.normal(seeds[5], (D,), jnp.float32), 0.5, 1.5).astype(jnp.bfloat16)
    attn_query = noise(seeds[6], (D, D), D ** -0.5, 0.1875, ((0, 32),))
    attn_key = noise(seeds[7], (D, D), D ** -0.5, 0.1875, ((0, 32),))
    attn_value = noise(seeds[8], (D, D), D ** -0.5, 0.1875, ((0, 32),))
    attn_out = noise(seeds[9], (D, D), (D // 16) ** -0.5, 0.75, ((0, 32),))
    norm_cross = jnp.clip(1.0 + 0.1 * jax.random.normal(seeds[10], (D,), jnp.float32), 0.5, 1.5).astype(jnp.bfloat16)
    cross_query = noise(seeds[11], (D, D), D ** -0.5, 0.1875, ((0, 32),))
    cross_key = noise(seeds[12], (D, D), D ** -0.5, 0.1875, ((0, 32),))
    cross_value = noise(seeds[13], (D, D), D ** -0.5, 0.1875, ((0, 32),))
    cross_out = noise(seeds[14], (D, D), (D // 16) ** -0.5, 0.75, ((0, 32),))
    norm_ffn = jnp.clip(1.0 + 0.1 * jax.random.normal(seeds[15], (D,), jnp.float32), 0.5, 1.5).astype(jnp.bfloat16)
    ffn_up = noise(seeds[16], (D, FF), D ** -0.5, 0.1875, ((0, 32),))
    ffn_down = noise(seeds[17], (FF, D), FF ** -0.5, 0.09375, ((0, 32),))
    return {"tokens": tokens, "images": images, "segment_ids": segment_ids, "image_map": image_map, "out_grad": out_grad, "norm_self": norm_self, "attn_query": attn_query, "attn_key": attn_key, "attn_value": attn_value, "attn_out": attn_out, "norm_cross": norm_cross, "cross_query": cross_query, "cross_key": cross_key, "cross_value": cross_value, "cross_out": cross_out, "norm_ffn": norm_ffn, "ffn_up": ffn_up, "ffn_down": ffn_down}


@jax.custom_vjp
def low(v):
    return lax.optimization_barrier(v.astype(jnp.bfloat16)).astype(jnp.float32)

@jax.custom_vjp
def low_back(v):
    return v

def low_keep(v):
    return (low(v), None)

def low_pass(kept, grad):
    return (grad,)

def back_keep(v):
    return (v, None)

def back_low(kept, grad):
    return (low(grad),)
low.defvjp(low_keep, low_pass)
low_back.defvjp(back_keep, back_low)
masked_score = -1e+30
epsilon = 1e-05

def matmul(left, right):
    return jnp.dot(left, right, precision=lax.Precision.HIGHEST, preferred_element_type=jnp.float32)

def normed(values, gain_vector):
    centred = values - lax.optimization_barrier(jnp.mean(values, axis=-1, keepdims=True))
    variance = lax.optimization_barrier(jnp.mean(centred * centred, axis=-1, keepdims=True))
    return centred * lax.rsqrt(variance + epsilon) * gain_vector

def attention(query_rows, key_rows, value_rows, allowed):
    length = query_rows.shape[0]
    width = query_rows.shape[1]
    head_width = width // HEADS
    per_head_queries = query_rows.reshape(length, HEADS, head_width)
    per_head_keys = key_rows.reshape(key_rows.shape[0], HEADS, head_width)
    per_head_values = value_rows.reshape(value_rows.shape[0], HEADS, head_width)
    attention_logits = jnp.einsum('jvn,gvn->vjg', per_head_queries, per_head_keys, precision=lax.Precision.HIGHEST) * head_width ** (-0.5)
    attention_logits = low_back(jnp.where(allowed[None], attention_logits, masked_score))
    highest = lax.optimization_barrier(jnp.max(attention_logits, axis=-1, keepdims=True))
    exponent = jnp.exp(attention_logits - highest)
    attention_weights_matrix = low(exponent / lax.optimization_barrier(jnp.sum(exponent, axis=-1, keepdims=True)))
    combined_head_outputs = jnp.einsum('onx,xoy->noy', attention_weights_matrix, per_head_values, precision=lax.Precision.HIGHEST)
    return low_back(low(combined_head_outputs.reshape(length, width)))

def layer_row(inputs, row_images, segment_row, image_row, norm_self, attn_query, attn_key, attn_value, attn_out, norm_cross, cross_query, cross_key, cross_value, cross_out, norm_ffn, ffn_up, ffn_down):
    length = inputs.shape[0]
    position = jnp.arange(length).astype(jnp.int32)
    causal = (position[None, :] <= position[:, None]) & (segment_row[:, None] == segment_row[None, :])
    page_index = jnp.arange(SEGS).astype(jnp.int32)
    token_image = lax.optimization_barrier(jnp.sum(jnp.where(segment_row[:, None] == page_index[None, :], image_row[None, :], 0), axis=1))
    key_image = (jnp.arange(IMG_DEV * IMG_TOK) // IMG_TOK).astype(jnp.int32)
    cross_ok = token_image[:, None] == key_image[None, :]
    hidden_one = low(normed(inputs, norm_self))
    query_one = low_back(low(matmul(hidden_one, attn_query)))
    key_one = low_back(low(matmul(hidden_one, attn_key)))
    value_one = low_back(low(matmul(hidden_one, attn_value)))
    after_self = inputs + low_back(matmul(attention(query_one, key_one, value_one, causal), attn_out))
    hidden_two = low(normed(after_self, norm_cross))
    flat_images = row_images.reshape(IMG_DEV * IMG_TOK, row_images.shape[2])
    query_two = low_back(low(matmul(hidden_two, cross_query)))
    key_two = low_back(low(matmul(flat_images, cross_key)))
    value_two = low_back(low(matmul(flat_images, cross_value)))
    after_cross = after_self + low_back(matmul(attention(query_two, key_two, value_two, cross_ok), cross_out))
    hidden_three = low(normed(after_cross, norm_ffn))
    inner = low_back(matmul(hidden_three, ffn_up))
    activated = low(jax.nn.gelu(inner, approximate=False))
    return after_cross + low_back(matmul(activated, ffn_down))

def reference(tokens, images, segment_ids, image_map, out_grad, norm_self, attn_query, attn_key, attn_value, attn_out, norm_cross, cross_query, cross_key, cross_value, cross_out, norm_ffn, ffn_up, ffn_down):
    weights = tuple((item.astype(jnp.float32) for item in (norm_self, attn_query, attn_key, attn_value, attn_out, norm_cross, cross_query, cross_key, cross_value, cross_out, norm_ffn, ffn_up, ffn_down)))

    def one_row(totals, sample):
        inputs, row_images, segment_row, image_row, cotangent = sample

        def forward(values, pictures, *params):
            return layer_row(values, pictures, segment_row, image_row, *params)
        result, pullback = jax.vjp(forward, inputs.astype(jnp.float32), row_images.astype(jnp.float32), *weights)
        grads = pullback(cotangent.astype(jnp.float32))
        totals = tuple((running + fresh for running, fresh in zip(totals, grads[2:])))
        return (totals, (result.astype(jnp.bfloat16), grads[0].astype(jnp.bfloat16), grads[1].astype(jnp.bfloat16)))
    starting = tuple((jnp.zeros_like(item) for item in weights))
    grouped = images.reshape(ROWS, IMG_DEV, IMG_TOK, images.shape[2])
    totals, (output, grad_tokens, grad_grouped) = lax.scan(one_row, starting, (tokens, grouped, segment_ids, image_map, out_grad))
    grad_images = grad_grouped.reshape(IMAGES, IMG_TOK, images.shape[2])
    return (output, grad_tokens, grad_images, totals[0], totals[1], totals[2], totals[3], totals[4], totals[5], totals[6], totals[7], totals[8], totals[9], totals[10], totals[11], totals[12])
```

```python
import functools

import jax
import jax.numpy as jnp
from jax import lax
from jax.experimental import pallas as pl
from jax.experimental.pallas import tpu as pltpu
from jax.sharding import PartitionSpec as P

HEADS = 16
AXES = ("dp", "fsdp")
LOG2E = 1.4426950408889634
EPSILON = 1e-05
MASKED = -1e30
TILE = 128
PAGE_MAX = 256
VMEM = 62 * 1024 * 1024

bf16 = jnp.bfloat16
f32 = jnp.float32


def product(left, right):
    return jnp.dot(left, right, preferred_element_type=f32)


def product_t(left, right):
    return lax.dot_general(left, right, (((1,), (1,)), ((), ())), preferred_element_type=f32)


def product_rows(left, right):
    return lax.dot_general(left, right, (((0,), (0,)), ((), ())), preferred_element_type=f32)


def normed(values, gain):
    centred = values - jnp.mean(values, axis=-1, keepdims=True)
    variance = jnp.mean(centred * centred, axis=-1, keepdims=True)
    inverse = lax.rsqrt(variance + EPSILON)
    unit = centred * inverse
    return unit * gain, unit, inverse


def norm_back(unit, inverse, gain, gradient):
    scaled = gradient * gain
    mean_scaled = jnp.mean(scaled, axis=-1, keepdims=True)
    mean_along = jnp.mean(scaled * unit, axis=-1, keepdims=True)
    return inverse * (scaled - mean_scaled - unit * mean_along), jnp.sum(gradient * unit, axis=0)


def params(count):
    return pltpu.CompilerParams(
        dimension_semantics=("arbitrary",) * count, vmem_limit_bytes=VMEM
    )


def two_heads(block):
    lane = lax.broadcasted_iota(jnp.int32, block.shape, 1)
    zero = jnp.zeros_like(block)
    half = block.shape[1] // 2
    return jnp.concatenate(
        [jnp.where(lane < half, block, zero), jnp.where(lane >= half, block, zero)], axis=0
    )


def join_heads(both):
    rows = both.shape[1] // 2
    feature = lax.broadcasted_iota(jnp.int32, (both.shape[0], rows), 0)
    return jnp.where(feature < both.shape[0] // 2, both[:, :rows], both[:, rows:]).T


def twice(row):
    return jnp.concatenate([row, row], axis=1)


def key_range(tile):
    return max(0, tile * TILE - PAGE_MAX), (tile + 1) * TILE


def fill_bias(page_column, page_row, bias, tiles):
    for tile in range(tiles):
        low, high = key_range(tile)
        keys = low + lax.broadcasted_iota(jnp.int32, (high - low, TILE), 0)
        queries = tile * TILE + lax.broadcasted_iota(jnp.int32, (high - low, TILE), 1)
        same = page_column[low:high, :] == page_row[:, tile * TILE : (tile + 1) * TILE]
        bias[tile, : high - low, :] = jnp.where((keys <= queries) & same, 0.0, MASKED)


def self_forward_kernel(page_column, page_row, q, k, v, out, totals, bias):
    tiles = q.shape[0] // TILE
    scale = LOG2E * (q.shape[1] // 2) ** (-0.5)

    @pl.when(pl.program_id(0) == 0)
    def _():
        fill_bias(page_column, page_row, bias, tiles)

    for tile in range(tiles):
        low, high = key_range(tile)
        here = slice(tile * TILE, (tile + 1) * TILE)
        scores = product_t(k[low:high, :], two_heads(q[here, :])) * scale + twice(
            bias[tile, : high - low, :]
        )
        highest = jnp.max(scores, axis=0, keepdims=True)
        weights = jnp.exp2(scores - highest)
        total = jnp.sum(weights, axis=0, keepdims=True)
        mixed = product_rows(v[low:high, :], weights.astype(bf16)) * (1.0 / total)
        out[here, :] = join_heads(mixed).astype(bf16)
        level = highest + jnp.log2(total)
        totals[0, 0:1, here] = level[:, :TILE]
        totals[0, 1:2, here] = level[:, TILE:]


def self_forward(pages, qkv):
    rows, width = qkv.shape[0], qkv.shape[1] // 3
    pairs = width // 128
    return pl.pallas_call(
        self_forward_kernel,
        grid=(pairs,),
        in_specs=[
            pl.BlockSpec((rows, 1), lambda j: (0, 0)),
            pl.BlockSpec((1, rows), lambda j: (0, 0)),
            pl.BlockSpec((rows, 128), lambda j: (0, j)),
            pl.BlockSpec((rows, 128), lambda j: (0, pairs + j)),
            pl.BlockSpec((rows, 128), lambda j: (0, 2 * pairs + j)),
        ],
        out_specs=[
            pl.BlockSpec((rows, 128), lambda j: (0, j)),
            pl.BlockSpec((1, 2, rows), lambda j: (j, 0, 0)),
        ],
        out_shape=[
            jax.ShapeDtypeStruct((rows, width), bf16),
            jax.ShapeDtypeStruct((pairs, 2, rows), f32),
        ],
        scratch_shapes=[pltpu.VMEM((rows // TILE, PAGE_MAX + TILE, TILE), f32)],
        compiler_params=params(1),
        name="self_forward",
    )(pages[:, None], pages[None, :], qkv, qkv, qkv)


def self_backward_kernel(page_column, page_row, q, k, v, g, totals, out, bias, dk, dv):
    tiles = q.shape[0] // TILE
    half_scale = (q.shape[1] // 2) ** (-0.5)
    scale = LOG2E * half_scale

    @pl.when(pl.program_id(0) == 0)
    def _():
        fill_bias(page_column, page_row, bias, tiles)

    dk[...] = jnp.zeros_like(dk)
    dv[...] = jnp.zeros_like(dv)
    for tile in range(tiles):
        low, high = key_range(tile)
        here = slice(tile * TILE, (tile + 1) * TILE)
        queries, grads = two_heads(q[here, :]), two_heads(g[here, :])
        keys, values = k[low:high, :], v[low:high, :]
        level = jnp.concatenate([totals[0, 0:1, here], totals[0, 1:2, here]], axis=1)
        weights = jnp.exp2(
            product_t(keys, queries) * scale + twice(bias[tile, : high - low, :]) - level
        )
        along = weights * product_t(values, grads)
        change = (along - weights * jnp.sum(along, axis=0, keepdims=True)).astype(bf16)
        dv[low:high, :] += product(weights.astype(bf16), grads)
        dk[low:high, :] += product(change, queries)
        out[0, here, :] = (join_heads(product_rows(keys, change)) * half_scale).astype(bf16)
    out[1] = (dk[...] * half_scale).astype(bf16)
    out[2] = dv[...].astype(bf16)


def self_backward(pages, qkv, grads, totals):
    rows, width = qkv.shape[0], qkv.shape[1] // 3
    pairs = width // 128
    return pl.pallas_call(
        self_backward_kernel,
        grid=(pairs,),
        in_specs=[
            pl.BlockSpec((rows, 1), lambda j: (0, 0)),
            pl.BlockSpec((1, rows), lambda j: (0, 0)),
            pl.BlockSpec((rows, 128), lambda j: (0, j)),
            pl.BlockSpec((rows, 128), lambda j: (0, pairs + j)),
            pl.BlockSpec((rows, 128), lambda j: (0, 2 * pairs + j)),
            pl.BlockSpec((rows, 128), lambda j: (0, j)),
            pl.BlockSpec((1, 2, rows), lambda j: (j, 0, 0)),
        ],
        out_specs=pl.BlockSpec((3, rows, 128), lambda j: (0, 0, j)),
        out_shape=jax.ShapeDtypeStruct((3, rows, width), bf16),
        scratch_shapes=[
            pltpu.VMEM((rows // TILE, PAGE_MAX + TILE, TILE), f32),
            pltpu.VMEM((rows, 128), f32),
            pltpu.VMEM((rows, 128), f32),
        ],
        compiler_params=params(1),
        name="self_backward",
    )(pages[:, None], pages[None, :], qkv, qkv, qkv, grads, totals)


def cross_steps(count, tiles):
    first = (count + TILE - 1) // TILE
    skip = count // TILE
    return first, skip, first + tiles - skip


def cross_step(step, first, skip):
    image = jnp.where(step < first, 0, 1)
    tile = jnp.where(step < first, step, step - first + skip)
    return image, pl.multiple_of(tile * TILE, TILE)


def cross_forward_kernel(count_ref, q, k, v, out, totals):
    scale = LOG2E * (q.shape[1] // 2) ** (-0.5)
    count = count_ref[0]
    first, skip, steps = cross_steps(count, q.shape[0] // TILE)

    def one(step, carry):
        image, start = cross_step(step, first, skip)
        here = pl.ds(start, TILE)
        scores = product_t(k[image], two_heads(q[here, :])) * scale
        highest = jnp.max(scores, axis=0, keepdims=True)
        weights = jnp.exp2(scores - highest)
        total = jnp.sum(weights, axis=0, keepdims=True)
        mixed = product_rows(v[image], weights.astype(bf16)) * (1.0 / total)
        row = start + lax.broadcasted_iota(jnp.int32, (TILE, 128), 0)
        mine = (row >= count) == (image == 1)
        out[here, :] = jnp.where(mine, join_heads(mixed), out[here, :].astype(f32)).astype(bf16)
        level = highest + jnp.log2(total)
        lane = start + lax.broadcasted_iota(jnp.int32, (1, TILE), 1)
        mine = (lane >= count) == (image == 1)
        totals[0, 0:1, here] = jnp.where(mine, level[:, :TILE], totals[0, 0:1, here])
        totals[0, 1:2, here] = jnp.where(mine, level[:, TILE:], totals[0, 1:2, here])
        return carry

    lax.fori_loop(0, steps, one, 0)


def cross_forward(count, query, kv):
    rows, width = query.shape
    pairs = width // 128
    images, length = kv.shape[:2]
    return pl.pallas_call(
        cross_forward_kernel,
        grid_spec=pltpu.PrefetchScalarGridSpec(
            num_scalar_prefetch=1,
            grid=(pairs,),
            in_specs=[
                pl.BlockSpec((rows, 128), lambda j, c: (0, j)),
                pl.BlockSpec((images, length, 128), lambda j, c: (0, 0, j)),
                pl.BlockSpec((images, length, 128), lambda j, c: (0, 0, pairs + j)),
            ],
            out_specs=[
                pl.BlockSpec((rows, 128), lambda j, c: (0, j)),
                pl.BlockSpec((1, 2, rows), lambda j, c: (j, 0, 0)),
            ],
        ),
        out_shape=[
            jax.ShapeDtypeStruct((rows, width), bf16),
            jax.ShapeDtypeStruct((pairs, 2, rows), f32),
        ],
        compiler_params=params(1),
        name="cross_forward",
    )(count, query, kv, kv)


def cross_backward_kernel(count_ref, q, k, v, g, totals, dq_out, dkv_out, dq, dk, dv):
    half_scale = (q.shape[1] // 2) ** (-0.5)
    scale = LOG2E * half_scale
    count = count_ref[0]
    first, skip, steps = cross_steps(count, q.shape[0] // TILE)
    dq[...] = jnp.zeros_like(dq)
    dk[...] = jnp.zeros_like(dk)
    dv[...] = jnp.zeros_like(dv)

    def one(step, carry):
        image, start = cross_step(step, first, skip)
        here = pl.ds(start, TILE)
        queries, grads = two_heads(q[here, :]), two_heads(g[here, :])
        lane = start + lax.broadcasted_iota(jnp.int32, (1, TILE), 1)
        mine = (lane >= count) == (image == 1)
        level = jnp.concatenate(
            [
                jnp.where(mine, totals[0, 0:1, here], -MASKED),
                jnp.where(mine, totals[0, 1:2, here], -MASKED),
            ],
            axis=1,
        )
        weights = jnp.exp2(product_t(k[image], queries) * scale - level)
        along = weights * product_t(v[image], grads)
        change = (along - weights * jnp.sum(along, axis=0, keepdims=True)).astype(bf16)
        dv[image] += product(weights.astype(bf16), grads)
        dk[image] += product(change, queries)
        dq[here, :] += join_heads(product_rows(k[image], change))
        return carry

    lax.fori_loop(0, steps, one, 0)
    dq_out[...] = (dq[...] * half_scale).astype(bf16)
    dkv_out[0] = (dk[...] * half_scale).astype(bf16)
    dkv_out[1] = dv[...].astype(bf16)


def cross_backward(count, query, kv, grads, totals):
    rows, width = query.shape
    pairs = width // 128
    images, length = kv.shape[:2]
    return pl.pallas_call(
        cross_backward_kernel,
        grid_spec=pltpu.PrefetchScalarGridSpec(
            num_scalar_prefetch=1,
            grid=(pairs,),
            in_specs=[
                pl.BlockSpec((rows, 128), lambda j, c: (0, j)),
                pl.BlockSpec((images, length, 128), lambda j, c: (0, 0, j)),
                pl.BlockSpec((images, length, 128), lambda j, c: (0, 0, pairs + j)),
                pl.BlockSpec((rows, 128), lambda j, c: (0, j)),
                pl.BlockSpec((1, 2, rows), lambda j, c: (j, 0, 0)),
            ],
            out_specs=[
                pl.BlockSpec((rows, 128), lambda j, c: (0, j)),
                pl.BlockSpec((2, images, length, 128), lambda j, c: (0, 0, 0, j)),
            ],
            scratch_shapes=[
                pltpu.VMEM((rows, 128), f32),
                pltpu.VMEM((images, length, 128), f32),
                pltpu.VMEM((images, length, 128), f32),
            ],
        ),
        out_shape=[
            jax.ShapeDtypeStruct((rows, width), bf16),
            jax.ShapeDtypeStruct((2, images, length, width), bf16),
        ],
        compiler_params=params(1),
        name="cross_backward",
    )(count, query, kv, kv, grads, totals)


def put_blocks(me, devices, lanes, total, send, keep):
    depth = total.shape[0] // devices
    for block in range(devices):
        relative = block ^ me
        place = (relative // (2 * lanes)) * lanes + relative % lanes
        piece = total[block * depth : (block + 1) * depth, :].astype(bf16)
        other = (relative // lanes) % 2 == 1

        @pl.when(other)
        def _():
            send[place] = piece

        @pl.when(jnp.logical_not(other))
        def _():
            keep[place] = piece


def weight_grad_kernel(devices, lanes, me_ref, left, right, send, keep, flipped):
    @pl.when((pl.program_id(0) == 0) & (pl.program_id(1) == 0))
    def _():
        for part in range(left.shape[0]):
            flipped[part] = left[part].T

    total = product(flipped[0], right[0, 0])
    for part in range(1, left.shape[0]):
        total += product(flipped[part], right[0, part])
    put_blocks(me_ref[0], devices, lanes, total, send, keep)


def weight_grad(me, devices, lanes, left, right):
    parts, rows, depth = left.shape
    kinds, columns = right.shape[0], right.shape[3]
    wide = 512
    steps = columns // wide
    block = (devices // 2, depth // devices, wide)
    spec = pl.BlockSpec(block, lambda i, j, m: (0, 0, i * steps + j))
    shape = jax.ShapeDtypeStruct((devices // 2, depth // devices, kinds * columns), bf16)
    return pl.pallas_call(
        functools.partial(weight_grad_kernel, devices, lanes),
        grid_spec=pltpu.PrefetchScalarGridSpec(
            num_scalar_prefetch=1,
            grid=(kinds, steps),
            in_specs=[
                pl.BlockSpec((parts, rows, depth), lambda i, j, m: (0, 0, 0)),
                pl.BlockSpec((1, parts, rows, wide), lambda i, j, m: (i, 0, 0, j)),
            ],
            out_specs=[spec, spec],
            scratch_shapes=[pltpu.VMEM((parts, depth, rows), bf16)],
        ),
        out_shape=[shape, shape],
        compiler_params=params(2),
        name="weight_grad",
    )(me, left, right)


def feed_kernel(
    devices, lanes, me_ref, x_ref, g_ref, gain_ref, up, down,
    out, gx, ggain, up_send, up_keep, down_send, down_keep,
    unit, inverse, hidden, flipped, total, back,
):
    step = pl.program_id(0)
    me = me_ref[0]

    @pl.when(step == 0)
    def _():
        h, u, i = normed(x_ref[...], gain_ref[...])
        unit[...] = u
        inverse[...] = i
        hidden[...] = h.astype(bf16)
        flipped[...] = h.T.astype(bf16)
        total[...] = jnp.zeros_like(total)
        back[...] = jnp.zeros_like(back)

    g = g_ref[...]
    inner = product(hidden[...], up[...])
    share = 0.5 + 0.5 * lax.erf(inner * (0.5**0.5))
    slope = share + inner * (jnp.exp(-0.5 * inner * inner) * 0.3989422804014327)
    active = (inner * share).astype(bf16)
    total[...] += product(active, down[...])
    change = (product_t(g, down[...]) * slope).astype(bf16)
    back[...] += product_t(change, up[...])
    put_blocks(me, devices, lanes, product(flipped[...], change), up_send, up_keep)
    grad_down = product_rows(active, g)
    depth = grad_down.shape[0] // lanes
    low = me % lanes

    def put(target):
        for block in range(lanes):
            target[0, block ^ low] = grad_down[block * depth : (block + 1) * depth, :].astype(bf16)

    @pl.when(step % 2 == 1)
    def _():
        put(down_send)

    @pl.when(step % 2 == 0)
    def _():
        put(down_keep)

    @pl.when(step == pl.num_programs(0) - 1)
    def _():
        out[...] = (x_ref[...] + total[...]).astype(bf16)
        gx_norm, gain_grad = norm_back(unit[...], inverse[...], gain_ref[...], back[...])
        gx[...] = g_ref[...].astype(f32) + gx_norm
        ggain[...] = gain_grad[None, :]


def feed(me, devices, lanes, x, g, gain, up, down):
    rows, width = x.shape
    hidden = up.shape[1]
    groups = devices // lanes
    tile = hidden // groups

    def group(s, m):
        return s ^ (m[0] // lanes)

    def whole(shape):
        return pl.BlockSpec(shape, lambda s, m: (0,) * len(shape))

    up_block = pl.BlockSpec((devices // 2, width // devices, tile), lambda s, m: (0, 0, group(s, m)))
    down_block = pl.BlockSpec((1, lanes, tile // lanes, width), lambda s, m: (s // 2, 0, 0, 0))
    up_shape = jax.ShapeDtypeStruct((devices // 2, width // devices, hidden), bf16)
    down_shape = jax.ShapeDtypeStruct((groups // 2, lanes, tile // lanes, width), bf16)
    return pl.pallas_call(
        functools.partial(feed_kernel, devices, lanes),
        grid_spec=pltpu.PrefetchScalarGridSpec(
            num_scalar_prefetch=1,
            grid=(groups,),
            in_specs=[
                whole((rows, width)),
                whole((rows, width)),
                whole((1, width)),
                pl.BlockSpec((width, tile), lambda s, m: (0, group(s, m))),
                pl.BlockSpec((tile, width), lambda s, m: (group(s, m), 0)),
            ],
            out_specs=[
                whole((rows, width)), whole((rows, width)), whole((1, width)),
                up_block, up_block, down_block, down_block,
            ],
            scratch_shapes=[
                pltpu.VMEM((rows, width), f32),
                pltpu.VMEM((rows, 1), f32),
                pltpu.VMEM((rows, width), bf16),
                pltpu.VMEM((width, rows), bf16),
                pltpu.VMEM((rows, width), f32),
                pltpu.VMEM((rows, width), f32),
            ],
        ),
        out_shape=[
            jax.ShapeDtypeStruct((rows, width), bf16),
            jax.ShapeDtypeStruct((rows, width), f32),
            jax.ShapeDtypeStruct((1, width), f32),
            up_shape, up_shape, down_shape, down_shape,
        ],
        compiler_params=params(1),
        name="feed",
    )(me, x, g, gain, up, down)


def swap(values, devices, bit):
    return lax.ppermute(values, AXES, [(i, i ^ bit) for i in range(devices)])


def owner_sums(send, keep, devices, lanes, order):
    depth, columns = keep.shape[-2:]
    send = send.reshape(devices // 2, depth, columns)
    keep = keep.reshape(devices // 2, depth, columns)
    arrived = swap(send, devices, lanes)
    left = [b for b in range(devices.bit_length() - 1) if (1 << b) != lanes]
    for bit in order:
        at = left.index(bit)
        inner = 1 << at
        shape = (keep.shape[0] // (2 * inner), 2, inner, depth, columns)
        a, b = keep.reshape(shape), arrived.reshape(shape)
        out = (a[:, 1].astype(f32) + b[:, 1].astype(f32)).astype(bf16)
        keep = (a[:, 0].astype(f32) + b[:, 0].astype(f32)).astype(bf16)
        out = out.reshape(-1, depth, columns)
        keep = keep.reshape(-1, depth, columns)
        arrived = swap(out, devices, 1 << bit)
        left.remove(bit)
    return (keep.astype(f32) + arrived.astype(f32)).reshape(depth, columns)


def orders(devices, lanes):
    core = lanes.bit_length() - 1
    low = list(range(core))
    high = list(range(core + 1, devices.bit_length() - 1))
    return low + high, low[::-1] + high


def small_sums(values, devices, me):
    kinds, depth = values.shape
    blocks = values.reshape(kinds, devices, depth // devices).transpose(1, 0, 2)
    blocks = blocks[jnp.arange(devices) ^ me]
    size = devices
    while size > 1:
        size //= 2
        blocks = blocks[:size] + swap(blocks[size:], devices, size)
    return blocks[0]


def shards(devices, lanes, tokens, images, segment_ids, image_map, out_grad, norm_self, attn_query,
           attn_key, attn_value, attn_out, norm_cross, cross_query, cross_key, cross_value, cross_out,
           norm_ffn, ffn_up, ffn_down):
    me = lax.axis_index("dp") * lanes + lax.axis_index("fsdp")
    me_ref = me.astype(jnp.int32)[None]
    depth, width = attn_query.shape
    gains = jnp.stack([norm_self, norm_cross, norm_ffn], axis=1)
    gains = jnp.pad(gains, ((0, 0), (0, 128 - 3)))
    attention_set = jnp.concatenate(
        [attn_query, attn_key, attn_value, attn_out, cross_key, cross_value, cross_query, cross_out, gains],
        axis=1,
    )
    attention_set = lax.all_gather(attention_set, AXES, axis=0, tiled=True)
    ffn_up = lax.all_gather(ffn_up, AXES, axis=0, tiled=True)
    ffn_down = lax.all_gather(ffn_down, AXES, axis=0, tiled=True)
    w_qkv = attention_set[:, : 3 * width]
    w_out = attention_set[:, 3 * width : 4 * width]
    w_kv = attention_set[:, 4 * width : 6 * width]
    w_cross_query = attention_set[:, 6 * width : 7 * width]
    w_cross_out = attention_set[:, 7 * width : 8 * width]
    gains = attention_set[:, 8 * width : 8 * width + 3].T.astype(f32)

    pages = segment_ids[0]
    length = pages.shape[0]
    page_index = jnp.arange(image_map.shape[1])
    second = jnp.sum(jnp.where(pages[:, None] == page_index[None, :], image_map[0][None, :], 0), axis=1)
    place_now = jnp.arange(length)
    earlier = place_now[None, :] < place_now[:, None]
    ones_before = jnp.sum(jnp.where(earlier, second[None, :], 0), axis=1)
    count = length - jnp.sum(second)
    place = jnp.where(second == 1, count + ones_before, place_now - ones_before)
    moved = place_now[:, None] == place[None, :]
    order = moved.astype(bf16)
    count = count.astype(jnp.int32)[None]
    pages = jnp.sum(jnp.where(moved, pages[None, :], 0), axis=1)
    inputs = product(order, tokens[0])
    grad_out = product(order, out_grad[0]).astype(bf16)

    hidden_one, unit_one, inverse_one = normed(inputs, gains[0:1])
    hidden_one = hidden_one.astype(bf16)
    qkv = product(hidden_one, w_qkv).astype(bf16)
    mixed_one, log_one = self_forward(pages, qkv)
    after_self = inputs + product(mixed_one, w_out)
    hidden_two, unit_two, inverse_two = normed(after_self, gains[1:2])
    hidden_two = hidden_two.astype(bf16)
    query_two = product(hidden_two, w_cross_query).astype(bf16)
    kv = lax.dot_general(images, w_kv, (((2,), (0,)), ((), ())), preferred_element_type=f32).astype(bf16)
    mixed_two, log_two = cross_forward(count, query_two, kv)
    after_cross = after_self + product(mixed_two, w_cross_out)

    (output, grad_after_cross, grad_gain_ffn, up_send, up_keep, down_send, down_keep) = feed(
        me_ref, devices, lanes, after_cross, grad_out, gains[2:3], ffn_up, ffn_down
    )
    one_way, other_way = orders(devices, lanes)
    grad_up = owner_sums(up_send, up_keep, devices, lanes, one_way)
    grad_down = owner_sums(down_send, down_keep, devices, lanes, other_way)

    branch_two = grad_after_cross.astype(bf16)
    grad_cross_out = owner_sums(
        *weight_grad(me_ref, devices, lanes, mixed_two[None], branch_two[None, None]),
        devices, lanes, one_way,
    )
    grad_mixed_two = product_t(branch_two, w_cross_out).astype(bf16)
    grad_query_two, grad_kv = cross_backward(count, query_two, kv, grad_mixed_two, log_two)
    grad_cross_query = owner_sums(
        *weight_grad(me_ref, devices, lanes, hidden_two[None], grad_query_two[None, None]),
        devices, lanes, other_way,
    )
    grad_cross_kv_send, grad_cross_kv_keep = weight_grad(me_ref, devices, lanes, images, grad_kv)
    grad_cross_key = owner_sums(
        grad_cross_kv_send[..., :width], grad_cross_kv_keep[..., :width], devices, lanes, one_way
    )
    grad_cross_value = owner_sums(
        grad_cross_kv_send[..., width:], grad_cross_kv_keep[..., width:], devices, lanes, other_way
    )
    grad_hidden_two = product_t(grad_query_two, w_cross_query)
    part_self, grad_gain_cross = norm_back(unit_two, inverse_two, gains[1:2], grad_hidden_two)
    grad_after_self = grad_after_cross + part_self
    back = (((2,), (1,)), ((), ()))
    grad_images = lax.dot_general(grad_kv[0], w_kv[:, :width], back, preferred_element_type=f32)
    grad_images += lax.dot_general(grad_kv[1], w_kv[:, width:], back, preferred_element_type=f32)

    branch_one = grad_after_self.astype(bf16)
    grad_attn_out = owner_sums(
        *weight_grad(me_ref, devices, lanes, mixed_one[None], branch_one[None, None]),
        devices, lanes, one_way,
    )
    grad_mixed_one = product_t(branch_one, w_out).astype(bf16)
    grad_qkv = self_backward(pages, qkv, grad_mixed_one, log_one)
    qkv_send, qkv_keep = weight_grad(me_ref, devices, lanes, hidden_one[None], grad_qkv[:, None])
    cut = 3 * width // 2
    grad_attn = jnp.concatenate(
        [
            owner_sums(qkv_send[..., :cut], qkv_keep[..., :cut], devices, lanes, one_way),
            owner_sums(qkv_send[..., cut:], qkv_keep[..., cut:], devices, lanes, other_way),
        ],
        axis=1,
    )
    grad_hidden_one = (
        product_t(grad_qkv[0], w_qkv[:, :width])
        + product_t(grad_qkv[1], w_qkv[:, width : 2 * width])
        + product_t(grad_qkv[2], w_qkv[:, 2 * width :])
    )
    part_input, grad_gain_self = norm_back(unit_one, inverse_one, gains[0:1], grad_hidden_one)
    grad_inputs = (grad_after_self + part_input).astype(bf16)
    gain_sums = small_sums(
        jnp.stack([grad_gain_self, grad_gain_cross, grad_gain_ffn[0]]), devices, me
    )
    output = product_rows(order, output).astype(bf16)
    grad_inputs = product_rows(order, grad_inputs).astype(bf16)
    return (
        output[None],
        grad_inputs[None],
        grad_images.astype(bf16),
        gain_sums[0],
        grad_attn[:, :width],
        grad_attn[:, width : 2 * width],
        grad_attn[:, 2 * width :],
        grad_attn_out,
        gain_sums[1],
        grad_cross_query,
        grad_cross_key,
        grad_cross_value,
        grad_cross_out,
        gain_sums[2],
        grad_up,
        grad_down,
    )


def solution(mesh):
    rows = P(AXES)
    devices, lanes = mesh.shape["dp"] * mesh.shape["fsdp"], mesh.shape["fsdp"]
    return jax.shard_map(
        functools.partial(shards, devices, lanes),
        mesh=mesh,
        in_specs=(rows,) * 18,
        out_specs=(rows,) * 16,
        check_vma=False,
    )
```

```python
import functools

import jax
import jax.numpy as jnp
from jax import lax
from jax.experimental import pallas as pl
from jax.experimental.pallas import tpu as pltpu
from jax.sharding import PartitionSpec as P


AXES = ("dp", "fsdp")
LOG2E = 1.4426950408889634
EPSILON = 1e-05
MASKED = -1e30
TILE = 128
PAGE_MAX = 256
VMEM = 62 * 1024 * 1024

bf16 = jnp.bfloat16
f32 = jnp.float32


def product(left, right):
    return jnp.dot(left, right, preferred_element_type=f32)


def product_t(left, right):
    return lax.dot_general(left, right, (((1,), (1,)), ((), ())), preferred_element_type=f32)


def product_rows(left, right):
    return lax.dot_general(left, right, (((0,), (0,)), ((), ())), preferred_element_type=f32)


def normed(values, gain):
    centred = values - jnp.mean(values, axis=-1, keepdims=True)
    variance = jnp.mean(centred * centred, axis=-1, keepdims=True)
    inverse = lax.rsqrt(variance + EPSILON)
    unit = centred * inverse
    return unit * gain, unit, inverse


def norm_back(unit, inverse, gain, gradient):
    scaled = gradient * gain
    mean_scaled = jnp.mean(scaled, axis=-1, keepdims=True)
    mean_along = jnp.mean(scaled * unit, axis=-1, keepdims=True)
    return inverse * (scaled - mean_scaled - unit * mean_along), jnp.sum(gradient * unit, axis=0)


def params(count):
    return pltpu.CompilerParams(
        dimension_semantics=("arbitrary",) * count, vmem_limit_bytes=VMEM
    )


def cost(microseconds):
    return pl.CostEstimate(flops=int(microseconds * 1e9), bytes_accessed=0, transcendentals=0)


def two_heads(block):
    lane = lax.broadcasted_iota(jnp.int32, block.shape, 1)
    zero = jnp.zeros_like(block)
    half = block.shape[1] // 2
    return jnp.concatenate(
        [jnp.where(lane < half, block, zero), jnp.where(lane >= half, block, zero)], axis=0
    )


def join_heads(both):
    rows = both.shape[1] // 2
    feature = lax.broadcasted_iota(jnp.int32, (both.shape[0], rows), 0)
    return jnp.where(feature < both.shape[0] // 2, both[:, :rows], both[:, rows:]).T


def twice(row):
    return jnp.concatenate([row, row], axis=1)


def key_range(tile):
    return max(0, tile * TILE - PAGE_MAX), (tile + 1) * TILE


def fill_bias(page_column, page_row, bias, tiles):
    for tile in range(tiles):
        low, high = key_range(tile)
        keys = low + lax.broadcasted_iota(jnp.int32, (high - low, TILE), 0)
        queries = tile * TILE + lax.broadcasted_iota(jnp.int32, (high - low, TILE), 1)
        same = page_column[low:high, :] == page_row[:, tile * TILE : (tile + 1) * TILE]
        bias[tile, : high - low, :] = jnp.where((keys <= queries) & same, 0.0, MASKED)


def self_forward_kernel(page_column, page_row, q, k, v, out, totals, bias):
    tiles = q.shape[0] // TILE
    scale = LOG2E * (q.shape[1] // 2) ** (-0.5)

    @pl.when(pl.program_id(0) == 0)
    def _():
        fill_bias(page_column, page_row, bias, tiles)

    for tile in range(tiles):
        low, high = key_range(tile)
        here = slice(tile * TILE, (tile + 1) * TILE)
        scores = product_t(k[low:high, :], two_heads(q[here, :])) * scale + twice(
            bias[tile, : high - low, :]
        )
        highest = jnp.max(scores, axis=0, keepdims=True)
        weights = jnp.exp2(scores - highest)
        total = jnp.sum(weights, axis=0, keepdims=True)
        mixed = product_rows(v[low:high, :], weights.astype(bf16)) * (1.0 / total)
        out[here, :] = join_heads(mixed).astype(bf16)
        level = highest + jnp.log2(total)
        totals[0, 0:1, here] = level[:, :TILE]
        totals[0, 1:2, here] = level[:, TILE:]


def self_forward(pages, qkv):
    rows, width = qkv.shape[0], qkv.shape[1] // 3
    pairs = width // 128
    return pl.pallas_call(
        self_forward_kernel,
        grid=(pairs,),
        in_specs=[
            pl.BlockSpec((rows, 1), lambda j: (0, 0)),
            pl.BlockSpec((1, rows), lambda j: (0, 0)),
            pl.BlockSpec((rows, 128), lambda j: (0, j)),
            pl.BlockSpec((rows, 128), lambda j: (0, pairs + j)),
            pl.BlockSpec((rows, 128), lambda j: (0, 2 * pairs + j)),
        ],
        out_specs=[
            pl.BlockSpec((rows, 128), lambda j: (0, j)),
            pl.BlockSpec((1, 2, rows), lambda j: (j, 0, 0)),
        ],
        out_shape=[
            jax.ShapeDtypeStruct((rows, width), bf16),
            jax.ShapeDtypeStruct((pairs, 2, rows), f32),
        ],
        scratch_shapes=[pltpu.VMEM((rows // TILE, PAGE_MAX + TILE, TILE), f32)],
        compiler_params=params(1),
        name="self_forward",
        cost_estimate=cost(14),
    )(pages[:, None], pages[None, :], qkv, qkv, qkv)


def self_backward_kernel(page_column, page_row, q, k, v, g, totals, out, bias, dk, dv):
    tiles = q.shape[0] // TILE
    half_scale = (q.shape[1] // 2) ** (-0.5)
    scale = LOG2E * half_scale

    @pl.when(pl.program_id(0) == 0)
    def _():
        fill_bias(page_column, page_row, bias, tiles)

    dk[...] = jnp.zeros_like(dk)
    dv[...] = jnp.zeros_like(dv)
    for tile in range(tiles):
        low, high = key_range(tile)
        here = slice(tile * TILE, (tile + 1) * TILE)
        queries, grads = two_heads(q[here, :]), two_heads(g[here, :])
        keys, values = k[low:high, :], v[low:high, :]
        level = jnp.concatenate([totals[0, 0:1, here], totals[0, 1:2, here]], axis=1)
        weights = jnp.exp2(
            product_t(keys, queries) * scale + twice(bias[tile, : high - low, :]) - level
        )
        along = weights * product_t(values, grads)
        change = (along - weights * jnp.sum(along, axis=0, keepdims=True)).astype(bf16)
        dv[low:high, :] += product(weights.astype(bf16), grads)
        dk[low:high, :] += product(change, queries)
        out[0, here, :] = (join_heads(product_rows(keys, change)) * half_scale).astype(bf16)
    out[1] = (dk[...] * half_scale).astype(bf16)
    out[2] = dv[...].astype(bf16)


def self_backward(pages, qkv, grads, totals):
    rows, width = qkv.shape[0], qkv.shape[1] // 3
    pairs = width // 128
    return pl.pallas_call(
        self_backward_kernel,
        grid=(pairs,),
        in_specs=[
            pl.BlockSpec((rows, 1), lambda j: (0, 0)),
            pl.BlockSpec((1, rows), lambda j: (0, 0)),
            pl.BlockSpec((rows, 128), lambda j: (0, j)),
            pl.BlockSpec((rows, 128), lambda j: (0, pairs + j)),
            pl.BlockSpec((rows, 128), lambda j: (0, 2 * pairs + j)),
            pl.BlockSpec((rows, 128), lambda j: (0, j)),
            pl.BlockSpec((1, 2, rows), lambda j: (j, 0, 0)),
        ],
        out_specs=pl.BlockSpec((3, rows, 128), lambda j: (0, 0, j)),
        out_shape=jax.ShapeDtypeStruct((3, rows, width), bf16),
        scratch_shapes=[
            pltpu.VMEM((rows // TILE, PAGE_MAX + TILE, TILE), f32),
            pltpu.VMEM((rows, 128), f32),
            pltpu.VMEM((rows, 128), f32),
        ],
        compiler_params=params(1),
        name="self_backward",
        cost_estimate=cost(15),
    )(pages[:, None], pages[None, :], qkv, qkv, qkv, grads, totals)


def cross_steps(count, tiles):
    first = (count + TILE - 1) // TILE
    skip = count // TILE
    return first, skip, first + tiles - skip


def cross_step(step, first, skip):
    image = jnp.where(step < first, 0, 1)
    tile = jnp.where(step < first, step, step - first + skip)
    return image, pl.multiple_of(tile * TILE, TILE)


def cross_forward_kernel(count_ref, q, k, v, out, totals):
    scale = LOG2E * (q.shape[1] // 2) ** (-0.5)
    count = count_ref[0]
    first, skip, steps = cross_steps(count, q.shape[0] // TILE)

    def one(step, carry):
        image, start = cross_step(step, first, skip)
        here = pl.ds(start, TILE)
        scores = product_t(k[image], two_heads(q[here, :])) * scale
        highest = jnp.max(scores, axis=0, keepdims=True)
        weights = jnp.exp2(scores - highest)
        total = jnp.sum(weights, axis=0, keepdims=True)
        mixed = product_rows(v[image], weights.astype(bf16)) * (1.0 / total)
        row = start + lax.broadcasted_iota(jnp.int32, (TILE, 128), 0)
        mine = (row >= count) == (image == 1)
        out[here, :] = jnp.where(mine, join_heads(mixed), out[here, :].astype(f32)).astype(bf16)
        level = highest + jnp.log2(total)
        lane = start + lax.broadcasted_iota(jnp.int32, (1, TILE), 1)
        mine = (lane >= count) == (image == 1)
        totals[0, 0:1, here] = jnp.where(mine, level[:, :TILE], totals[0, 0:1, here])
        totals[0, 1:2, here] = jnp.where(mine, level[:, TILE:], totals[0, 1:2, here])
        return carry

    lax.fori_loop(0, steps, one, 0)


def cross_forward(count, query, kv):
    rows, width = query.shape
    pairs = width // 128
    images, length = kv.shape[:2]
    return pl.pallas_call(
        cross_forward_kernel,
        grid_spec=pltpu.PrefetchScalarGridSpec(
            num_scalar_prefetch=1,
            grid=(pairs,),
            in_specs=[
                pl.BlockSpec((rows, 128), lambda j, c: (0, j)),
                pl.BlockSpec((images, length, 128), lambda j, c: (0, 0, j)),
                pl.BlockSpec((images, length, 128), lambda j, c: (0, 0, pairs + j)),
            ],
            out_specs=[
                pl.BlockSpec((rows, 128), lambda j, c: (0, j)),
                pl.BlockSpec((1, 2, rows), lambda j, c: (j, 0, 0)),
            ],
        ),
        out_shape=[
            jax.ShapeDtypeStruct((rows, width), bf16),
            jax.ShapeDtypeStruct((pairs, 2, rows), f32),
        ],
        compiler_params=params(1),
        name="cross_forward",
        cost_estimate=cost(24),
    )(count, query, kv, kv)


def cross_backward_kernel(count_ref, q, k, v, g, totals, dq_out, dkv_out, dq, dk, dv):
    half_scale = (q.shape[1] // 2) ** (-0.5)
    scale = LOG2E * half_scale
    count = count_ref[0]
    first, skip, steps = cross_steps(count, q.shape[0] // TILE)
    dq[...] = jnp.zeros_like(dq)
    dk[...] = jnp.zeros_like(dk)
    dv[...] = jnp.zeros_like(dv)

    def one(step, carry):
        image, start = cross_step(step, first, skip)
        here = pl.ds(start, TILE)
        queries, grads = two_heads(q[here, :]), two_heads(g[here, :])
        lane = start + lax.broadcasted_iota(jnp.int32, (1, TILE), 1)
        mine = (lane >= count) == (image == 1)
        level = jnp.concatenate(
            [
                jnp.where(mine, totals[0, 0:1, here], -MASKED),
                jnp.where(mine, totals[0, 1:2, here], -MASKED),
            ],
            axis=1,
        )
        weights = jnp.exp2(product_t(k[image], queries) * scale - level)
        along = weights * product_t(v[image], grads)
        change = (along - weights * jnp.sum(along, axis=0, keepdims=True)).astype(bf16)
        dv[image] += product(weights.astype(bf16), grads)
        dk[image] += product(change, queries)
        dq[here, :] += join_heads(product_rows(k[image], change))
        return carry

    lax.fori_loop(0, steps, one, 0)
    dq_out[...] = (dq[...] * half_scale).astype(bf16)
    dkv_out[0] = (dk[...] * half_scale).astype(bf16)
    dkv_out[1] = dv[...].astype(bf16)


def cross_backward(count, query, kv, grads, totals):
    rows, width = query.shape
    pairs = width // 128
    images, length = kv.shape[:2]
    return pl.pallas_call(
        cross_backward_kernel,
        grid_spec=pltpu.PrefetchScalarGridSpec(
            num_scalar_prefetch=1,
            grid=(pairs,),
            in_specs=[
                pl.BlockSpec((rows, 128), lambda j, c: (0, j)),
                pl.BlockSpec((images, length, 128), lambda j, c: (0, 0, j)),
                pl.BlockSpec((images, length, 128), lambda j, c: (0, 0, pairs + j)),
                pl.BlockSpec((rows, 128), lambda j, c: (0, j)),
                pl.BlockSpec((1, 2, rows), lambda j, c: (j, 0, 0)),
            ],
            out_specs=[
                pl.BlockSpec((rows, 128), lambda j, c: (0, j)),
                pl.BlockSpec((2, images, length, 128), lambda j, c: (0, 0, 0, j)),
            ],
            scratch_shapes=[
                pltpu.VMEM((rows, 128), f32),
                pltpu.VMEM((images, length, 128), f32),
                pltpu.VMEM((images, length, 128), f32),
            ],
        ),
        out_shape=[
            jax.ShapeDtypeStruct((rows, width), bf16),
            jax.ShapeDtypeStruct((2, images, length, width), bf16),
        ],
        compiler_params=params(1),
        name="cross_backward",
        cost_estimate=cost(28),
    )(count, query, kv, kv, grads, totals)


def put_rows(me, devices, lanes, left, staged):
    flipped = left.astype(f32).T
    depth = flipped.shape[0] // devices
    for block in range(devices):
        relative = block ^ me
        other = (relative // lanes) % 2
        place = (relative // (2 * lanes)) * lanes + relative % lanes + (1 - other) * (devices // 2)
        start = pl.multiple_of(place * depth, depth)
        staged[pl.ds(start, depth), :] = flipped[block * depth : (block + 1) * depth, :]


def put_halves(total, send, keep):
    half = total.shape[0] // 2
    send[...] = total[:half, :].astype(bf16).reshape(send.shape)
    keep[...] = total[half:, :].astype(bf16).reshape(keep.shape)


def weight_grad_kernel(devices, lanes, me_ref, left, right, send, keep, staged, flipped):
    @pl.when((pl.program_id(0) == 0) & (pl.program_id(1) == 0))
    def _():
        for part in range(left.shape[0]):
            put_rows(me_ref[0], devices, lanes, left[part], staged)
            flipped[part] = staged[...].astype(bf16)

    total = product(flipped[0], right[0, 0])
    for part in range(1, left.shape[0]):
        total += product(flipped[part], right[0, part])
    put_halves(total, send, keep)


def weight_grad(me, devices, lanes, left, right):
    parts, rows, depth = left.shape
    kinds, columns = right.shape[0], right.shape[3]
    wide = 512
    steps = columns // wide
    block = (1, devices // 2, depth // devices, wide)
    spec = pl.BlockSpec(block, lambda i, j, m: (i, 0, 0, j))
    shape = jax.ShapeDtypeStruct((kinds, devices // 2, depth // devices, columns), bf16)
    return pl.pallas_call(
        functools.partial(weight_grad_kernel, devices, lanes),
        grid_spec=pltpu.PrefetchScalarGridSpec(
            num_scalar_prefetch=1,
            grid=(kinds, steps),
            in_specs=[
                pl.BlockSpec((parts, rows, depth), lambda i, j, m: (0, 0, 0)),
                pl.BlockSpec((1, parts, rows, wide), lambda i, j, m: (i, 0, 0, j)),
            ],
            out_specs=[spec, spec],
            scratch_shapes=[pltpu.VMEM((depth, rows), f32), pltpu.VMEM((parts, depth, rows), bf16)],
        ),
        out_shape=[shape, shape],
        compiler_params=params(2),
        name="weight_grad",
        cost_estimate=cost(3 * kinds * parts),
    )(me, left, right)


def norm_grad_kernel(d_ref, w_ref, unit, inverse, gain, g_ref, out, low, gain_out, total):
    step = pl.program_id(0)
    kinds, _, width = d_ref.shape
    part = product_t(d_ref[0], w_ref[:, :width])
    for kind in range(1, kinds):
        part += product_t(d_ref[kind], w_ref[:, kind * width : (kind + 1) * width])
    wide = part.shape[1]
    total[:, pl.ds(pl.multiple_of(step * wide, wide), wide)] = part

    @pl.when(step == pl.num_programs(0) - 1)
    def _():
        change, gain_grad = norm_back(unit[...], inverse[...], gain[...], total[...])
        result = g_ref[...] + change
        out[...] = result
        low[...] = result.astype(bf16)
        gain_out[...] = gain_grad[None, :]


def norm_grad(grads, weights, first, unit, inverse, gain, g):
    kinds, rows, width = grads.shape
    wide = 256

    def whole(shape):
        return pl.BlockSpec(shape, lambda j: (0,) * len(shape))

    return pl.pallas_call(
        norm_grad_kernel,
        grid=(width // wide,),
        in_specs=[
            whole((kinds, rows, width)),
            pl.BlockSpec((wide, kinds * width), lambda j: (j, first)),
            whole((rows, width)), whole((rows, 1)), whole((1, width)), whole((rows, width)),
        ],
        out_specs=[whole((rows, width)), whole((rows, width)), whole((1, width))],
        out_shape=[
            jax.ShapeDtypeStruct((rows, width), f32),
            jax.ShapeDtypeStruct((rows, width), bf16),
            jax.ShapeDtypeStruct((1, width), f32),
        ],
        scratch_shapes=[pltpu.VMEM((rows, width), f32)],
        compiler_params=params(1),
        name="norm_grad",
        cost_estimate=cost(4 * kinds),
    )(grads, weights, unit, inverse, gain, g)


def feed_kernel(
    devices, lanes, me_ref, x_ref, g_ref, gain_ref, up_ref, down_ref,
    out, gx, ggain, up_send, up_keep, down_send, down_keep,
    unit, inverse, hidden, staged, flipped, total, back,
):
    step = pl.program_id(0)
    me = me_ref[0]

    @pl.when(step == 0)
    def _():
        h, u, i = normed(x_ref[...], gain_ref[...])
        unit[...] = u
        inverse[...] = i
        hidden[...] = h.astype(bf16)
        put_rows(me, devices, lanes, h, staged)
        flipped[...] = staged[...].astype(bf16)
        total[...] = jnp.zeros_like(total)
        back[...] = jnp.zeros_like(back)

    g = g_ref[...]
    up = up_ref[...].reshape(-1, up_ref.shape[-1])
    down = down_ref[...].reshape(-1, down_ref.shape[-1])
    inner = product(hidden[...], up)
    share = 0.5 + 0.5 * lax.erf(inner * (0.5**0.5))
    slope = share + inner * (jnp.exp(-0.5 * inner * inner) * 0.3989422804014327)
    active = (inner * share).astype(bf16)
    total[...] += product(active, down)
    change = (product_t(g, down) * slope).astype(bf16)
    back[...] += product_t(change, up)
    put_halves(product(flipped[...], change), up_send, up_keep)
    grad_down = product_rows(active, g)
    depth = grad_down.shape[0] // lanes
    low = me % lanes

    def put(target):
        for block in range(lanes):
            target[0, block ^ low] = grad_down[block * depth : (block + 1) * depth, :].astype(bf16)

    @pl.when(step % 2 == 1)
    def _():
        put(down_send)

    @pl.when(step % 2 == 0)
    def _():
        put(down_keep)

    @pl.when(step == pl.num_programs(0) - 1)
    def _():
        out[...] = (x_ref[...] + total[...]).astype(bf16)
        gx_norm, gain_grad = norm_back(unit[...], inverse[...], gain_ref[...], back[...])
        gx[...] = g_ref[...].astype(f32) + gx_norm
        ggain[...] = gain_grad[None, :]


def feed(me, devices, lanes, x, g, gain, weights):
    rows, width = x.shape
    pieces, depth = weights.shape[2:4]
    hidden = pieces * width
    groups = devices // lanes
    tile = hidden // groups
    across = width // tile

    def group(s, m):
        return s ^ (m[0] // lanes)

    def whole(shape):
        return pl.BlockSpec(shape, lambda s, m: (0,) * len(shape))

    up_block = pl.BlockSpec((devices // 2, width // devices, tile), lambda s, m: (0, 0, group(s, m)))
    down_block = pl.BlockSpec((1, lanes, tile // lanes, width), lambda s, m: (s // 2, 0, 0, 0))
    up_shape = jax.ShapeDtypeStruct((devices // 2, width // devices, hidden), bf16)
    down_shape = jax.ShapeDtypeStruct((groups // 2, lanes, tile // lanes, width), bf16)
    return pl.pallas_call(
        functools.partial(feed_kernel, devices, lanes),
        grid_spec=pltpu.PrefetchScalarGridSpec(
            num_scalar_prefetch=1,
            grid=(groups,),
            in_specs=[
                whole((rows, width)),
                whole((rows, width)),
                whole((1, width)),
                pl.BlockSpec(
                    (devices, None, None, depth, tile),
                    lambda s, m: (0, 0, group(s, m) // across, 0, group(s, m) % across),
                ),
                pl.BlockSpec(
                    (lanes, None, pieces, depth, width), lambda s, m: (group(s, m), 1, 0, 0, 0)
                ),
            ],
            out_specs=[
                whole((rows, width)), whole((rows, width)), whole((1, width)),
                up_block, up_block, down_block, down_block,
            ],
            scratch_shapes=[
                pltpu.VMEM((rows, width), f32),
                pltpu.VMEM((rows, 1), f32),
                pltpu.VMEM((rows, width), bf16),
                pltpu.VMEM((width, rows), f32),
                pltpu.VMEM((width, rows), bf16),
                pltpu.VMEM((rows, width), f32),
                pltpu.VMEM((rows, width), f32),
            ],
        ),
        out_shape=[
            jax.ShapeDtypeStruct((rows, width), bf16),
            jax.ShapeDtypeStruct((rows, width), f32),
            jax.ShapeDtypeStruct((1, width), f32),
            up_shape, up_shape, down_shape, down_shape,
        ],
        compiler_params=params(1),
        name="feed",
        cost_estimate=cost(45),
    )(me, x, g, gain, weights, weights)


def gather_kernel(devices, lanes, tracks, x_ref, out, own_sem, send_sem, recv_sem):
    me = lax.axis_index("dp") * lanes + lax.axis_index("fsdp")
    count = devices // 2

    def device(bit):
        other = me ^ bit
        return (other // lanes, lax.rem(other, lanes))

    barrier = pltpu.get_barrier_semaphore()
    every = [1 << b for b in range(devices.bit_length() - 1)]
    for bit in every:
        pl.semaphore_signal(
            barrier, inc=1, device_id=device(bit), device_id_type=pl.DeviceIdType.MESH
        )
    pl.semaphore_wait(barrier, len(every))
    own = pltpu.make_async_copy(x_ref, out.at[me], own_sem)
    own.start()
    sends = []

    def block(track, number, to_core):
        low, high, bits = tracks[track]
        owner = me ^ sum(b for p, b in enumerate(bits) if (number >> p) & 1)
        return out.at[owner ^ lanes if to_core else owner, :, low:high]

    def arrived(track, number):
        to_core = number >= count
        here = block(track, number - count if to_core else number, to_core)
        pltpu.make_async_remote_copy(
            src_ref=here,
            dst_ref=here,
            send_sem=send_sem.at[0],
            recv_sem=recv_sem.at[track, number],
            device_id=device(lanes),
            device_id_type=pl.DeviceIdType.MESH,
        ).wait_recv()
        return here

    for number in sorted(range(count), key=lambda k: (bin(k).count("1"), k)):
        for track, (low, high, bits) in enumerate(tracks):
            there = block(track, number, False)
            here = arrived(track, number) if number else x_ref.at[:, low:high]
            for place, bit in enumerate(bits + (lanes,)):
                if number >> place == 0 or bit == lanes:
                    copy = pltpu.make_async_remote_copy(
                        src_ref=here,
                        dst_ref=there,
                        send_sem=send_sem.at[len(sends)],
                        recv_sem=recv_sem.at[track, number + (1 << place)],
                        device_id=device(bit),
                        device_id_type=pl.DeviceIdType.MESH,
                    )
                    copy.start()
                    sends.append(copy)
    for number in range(count, devices):
        for track in range(len(tracks)):
            arrived(track, number)
    for copy in sends:
        copy.wait_send()
    own.wait()


def gather(number, devices, lanes, values):
    depth, columns = values.shape
    middle = (columns // 256) * 128
    high = tuple(2 * lanes << b for b in range((devices // (2 * lanes)).bit_length() - 1))
    links = [high + tuple(1 << b for b in way) for way in orders(lanes)]
    tracks = ((0, middle, links[0]), (middle, columns, links[1]))
    return pl.pallas_call(
        functools.partial(gather_kernel, devices, lanes, tracks),
        in_specs=[pl.BlockSpec(memory_space=pltpu.VMEM)],
        out_specs=pl.BlockSpec(memory_space=pltpu.HBM),
        out_shape=jax.ShapeDtypeStruct((devices, depth, columns), values.dtype),
        scratch_shapes=[
            pltpu.SemaphoreType.DMA,
            pltpu.SemaphoreType.DMA((len(tracks) * (devices - 1),)),
            pltpu.SemaphoreType.DMA((len(tracks), devices)),
        ],
        compiler_params=pltpu.CompilerParams(collective_id=number, has_side_effects=True),
        name="gather",
        cost_estimate=cost(40),
    )(values).reshape(-1, columns)


def swap(values, devices, bit):
    return lax.ppermute(values, AXES, [(i, i ^ bit) for i in range(devices)])


def cross_core(halves, devices, lanes):
    send, keep = (half.reshape(-1, devices // 2, *half.shape[-2:]) for half in halves)
    arrived = swap(send, devices, lanes)
    return [(keep[kind], arrived[kind]) for kind in range(keep.shape[0])]


def halved(pairs, devices, left, bit):
    inner = 1 << left.index(bit)

    def total(pair, pick):
        keep, arrived = pair
        shape = (keep.shape[0] // (2 * inner), 2, inner, *keep.shape[1:])
        a, b = keep.reshape(shape)[:, pick], arrived.reshape(shape)[:, pick]
        return (a.astype(f32) + b.astype(f32)).astype(bf16).reshape(-1, *keep.shape[1:])

    out, keep = (jnp.concatenate([total(pair, pick) for pair in pairs], axis=-1) for pick in (1, 0))
    return keep, swap(out, devices, 1 << bit)


def owner_sums(pairs, devices, lanes, order, late=()):
    left = list(range(lanes.bit_length() - 1))
    for stage, bit in enumerate(order):
        pairs = [halved(pairs, devices, left, bit)]
        if stage == 0 and late:
            pairs.append(halved(late, devices, left, bit))
        left.remove(bit)
    ((keep, arrived),) = pairs
    result = keep[0].astype(f32) + arrived[0].astype(f32)
    for high in range(1, devices // (2 * lanes)):
        out = (keep[high].astype(f32) + arrived[high].astype(f32)).astype(bf16)
        result += swap(out, devices, high * 2 * lanes).astype(f32)
    return result


def after(values, first):
    return lax.optimization_barrier((values, first))[0]


def orders(lanes):
    low = list(range(lanes.bit_length() - 1))
    return low, low[::-1]


def gain_halves(values, devices, lanes, me):
    kinds, depth = values.shape
    blocks = jnp.pad(values.T, ((0, 0), (0, 128 - kinds))).astype(bf16)
    blocks = blocks.reshape(devices, depth // devices, 128)[jnp.arange(devices) ^ me]
    blocks = blocks.reshape(-1, 2, lanes, depth // devices, 128)
    return blocks[:, 1], blocks[:, 0]


def shards(devices, lanes, tokens, images, segment_ids, image_map, out_grad, norm_self, attn_query,
           attn_key, attn_value, attn_out, norm_cross, cross_query, cross_key, cross_value, cross_out,
           norm_ffn, ffn_up, ffn_down):
    me = lax.axis_index("dp") * lanes + lax.axis_index("fsdp")
    me_ref = me.astype(jnp.int32)[None]
    depth, width = attn_query.shape
    gains = jnp.stack([norm_self, norm_cross, norm_ffn], axis=1)
    gains = jnp.pad(gains, ((0, 0), (0, 128 - 3)))
    first_set = jnp.concatenate([attn_query, attn_key, attn_value, cross_key, cross_value, gains], axis=1)
    second_set = jnp.concatenate([attn_out, cross_query, cross_out], axis=1)
    pieces = ffn_up.shape[1] // width
    feed_set = jnp.stack(
        [ffn_up.reshape(depth, pieces, width).transpose(1, 0, 2), ffn_down.reshape(pieces, depth, width)]
    )
    first_set = gather(0, devices, lanes, first_set)
    feed_set = lax.all_gather(after(feed_set, first_set), AXES, axis=0)
    w_qkv = first_set[:, : 3 * width]
    w_kv = first_set[:, 3 * width : 5 * width]
    gains = first_set[:, 5 * width : 5 * width + 3].T.astype(f32)

    pages = segment_ids[0]
    length = pages.shape[0]
    page_index = jnp.arange(image_map.shape[1])
    second = jnp.sum(jnp.where(pages[:, None] == page_index[None, :], image_map[0][None, :], 0), axis=1)
    place_now = jnp.arange(length)
    earlier = place_now[None, :] < place_now[:, None]
    ones_before = jnp.sum(jnp.where(earlier, second[None, :], 0), axis=1)
    count = length - jnp.sum(second)
    place = jnp.where(second == 1, count + ones_before, place_now - ones_before)
    moved = place_now[:, None] == place[None, :]
    order = moved.astype(bf16)
    count = count.astype(jnp.int32)[None]
    pages = jnp.sum(jnp.where(moved, pages[None, :], 0), axis=1)
    inputs = product(order, tokens[0])
    grad_out = product(order, out_grad[0]).astype(bf16)

    hidden_one, unit_one, inverse_one = normed(inputs, gains[0:1])
    hidden_one = hidden_one.astype(bf16)
    qkv = product(hidden_one, w_qkv).astype(bf16)
    mixed_one, log_one = self_forward(pages, qkv)
    kv = lax.dot_general(images, w_kv, (((2,), (0,)), ((), ())), preferred_element_type=f32).astype(bf16)
    second_set = gather(1, devices, lanes, after(second_set, (mixed_one, kv)))
    w_out = second_set[:, :width]
    w_cross_query = second_set[:, width : 2 * width]
    w_cross_out = second_set[:, 2 * width :]
    after_self = inputs + product(mixed_one, w_out)
    hidden_two, unit_two, inverse_two = normed(after_self, gains[1:2])
    hidden_two = hidden_two.astype(bf16)
    query_two = product(hidden_two, w_cross_query).astype(bf16)
    mixed_two, log_two = cross_forward(count, query_two, kv)
    after_cross = after_self + product(mixed_two, w_cross_out)

    (output, grad_after_cross, grad_gain_ffn, up_send, up_keep, down_send, down_keep) = feed(
        me_ref, devices, lanes, after_cross, grad_out, gains[2:3], feed_set
    )
    one_way, other_way = orders(lanes)

    def sums(way, *pairs, late=()):
        return owner_sums(sum(pairs, []), devices, lanes, way, late)

    def halves_of(left, right):
        return weight_grad(me_ref, devices, lanes, left, right)

    def paired(halves):
        return cross_core(halves, devices, lanes)

    grad_up = sums(one_way, paired((up_send, up_keep)))
    grad_down = sums(other_way, paired((down_send, down_keep)))

    branch_two = grad_after_cross.astype(bf16)
    grad_mixed_two = product_t(branch_two, w_cross_out).astype(bf16)
    halves = halves_of(mixed_two[None], branch_two[None, None])
    pair_out_two = paired(halves)
    grad_mixed_two = after(grad_mixed_two, halves[0])
    grad_query_two, grad_kv = cross_backward(count, query_two, kv, grad_mixed_two, log_two)
    halves = halves_of(images, grad_kv)
    pair_kv = paired(halves)
    halves = halves_of(hidden_two[None], after(grad_query_two, halves[0])[None, None])
    pair_query_two = paired(halves)
    grad_c = sums(one_way, pair_out_two, pair_query_two)
    grad_d = sums(other_way, pair_kv)
    grad_after_self, branch_one, grad_gain_cross = norm_grad(
        after(grad_query_two, halves[0])[None], second_set, 1, unit_two, inverse_two, gains[1:2], grad_after_cross
    )
    grad_mixed_one = product_t(branch_one, w_out).astype(bf16)
    grad_qkv = self_backward(pages, qkv, grad_mixed_one, log_one)
    halves = halves_of(mixed_one[None], after(branch_one, grad_qkv)[None, None])
    pair_out_one = paired(halves)
    halves = halves_of(hidden_one[None], after(grad_qkv, halves[0])[:, None])
    pair_qkv = paired(halves)
    _, grad_inputs, grad_gain_self = norm_grad(
        after(grad_qkv, halves[0]), first_set, 0, unit_one, inverse_one, gains[0:1], grad_after_self
    )
    gain_grads = jnp.concatenate([grad_gain_self, grad_gain_cross, grad_gain_ffn])
    pair_gains = paired(gain_halves(gain_grads, devices, lanes, me))
    grad_a = sums(one_way, pair_out_one, pair_qkv[:1])
    grad_b = sums(other_way, pair_qkv[1:], late=pair_gains)
    gain_sums = grad_b[:, 2 * width :]

    grad_kv = after(grad_kv, grad_inputs)
    back = (((2,), (1,)), ((), ()))
    grad_images = lax.dot_general(grad_kv[0], w_kv[:, :width], back, preferred_element_type=f32)
    grad_images += lax.dot_general(grad_kv[1], w_kv[:, width:], back, preferred_element_type=f32)
    output = product_rows(order, output).astype(bf16)
    grad_inputs = product_rows(order, grad_inputs).astype(bf16)
    return (
        output[None],
        grad_inputs[None],
        grad_images.astype(bf16),
        gain_sums[:, 0],
        grad_a[:, width:],
        grad_b[:, :width],
        grad_b[:, width : 2 * width],
        grad_a[:, :width],
        gain_sums[:, 1],
        grad_c[:, width:],
        grad_d[:, :width],
        grad_d[:, width:],
        grad_c[:, :width],
        gain_sums[:, 2],
        grad_up,
        grad_down,
    )


def solution(mesh):
    rows = P(AXES)
    devices, lanes = mesh.shape["dp"] * mesh.shape["fsdp"], mesh.shape["fsdp"]
    return jax.shard_map(
        functools.partial(shards, devices, lanes),
        mesh=mesh,
        in_specs=(rows,) * 18,
        out_specs=(rows,) * 16,
        check_vma=False,
    )
```

```python
import functools

import jax
import jax.numpy as jnp
from jax import lax
from jax.experimental import pallas as pl
from jax.experimental.pallas import tpu as pltpu
from jax.sharding import PartitionSpec as P


AXES = ("dp", "fsdp")
LOG2E = 1.4426950408889634
EPSILON = 1e-05
MASKED = -1e30
TILE = 128
PAGE_MAX = 256
VMEM = 62 * 1024 * 1024

bf16 = jnp.bfloat16
f32 = jnp.float32


def product(left, right):
    return jnp.dot(left, right, preferred_element_type=f32)


def product_t(left, right):
    return lax.dot_general(left, right, (((1,), (1,)), ((), ())), preferred_element_type=f32)


def product_rows(left, right):
    return lax.dot_general(left, right, (((0,), (0,)), ((), ())), preferred_element_type=f32)


def normed(values, gain):
    centred = values - jnp.mean(values, axis=-1, keepdims=True)
    variance = jnp.mean(centred * centred, axis=-1, keepdims=True)
    inverse = lax.rsqrt(variance + EPSILON)
    unit = centred * inverse
    return unit * gain, unit, inverse


def norm_back(unit, inverse, gain, gradient):
    scaled = gradient * gain
    mean_scaled = jnp.mean(scaled, axis=-1, keepdims=True)
    mean_along = jnp.mean(scaled * unit, axis=-1, keepdims=True)
    return inverse * (scaled - mean_scaled - unit * mean_along), jnp.sum(gradient * unit, axis=0)


def params(count):
    return pltpu.CompilerParams(
        dimension_semantics=("arbitrary",) * count, vmem_limit_bytes=VMEM
    )


def cost(microseconds):
    return pl.CostEstimate(flops=int(microseconds * 1e9), bytes_accessed=0, transcendentals=0)


def two_heads(block):
    lane = lax.broadcasted_iota(jnp.int32, block.shape, 1)
    zero = jnp.zeros_like(block)
    half = block.shape[1] // 2
    return jnp.concatenate(
        [jnp.where(lane < half, block, zero), jnp.where(lane >= half, block, zero)], axis=0
    )


def join_heads(both):
    rows = both.shape[1] // 2
    feature = lax.broadcasted_iota(jnp.int32, (both.shape[0], rows), 0)
    return jnp.where(feature < both.shape[0] // 2, both[:, :rows], both[:, rows:]).T


def twice(row):
    return jnp.concatenate([row, row], axis=1)


def key_range(tile):
    return max(0, tile * TILE - PAGE_MAX), (tile + 1) * TILE


def fill_bias(page_column, page_row, bias, tiles):
    for tile in range(tiles):
        low, high = key_range(tile)
        keys = low + lax.broadcasted_iota(jnp.int32, (high - low, TILE), 0)
        queries = tile * TILE + lax.broadcasted_iota(jnp.int32, (high - low, TILE), 1)
        same = page_column[low:high, :] == page_row[:, tile * TILE : (tile + 1) * TILE]
        bias[tile, : high - low, :] = jnp.where((keys <= queries) & same, 0.0, MASKED)


def self_forward_kernel(page_column, page_row, q, k, v, out, totals, bias):
    tiles = q.shape[0] // TILE
    scale = LOG2E * (q.shape[1] // 2) ** (-0.5)

    @pl.when(pl.program_id(0) == 0)
    def _():
        fill_bias(page_column, page_row, bias, tiles)

    for tile in range(tiles):
        low, high = key_range(tile)
        here = slice(tile * TILE, (tile + 1) * TILE)
        scores = product_t(k[low:high, :], two_heads(q[here, :])) * scale + twice(
            bias[tile, : high - low, :]
        )
        highest = jnp.max(scores, axis=0, keepdims=True)
        weights = jnp.exp2(scores - highest)
        total = jnp.sum(weights, axis=0, keepdims=True)
        mixed = product_rows(v[low:high, :], weights.astype(bf16)) * (1.0 / total)
        out[here, :] = join_heads(mixed).astype(bf16)
        level = highest + jnp.log2(total)
        totals[0, 0:1, here] = level[:, :TILE]
        totals[0, 1:2, here] = level[:, TILE:]


def self_forward(pages, qkv):
    rows, width = qkv.shape[0], qkv.shape[1] // 3
    pairs = width // 128
    return pl.pallas_call(
        self_forward_kernel,
        grid=(pairs,),
        in_specs=[
            pl.BlockSpec((rows, 1), lambda j: (0, 0)),
            pl.BlockSpec((1, rows), lambda j: (0, 0)),
            pl.BlockSpec((rows, 128), lambda j: (0, j)),
            pl.BlockSpec((rows, 128), lambda j: (0, pairs + j)),
            pl.BlockSpec((rows, 128), lambda j: (0, 2 * pairs + j)),
        ],
        out_specs=[
            pl.BlockSpec((rows, 128), lambda j: (0, j)),
            pl.BlockSpec((1, 2, rows), lambda j: (j, 0, 0)),
        ],
        out_shape=[
            jax.ShapeDtypeStruct((rows, width), bf16),
            jax.ShapeDtypeStruct((pairs, 2, rows), f32),
        ],
        scratch_shapes=[pltpu.VMEM((rows // TILE, PAGE_MAX + TILE, TILE), f32)],
        compiler_params=params(1),
        name="self_forward",
        cost_estimate=cost(14),
    )(pages[:, None], pages[None, :], qkv, qkv, qkv)


def self_backward_kernel(page_column, page_row, q, k, v, g, totals, out, bias, dk, dv):
    tiles = q.shape[0] // TILE
    half_scale = (q.shape[1] // 2) ** (-0.5)
    scale = LOG2E * half_scale

    @pl.when(pl.program_id(0) == 0)
    def _():
        fill_bias(page_column, page_row, bias, tiles)

    dk[...] = jnp.zeros_like(dk)
    dv[...] = jnp.zeros_like(dv)
    for tile in range(tiles):
        low, high = key_range(tile)
        here = slice(tile * TILE, (tile + 1) * TILE)
        queries, grads = two_heads(q[here, :]), two_heads(g[here, :])
        keys, values = k[low:high, :], v[low:high, :]
        level = jnp.concatenate([totals[0, 0:1, here], totals[0, 1:2, here]], axis=1)
        weights = jnp.exp2(
            product_t(keys, queries) * scale + twice(bias[tile, : high - low, :]) - level
        )
        along = weights * product_t(values, grads)
        change = (along - weights * jnp.sum(along, axis=0, keepdims=True)).astype(bf16)
        dv[low:high, :] += product(weights.astype(bf16), grads)
        dk[low:high, :] += product(change, queries)
        out[0, here, :] = (join_heads(product_rows(keys, change)) * half_scale).astype(bf16)
    out[1] = (dk[...] * half_scale).astype(bf16)
    out[2] = dv[...].astype(bf16)


def self_backward(pages, qkv, grads, totals):
    rows, width = qkv.shape[0], qkv.shape[1] // 3
    pairs = width // 128
    return pl.pallas_call(
        self_backward_kernel,
        grid=(pairs,),
        in_specs=[
            pl.BlockSpec((rows, 1), lambda j: (0, 0)),
            pl.BlockSpec((1, rows), lambda j: (0, 0)),
            pl.BlockSpec((rows, 128), lambda j: (0, j)),
            pl.BlockSpec((rows, 128), lambda j: (0, pairs + j)),
            pl.BlockSpec((rows, 128), lambda j: (0, 2 * pairs + j)),
            pl.BlockSpec((rows, 128), lambda j: (0, j)),
            pl.BlockSpec((1, 2, rows), lambda j: (j, 0, 0)),
        ],
        out_specs=pl.BlockSpec((3, rows, 128), lambda j: (0, 0, j)),
        out_shape=jax.ShapeDtypeStruct((3, rows, width), bf16),
        scratch_shapes=[
            pltpu.VMEM((rows // TILE, PAGE_MAX + TILE, TILE), f32),
            pltpu.VMEM((rows, 128), f32),
            pltpu.VMEM((rows, 128), f32),
        ],
        compiler_params=params(1),
        name="self_backward",
        cost_estimate=cost(15),
    )(pages[:, None], pages[None, :], qkv, qkv, qkv, grads, totals)


def cross_steps(count, tiles):
    first = (count + TILE - 1) // TILE
    skip = count // TILE
    return first, skip, first + tiles - skip


def cross_step(step, first, skip):
    image = jnp.where(step < first, 0, 1)
    tile = jnp.where(step < first, step, step - first + skip)
    return image, pl.multiple_of(tile * TILE, TILE)


def cross_forward_kernel(count_ref, q, k, v, out, totals):
    scale = LOG2E * (q.shape[1] // 2) ** (-0.5)
    count = count_ref[0]
    first, skip, steps = cross_steps(count, q.shape[0] // TILE)

    def one(step, carry):
        image, start = cross_step(step, first, skip)
        here = pl.ds(start, TILE)
        scores = product_t(k[image], two_heads(q[here, :])) * scale
        highest = jnp.max(scores, axis=0, keepdims=True)
        weights = jnp.exp2(scores - highest)
        total = jnp.sum(weights, axis=0, keepdims=True)
        mixed = product_rows(v[image], weights.astype(bf16)) * (1.0 / total)
        row = start + lax.broadcasted_iota(jnp.int32, (TILE, 128), 0)
        mine = (row >= count) == (image == 1)
        out[here, :] = jnp.where(mine, join_heads(mixed), out[here, :].astype(f32)).astype(bf16)
        level = highest + jnp.log2(total)
        lane = start + lax.broadcasted_iota(jnp.int32, (1, TILE), 1)
        mine = (lane >= count) == (image == 1)
        totals[0, 0:1, here] = jnp.where(mine, level[:, :TILE], totals[0, 0:1, here])
        totals[0, 1:2, here] = jnp.where(mine, level[:, TILE:], totals[0, 1:2, here])
        return carry

    lax.fori_loop(0, steps, one, 0)


def cross_forward(count, query, kv):
    rows, width = query.shape
    pairs = width // 128
    images, length = kv.shape[:2]
    return pl.pallas_call(
        cross_forward_kernel,
        grid_spec=pltpu.PrefetchScalarGridSpec(
            num_scalar_prefetch=1,
            grid=(pairs,),
            in_specs=[
                pl.BlockSpec((rows, 128), lambda j, c: (0, j)),
                pl.BlockSpec((images, length, 128), lambda j, c: (0, 0, j)),
                pl.BlockSpec((images, length, 128), lambda j, c: (0, 0, pairs + j)),
            ],
            out_specs=[
                pl.BlockSpec((rows, 128), lambda j, c: (0, j)),
                pl.BlockSpec((1, 2, rows), lambda j, c: (j, 0, 0)),
            ],
        ),
        out_shape=[
            jax.ShapeDtypeStruct((rows, width), bf16),
            jax.ShapeDtypeStruct((pairs, 2, rows), f32),
        ],
        compiler_params=params(1),
        name="cross_forward",
        cost_estimate=cost(24),
    )(count, query, kv, kv)


def cross_backward_kernel(count_ref, q, k, v, g, totals, dq_out, dkv_out, dq, dk, dv):
    half_scale = (q.shape[1] // 2) ** (-0.5)
    scale = LOG2E * half_scale
    count = count_ref[0]
    first, skip, steps = cross_steps(count, q.shape[0] // TILE)
    dq[...] = jnp.zeros_like(dq)
    dk[...] = jnp.zeros_like(dk)
    dv[...] = jnp.zeros_like(dv)

    def one(step, carry):
        image, start = cross_step(step, first, skip)
        here = pl.ds(start, TILE)
        queries, grads = two_heads(q[here, :]), two_heads(g[here, :])
        lane = start + lax.broadcasted_iota(jnp.int32, (1, TILE), 1)
        mine = (lane >= count) == (image == 1)
        level = jnp.concatenate(
            [
                jnp.where(mine, totals[0, 0:1, here], -MASKED),
                jnp.where(mine, totals[0, 1:2, here], -MASKED),
            ],
            axis=1,
        )
        weights = jnp.exp2(product_t(k[image], queries) * scale - level)
        along = weights * product_t(v[image], grads)
        change = (along - weights * jnp.sum(along, axis=0, keepdims=True)).astype(bf16)
        dv[image] += product(weights.astype(bf16), grads)
        dk[image] += product(change, queries)
        dq[here, :] += join_heads(product_rows(k[image], change))
        return carry

    lax.fori_loop(0, steps, one, 0)
    dq_out[...] = (dq[...] * half_scale).astype(bf16)
    dkv_out[0] = (dk[...] * half_scale).astype(bf16)
    dkv_out[1] = dv[...].astype(bf16)


def cross_backward(count, query, kv, grads, totals):
    rows, width = query.shape
    pairs = width // 128
    images, length = kv.shape[:2]
    return pl.pallas_call(
        cross_backward_kernel,
        grid_spec=pltpu.PrefetchScalarGridSpec(
            num_scalar_prefetch=1,
            grid=(pairs,),
            in_specs=[
                pl.BlockSpec((rows, 128), lambda j, c: (0, j)),
                pl.BlockSpec((images, length, 128), lambda j, c: (0, 0, j)),
                pl.BlockSpec((images, length, 128), lambda j, c: (0, 0, pairs + j)),
                pl.BlockSpec((rows, 128), lambda j, c: (0, j)),
                pl.BlockSpec((1, 2, rows), lambda j, c: (j, 0, 0)),
            ],
            out_specs=[
                pl.BlockSpec((rows, 128), lambda j, c: (0, j)),
                pl.BlockSpec((2, images, length, 128), lambda j, c: (0, 0, 0, j)),
            ],
            scratch_shapes=[
                pltpu.VMEM((rows, 128), f32),
                pltpu.VMEM((images, length, 128), f32),
                pltpu.VMEM((images, length, 128), f32),
            ],
        ),
        out_shape=[
            jax.ShapeDtypeStruct((rows, width), bf16),
            jax.ShapeDtypeStruct((2, images, length, width), bf16),
        ],
        compiler_params=params(1),
        name="cross_backward",
        cost_estimate=cost(28),
    )(count, query, kv, kv, grads, totals)


def here(lanes):
    return lax.axis_index("dp") * lanes + lax.axis_index("fsdp")


def bit_of(number, bit):
    return (number // (1 << bit)) % 2


def stages(devices, lanes, way):
    return list(way) + list(range(lanes.bit_length(), devices.bit_length() - 1))


def place_of(relative, devices, lanes, way):
    place = 0
    for bit in stages(devices, lanes, way)[1:]:
        place = place * 2 + bit_of(relative, bit)
    return place


def put_rows(me, devices, lanes, way, left, staged):
    flipped = left.astype(f32).T
    depth = flipped.shape[0] // devices
    for block in range(devices):
        relative = block ^ me
        quarter = 2 * (1 - bit_of(relative, lanes.bit_length() - 1)) + (1 - bit_of(relative, way[0]))
        place = quarter * (devices // 4) + place_of(relative, devices, lanes, way)
        start = pl.multiple_of(place * depth, depth)
        staged[pl.ds(start, depth), :] = flipped[block * depth : (block + 1) * depth, :]


def greet(partner):
    barrier = pltpu.get_barrier_semaphore()
    pl.semaphore_signal(barrier, inc=1, device_id=partner, device_id_type=pl.DeviceIdType.MESH)
    pl.semaphore_wait(barrier, 1)


def other_core(me, lanes):
    other = me ^ lanes
    return (other // lanes, lax.rem(other, lanes))


def to_core(partner, source, target, send_sem, recv_sem):
    return pltpu.make_async_remote_copy(
        src_ref=source,
        dst_ref=target,
        send_sem=send_sem,
        recv_sem=recv_sem,
        device_id=partner,
        device_id_type=pl.DeviceIdType.MESH,
    )


def put_halves(total, out, keep):
    half = total.shape[0] // 2
    out[...] = total[:half, :].astype(bf16).reshape(out.shape)
    keep[...] = total[half:, :].astype(bf16).reshape(keep.shape)


def weight_grad_kernel(devices, lanes, way, given, *refs):
    left, right = refs[:2]
    out, keep, staged, flipped, sent, own, came, send_sem, recv_sem = refs[2 + given :]
    step, steps = pl.program_id(0), pl.num_programs(0) - 1
    me = here(lanes)
    partner = other_core(me, lanes)
    half = flipped.shape[1] // 2

    @pl.when(step == 0)
    def _():
        greet(partner)
        for part in range(left.shape[0]):
            put_rows(me, devices, lanes, way, left[part], staged)
            flipped[part] = staged[...].astype(bf16)

    def copy(at):
        return to_core(partner, sent.at[at % 2], came.at[at], send_sem.at[at], recv_sem.at[at])

    @pl.when(step < steps)
    def _():
        def rows(low):
            total = product(flipped[0, low : low + half, :], right[0, 0])
            for part in range(1, left.shape[0]):
                total += product(flipped[part, low : low + half, :], right[0, part])
            return total

        sent[step % 2] = rows(0).astype(bf16)
        own[step % 2] = rows(half)
        copy(step).start()

    @pl.when(step > 0)
    def _():
        copy(step - 1).wait()
        put_halves(own[(step - 1) % 2] + came[step - 1].astype(f32), out, keep)


def weight_grad(number, devices, lanes, way, left, right, columns, first=0, into=(), only=None):
    parts, rows, depth = left.shape
    low, high = only or (0, right.shape[0])
    kinds, width = high - low, right.shape[3]
    wide = 512
    across = width // wide
    steps = kinds * across
    block = (devices // 4, depth // devices, wide)
    spec = pl.BlockSpec(block, lambda s: (0, 0, first // wide + jnp.maximum(s - 1, 0)))
    shape = jax.ShapeDtypeStruct((devices // 4, depth // devices, columns), bf16)

    def source(s):
        s = jnp.minimum(s, steps - 1)
        return (low + s // across, 0, 0, s % across)

    return pl.pallas_call(
        functools.partial(weight_grad_kernel, devices, lanes, way, len(into)),
        grid=(steps + 1,),
        in_specs=[
            pl.BlockSpec((parts, rows, depth), lambda s: (0, 0, 0)),
            pl.BlockSpec((1, parts, rows, wide), source),
        ]
        + [pl.BlockSpec(memory_space=pltpu.HBM)] * len(into),
        out_specs=[spec, spec],
        scratch_shapes=[
            pltpu.VMEM((depth, rows), f32),
            pltpu.VMEM((parts, depth, rows), bf16),
            pltpu.VMEM((2, depth // 2, wide), bf16),
            pltpu.VMEM((2, depth // 2, wide), f32),
            pltpu.VMEM((steps, depth // 2, wide), bf16),
            pltpu.SemaphoreType.DMA((steps,)),
            pltpu.SemaphoreType.DMA((steps,)),
        ],
        out_shape=[shape, shape],
        input_output_aliases={2 + i: i for i in range(len(into))},
        compiler_params=pltpu.CompilerParams(
            dimension_semantics=("arbitrary",),
            vmem_limit_bytes=VMEM,
            collective_id=number,
            has_side_effects=True,
        ),
        name="weight_grad",
        cost_estimate=cost(3 * kinds * parts),
    )(left, right, *into)


def norm_grad_kernel(d_ref, w_ref, unit, inverse, gain, g_ref, out, low, gain_out, total):
    step = pl.program_id(0)
    kinds, _, width = d_ref.shape
    part = product_t(d_ref[0], w_ref[:, :width])
    for kind in range(1, kinds):
        part += product_t(d_ref[kind], w_ref[:, kind * width : (kind + 1) * width])
    wide = part.shape[1]
    total[:, pl.ds(pl.multiple_of(step * wide, wide), wide)] = part

    @pl.when(step == pl.num_programs(0) - 1)
    def _():
        change, gain_grad = norm_back(unit[...], inverse[...], gain[...], total[...])
        result = g_ref[...] + change
        out[...] = result
        low[...] = result.astype(bf16)
        gain_out[...] = gain_grad[None, :]


def norm_grad(grads, weights, first, unit, inverse, gain, g):
    kinds, rows, width = grads.shape
    wide = 256

    def whole(shape):
        return pl.BlockSpec(shape, lambda j: (0,) * len(shape))

    return pl.pallas_call(
        norm_grad_kernel,
        grid=(width // wide,),
        in_specs=[
            whole((kinds, rows, width)),
            pl.BlockSpec((wide, kinds * width), lambda j: (j, first)),
            whole((rows, width)), whole((rows, 1)), whole((1, width)), whole((rows, width)),
        ],
        out_specs=[whole((rows, width)), whole((rows, width)), whole((1, width))],
        out_shape=[
            jax.ShapeDtypeStruct((rows, width), f32),
            jax.ShapeDtypeStruct((rows, width), bf16),
            jax.ShapeDtypeStruct((1, width), f32),
        ],
        scratch_shapes=[pltpu.VMEM((rows, width), f32)],
        compiler_params=params(1),
        name="norm_grad",
        cost_estimate=cost(4 * kinds),
    )(grads, weights, unit, inverse, gain, g)


def feed_kernel(
    devices, lanes, ways, x_ref, g_ref, gain_ref, up_ref, down_ref,
    out, gx, low_gx, ggain, up_out, up_keep, down_out, down_keep,
    unit, inverse, hidden, staged, flipped, total, back,
    up_sent, up_own, up_came, down_sent, down_own, down_came,
    up_send_sem, up_recv_sem, down_send_sem, down_recv_sem,
):
    step, groups = pl.program_id(0), pl.num_programs(0) - 1
    me = here(lanes)
    partner = other_core(me, lanes)
    core, low, high = (me // lanes) % 2, me % lanes, me // (2 * lanes)

    @pl.when(step == 0)
    def _():
        greet(partner)
        h, u, i = normed(x_ref[...], gain_ref[...])
        unit[...] = u
        inverse[...] = i
        hidden[...] = h.astype(bf16)
        put_rows(me, devices, lanes, ways[0], h, staged)
        flipped[...] = staged[...].astype(bf16)
        total[...] = jnp.zeros_like(total)
        back[...] = jnp.zeros_like(back)

    def up_copy(at):
        return to_core(partner, up_sent.at[at % 2], up_came.at[at], up_send_sem.at[at], up_recv_sem.at[at])

    def down_copy(at):
        return to_core(partner, down_sent, down_came.at[at], down_send_sem.at[at], down_recv_sem.at[at])

    @pl.when(step < groups)
    def _():
        g = g_ref[...]
        up = up_ref[...].reshape(-1, up_ref.shape[-1])
        down = down_ref[...].reshape(-1, down_ref.shape[-1])
        inner = product(hidden[...], up)
        share = 0.5 + 0.5 * lax.erf(inner * (0.5**0.5))
        slope = share + inner * (jnp.exp(-0.5 * inner * inner) * 0.3989422804014327)
        active = (inner * share).astype(bf16)
        change = (product_t(g, down) * slope).astype(bf16)
        half = flipped.shape[0] // 2
        up_sent[step % 2] = product(flipped[:half, :], change).astype(bf16)
        grad_down = product_rows(active, g)

        @pl.when(step % 2 != core)
        def _():
            down_sent[...] = grad_down.astype(bf16)

        @pl.when(step % 2 == core)
        def _():
            down_own[...] = grad_down

        up_own[step % 2] = product(flipped[half:, :], change)
        total[...] += product(active, down)
        back[...] += product_t(change, up)
        up_copy(step).start()

        @pl.when(step % 2 != core)
        def _():
            down_copy(step // 2).start()

    @pl.when(step == groups)
    def _():
        out[...] = (x_ref[...] + total[...]).astype(bf16)
        gx_norm, gain_grad = norm_back(unit[...], inverse[...], gain_ref[...], back[...])
        result = g_ref[...].astype(f32) + gx_norm
        gx[...] = result
        low_gx[...] = result.astype(bf16)
        ggain[...] = gain_grad[None, :]

    @pl.when(step > 0)
    def _():
        before = step - 1
        up_copy(before).wait()
        put_halves(up_own[before % 2] + up_came[before].astype(f32), up_out, up_keep)

        @pl.when(before % 2 != core)
        def _():
            down_copy(before // 2).wait_send()

        @pl.when(before % 2 == core)
        def _():
            down_copy(before // 2).wait_recv()
            sums = down_own[...] + down_came[before // 2].astype(f32)
            depth = sums.shape[0] // lanes
            for block in range(lanes):
                relative = (block ^ low) + 2 * lanes * ((before // 2) ^ high)
                place = place_of(relative, devices, lanes, ways[1])
                piece = sums[block * depth : (block + 1) * depth, :].astype(bf16)
                goes = bit_of(relative, ways[1][0]) == 1

                @pl.when(goes)
                def _(place=place, piece=piece):
                    down_out[place] = piece

                @pl.when(jnp.logical_not(goes))
                def _(place=place, piece=piece):
                    down_keep[place] = piece


def feed(number, devices, lanes, ways, x, g, gain, weights):
    rows, width = x.shape
    pieces, depth = weights.shape[2:4]
    hidden = pieces * width
    groups = devices // lanes
    tile = hidden // groups
    across = width // tile

    def group(s):
        return jnp.minimum(s, groups - 1)

    def whole(shape):
        return pl.BlockSpec(shape, lambda s: (0,) * len(shape))

    up_block = pl.BlockSpec((devices // 4, depth, tile), lambda s: (0, 0, jnp.maximum(s - 1, 0)))
    up_shape = jax.ShapeDtypeStruct((devices // 4, depth, hidden), bf16)
    down_shape = jax.ShapeDtypeStruct((devices // 4, hidden // devices, width), bf16)
    return pl.pallas_call(
        functools.partial(feed_kernel, devices, lanes, ways),
        grid=(groups + 1,),
        in_specs=[
            whole((rows, width)),
            whole((rows, width)),
            whole((1, width)),
            pl.BlockSpec(
                (devices, None, None, depth, tile),
                lambda s: (0, 0, group(s) // across, 0, group(s) % across),
            ),
            pl.BlockSpec((lanes, None, pieces, depth, width), lambda s: (group(s), 1, 0, 0, 0)),
        ],
        out_specs=[
            whole((rows, width)), whole((rows, width)), whole((rows, width)), whole((1, width)),
            up_block, up_block, whole(down_shape.shape), whole(down_shape.shape),
        ],
        scratch_shapes=[
            pltpu.VMEM((rows, width), f32),
            pltpu.VMEM((rows, 1), f32),
            pltpu.VMEM((rows, width), bf16),
            pltpu.VMEM((width, rows), f32),
            pltpu.VMEM((width, rows), bf16),
            pltpu.VMEM((rows, width), f32),
            pltpu.VMEM((rows, width), f32),
            pltpu.VMEM((2, width // 2, tile), bf16),
            pltpu.VMEM((2, width // 2, tile), f32),
            pltpu.VMEM((groups, width // 2, tile), bf16),
            pltpu.VMEM((tile, width), bf16),
            pltpu.VMEM((tile, width), f32),
            pltpu.VMEM((groups // 2, tile, width), bf16),
            pltpu.SemaphoreType.DMA((groups,)),
            pltpu.SemaphoreType.DMA((groups,)),
            pltpu.SemaphoreType.DMA((groups // 2,)),
            pltpu.SemaphoreType.DMA((groups // 2,)),
        ],
        out_shape=[
            jax.ShapeDtypeStruct((rows, width), bf16),
            jax.ShapeDtypeStruct((rows, width), f32),
            jax.ShapeDtypeStruct((rows, width), bf16),
            jax.ShapeDtypeStruct((1, width), f32),
            up_shape, up_shape, down_shape, down_shape,
        ],
        compiler_params=pltpu.CompilerParams(
            dimension_semantics=("arbitrary",),
            vmem_limit_bytes=VMEM,
            collective_id=number,
            has_side_effects=True,
        ),
        name="feed",
        cost_estimate=cost(40),
    )(x, g, gain, weights, weights)


def gather_kernel(devices, lanes, tracks, x_ref, out, own_sem, send_sem, recv_sem):
    me = lax.axis_index("dp") * lanes + lax.axis_index("fsdp")
    count = devices // 2

    def device(bit):
        other = me ^ bit
        return (other // lanes, lax.rem(other, lanes))

    barrier = pltpu.get_barrier_semaphore()
    every = [1 << b for b in range(devices.bit_length() - 1)]
    for bit in every:
        pl.semaphore_signal(
            barrier, inc=1, device_id=device(bit), device_id_type=pl.DeviceIdType.MESH
        )
    pl.semaphore_wait(barrier, len(every))
    own = pltpu.make_async_copy(x_ref, out.at[me], own_sem)
    own.start()
    sends = []

    def block(track, number, to_core):
        low, high, bits = tracks[track]
        owner = me ^ sum(b for p, b in enumerate(bits) if (number >> p) & 1)
        return out.at[owner ^ lanes if to_core else owner, :, low:high]

    def arrived(track, number):
        to_core = number >= count
        here = block(track, number - count if to_core else number, to_core)
        pltpu.make_async_remote_copy(
            src_ref=here,
            dst_ref=here,
            send_sem=send_sem.at[0],
            recv_sem=recv_sem.at[track, number],
            device_id=device(lanes),
            device_id_type=pl.DeviceIdType.MESH,
        ).wait_recv()
        return here

    for number in sorted(range(count), key=lambda k: (bin(k).count("1"), k)):
        for track, (low, high, bits) in enumerate(tracks):
            there = block(track, number, False)
            here = arrived(track, number) if number else x_ref.at[:, low:high]
            for place, bit in enumerate(bits + (lanes,)):
                if number >> place == 0 or bit == lanes:
                    copy = pltpu.make_async_remote_copy(
                        src_ref=here,
                        dst_ref=there,
                        send_sem=send_sem.at[len(sends)],
                        recv_sem=recv_sem.at[track, number + (1 << place)],
                        device_id=device(bit),
                        device_id_type=pl.DeviceIdType.MESH,
                    )
                    copy.start()
                    sends.append(copy)
    for number in range(count, devices):
        for track in range(len(tracks)):
            arrived(track, number)
    for copy in sends:
        copy.wait_send()
    own.wait()


def gather(number, devices, lanes, values):
    depth, columns = values.shape
    middle = (columns // 256) * 128
    high = tuple(2 * lanes << b for b in range((devices // (2 * lanes)).bit_length() - 1))
    links = [high + tuple(1 << b for b in way) for way in orders(lanes)]
    tracks = ((0, middle, links[0]), (middle, columns, links[1]))
    return pl.pallas_call(
        functools.partial(gather_kernel, devices, lanes, tracks),
        in_specs=[pl.BlockSpec(memory_space=pltpu.VMEM)],
        out_specs=pl.BlockSpec(memory_space=pltpu.HBM),
        out_shape=jax.ShapeDtypeStruct((devices, depth, columns), values.dtype),
        scratch_shapes=[
            pltpu.SemaphoreType.DMA,
            pltpu.SemaphoreType.DMA((len(tracks) * (devices - 1),)),
            pltpu.SemaphoreType.DMA((len(tracks), devices)),
        ],
        compiler_params=pltpu.CompilerParams(collective_id=number, has_side_effects=True),
        name="gather",
        cost_estimate=cost(40),
    )(values).reshape(-1, columns)


def swap(values, devices, bit):
    return lax.ppermute(values, AXES, [(i, i ^ bit) for i in range(devices)])


def plus(a, b):
    return (a.astype(f32) + b.astype(f32)).astype(bf16)


def owner_sums(halves, devices, lanes, way, late=None):
    bits = stages(devices, lanes, way)
    out, keep = halves
    for stage, bit in enumerate(bits):
        arrived = swap(out, devices, 1 << bit)
        if stage == len(bits) - 1:
            return keep[0].astype(f32) + arrived[0].astype(f32)
        half = keep.shape[0] // 2
        out, keep = plus(keep[half:], arrived[half:]), plus(keep[:half], arrived[:half])
        if stage == 0 and late is not None:
            late_out, late_keep = late
            late_arrived = swap(late_out, devices, 1 << bit)
            out = jnp.concatenate([out, plus(late_keep[half:], late_arrived[half:])], axis=-1)
            keep = jnp.concatenate([keep, plus(late_keep[:half], late_arrived[:half])], axis=-1)


def gain_halves(values, devices, lanes, way, me):
    kinds, depth = values.shape
    blocks = jnp.pad(values.T, ((0, 0), (0, 128 - kinds))).astype(bf16)
    every = range(devices)
    core = lanes.bit_length() - 1
    order = sorted(every, key=lambda r: (1 - bit_of(r, core), 1 - bit_of(r, way[0]), place_of(r, devices, lanes, way)))
    blocks = blocks.reshape(devices, depth // devices, 128)[jnp.array(order) ^ me]
    arrived = swap(blocks[: devices // 2], devices, lanes)
    sums = plus(blocks[devices // 2 :], arrived)
    return sums[: devices // 4], sums[devices // 4 :]


def after(values, first):
    return lax.optimization_barrier((values, first))[0]


def orders(lanes):
    low = list(range(lanes.bit_length() - 1))
    return low, low[::-1]


def shards(devices, lanes, tokens, images, segment_ids, image_map, out_grad, norm_self, attn_query,
           attn_key, attn_value, attn_out, norm_cross, cross_query, cross_key, cross_value, cross_out,
           norm_ffn, ffn_up, ffn_down):
    me = lax.axis_index("dp") * lanes + lax.axis_index("fsdp")
    me_ref = me.astype(jnp.int32)[None]
    depth, width = attn_query.shape
    gains = jnp.stack([norm_self, norm_cross, norm_ffn], axis=1)
    gains = jnp.pad(gains, ((0, 0), (0, 128 - 3)))
    first_set = jnp.concatenate([attn_query, attn_key, attn_value, cross_key, cross_value, gains], axis=1)
    second_set = jnp.concatenate([attn_out, cross_query, cross_out], axis=1)
    pieces = ffn_up.shape[1] // width
    feed_set = jnp.stack(
        [ffn_up.reshape(depth, pieces, width).transpose(1, 0, 2), ffn_down.reshape(pieces, depth, width)]
    )
    first_set = gather(0, devices, lanes, first_set)
    feed_set = lax.all_gather(after(feed_set, first_set), AXES, axis=0)
    w_qkv = first_set[:, : 3 * width]
    w_kv = first_set[:, 3 * width : 5 * width]
    gains = first_set[:, 5 * width : 5 * width + 3].T.astype(f32)

    pages = segment_ids[0]
    length = pages.shape[0]
    page_index = jnp.arange(image_map.shape[1])
    second = jnp.sum(jnp.where(pages[:, None] == page_index[None, :], image_map[0][None, :], 0), axis=1)
    place_now = jnp.arange(length)
    earlier = place_now[None, :] < place_now[:, None]
    ones_before = jnp.sum(jnp.where(earlier, second[None, :], 0), axis=1)
    count = length - jnp.sum(second)
    place = jnp.where(second == 1, count + ones_before, place_now - ones_before)
    moved = place_now[:, None] == place[None, :]
    order = moved.astype(bf16)
    count = count.astype(jnp.int32)[None]
    pages = jnp.sum(jnp.where(moved, pages[None, :], 0), axis=1)
    inputs = product(order, tokens[0])
    grad_out = product(order, out_grad[0]).astype(bf16)

    hidden_one, unit_one, inverse_one = normed(inputs, gains[0:1])
    hidden_one = hidden_one.astype(bf16)
    qkv = product(hidden_one, w_qkv).astype(bf16)
    mixed_one, log_one = self_forward(pages, qkv)
    kv = lax.dot_general(images, w_kv, (((2,), (0,)), ((), ())), preferred_element_type=f32).astype(bf16)
    second_set = gather(1, devices, lanes, after(second_set, (mixed_one, kv)))
    w_out = second_set[:, :width]
    w_cross_query = second_set[:, width : 2 * width]
    w_cross_out = second_set[:, 2 * width :]
    after_self = inputs + product(mixed_one, w_out)
    hidden_two, unit_two, inverse_two = normed(after_self, gains[1:2])
    hidden_two = hidden_two.astype(bf16)
    query_two = product(hidden_two, w_cross_query).astype(bf16)
    mixed_two, log_two = cross_forward(count, query_two, kv)
    after_cross = after_self + product(mixed_two, w_cross_out)

    one_way, other_way = orders(lanes)
    (output, grad_after_cross, branch_two, grad_gain_ffn, *halves) = feed(
        2, devices, lanes, (one_way, other_way), after_cross, grad_out, gains[2:3], feed_set
    )

    def sums(way, halves, late=None):
        return owner_sums(halves, devices, lanes, way, late)

    def halves_of(number, way, left, right, **options):
        return weight_grad(number, devices, lanes, way, left, right, 2 * width, **options)

    grad_up = sums(one_way, halves[:2])
    grad_down = sums(other_way, halves[2:])

    grad_mixed_two = product_t(branch_two, w_cross_out).astype(bf16)
    grad_query_two, grad_kv = cross_backward(count, query_two, kv, grad_mixed_two, log_two)
    halves = halves_of(3, one_way, mixed_two[None], after(branch_two, grad_kv)[None, None])
    halves = halves_of(4, one_way, hidden_two[None], grad_query_two[None, None], first=width, into=halves)
    grad_c = sums(one_way, halves)
    halves = halves_of(5, other_way, images, after(grad_kv, halves[0]))
    grad_d = sums(other_way, halves)
    grad_after_self, branch_one, grad_gain_cross = norm_grad(
        after(grad_query_two, halves[0])[None], second_set, 1, unit_two, inverse_two, gains[1:2], grad_after_cross
    )
    grad_mixed_one = product_t(branch_one, w_out).astype(bf16)
    grad_qkv = self_backward(pages, qkv, grad_mixed_one, log_one)
    halves = halves_of(6, one_way, mixed_one[None], after(branch_one, grad_qkv)[None, None])
    options = dict(first=width, into=halves, only=(0, 1))
    halves = halves_of(7, one_way, hidden_one[None], grad_qkv[:, None], **options)
    grad_qkv_again = after(grad_qkv, halves[0])
    _, grad_inputs, grad_gain_self = norm_grad(
        grad_qkv_again, first_set, 0, unit_one, inverse_one, gains[0:1], grad_after_self
    )
    grad_qkv_again = after(grad_qkv, grad_inputs)
    halves_kv = halves_of(8, one_way, hidden_one[None], grad_qkv_again[:, None], only=(1, 3))
    gain_grads = jnp.concatenate([grad_gain_self, grad_gain_cross, grad_gain_ffn])
    late = gain_halves(gain_grads, devices, lanes, one_way, me)
    grad_a = sums(one_way, halves)
    grad_b = sums(one_way, halves_kv, late)
    gain_sums = grad_b[:, 2 * width :]

    grad_kv = after(grad_kv, halves_kv[0])
    back = (((2,), (1,)), ((), ()))
    grad_images = lax.dot_general(grad_kv[0], w_kv[:, :width], back, preferred_element_type=f32)
    grad_images += lax.dot_general(grad_kv[1], w_kv[:, width:], back, preferred_element_type=f32)
    output = product_rows(order, output).astype(bf16)
    grad_inputs = product_rows(order, grad_inputs).astype(bf16)
    return (
        output[None],
        grad_inputs[None],
        grad_images.astype(bf16),
        gain_sums[:, 0],
        grad_a[:, width:],
        grad_b[:, :width],
        grad_b[:, width : 2 * width],
        grad_a[:, :width],
        gain_sums[:, 1],
        grad_c[:, width:],
        grad_d[:, :width],
        grad_d[:, width:],
        grad_c[:, :width],
        gain_sums[:, 2],
        grad_up,
        grad_down,
    )


def solution(mesh):
    rows = P(AXES)
    devices, lanes = mesh.shape["dp"] * mesh.shape["fsdp"], mesh.shape["fsdp"]
    return jax.shard_map(
        functools.partial(shards, devices, lanes),
        mesh=mesh,
        in_specs=(rows,) * 18,
        out_specs=(rows,) * 16,
        check_vma=False,
    )
```

```python
import functools

import jax
import jax.numpy as jnp
from jax import lax
from jax.experimental import pallas as pl
from jax.experimental.pallas import tpu as pltpu
from jax.sharding import PartitionSpec as P


AXES = ("dp", "fsdp")
LOG2E = 1.4426950408889634
EPSILON = 1e-05
MASKED = -1e30
TILE = 128
PAGE_MAX = 256
VMEM = 62 * 1024 * 1024

bf16 = jnp.bfloat16
f32 = jnp.float32


def product(left, right):
    return jnp.dot(left, right, preferred_element_type=f32)


def product_t(left, right):
    return lax.dot_general(left, right, (((1,), (1,)), ((), ())), preferred_element_type=f32)


def product_rows(left, right):
    return lax.dot_general(left, right, (((0,), (0,)), ((), ())), preferred_element_type=f32)


def normed(values, gain):
    centred = values - jnp.mean(values, axis=-1, keepdims=True)
    variance = jnp.mean(centred * centred, axis=-1, keepdims=True)
    inverse = lax.rsqrt(variance + EPSILON)
    unit = centred * inverse
    return unit * gain, unit, inverse


def norm_back(unit, inverse, gain, gradient):
    scaled = gradient * gain
    mean_scaled = jnp.mean(scaled, axis=-1, keepdims=True)
    mean_along = jnp.mean(scaled * unit, axis=-1, keepdims=True)
    return inverse * (scaled - mean_scaled - unit * mean_along), jnp.sum(gradient * unit, axis=0)


def params(count):
    return pltpu.CompilerParams(
        dimension_semantics=("arbitrary",) * count, vmem_limit_bytes=VMEM
    )


def cost(microseconds):
    return pl.CostEstimate(flops=int(microseconds * 1e9), bytes_accessed=0, transcendentals=0)


def two_heads(block):
    lane = lax.broadcasted_iota(jnp.int32, block.shape, 1)
    zero = jnp.zeros_like(block)
    half = block.shape[1] // 2
    return jnp.concatenate(
        [jnp.where(lane < half, block, zero), jnp.where(lane >= half, block, zero)], axis=0
    )


def join_heads(both):
    rows = both.shape[1] // 2
    feature = lax.broadcasted_iota(jnp.int32, (both.shape[0], rows), 0)
    return jnp.where(feature < both.shape[0] // 2, both[:, :rows], both[:, rows:]).T


def twice(row):
    return jnp.concatenate([row, row], axis=1)


def arrange_kernel(
    map_ref, page_column, page_row, tokens, g, columns,
    count, order, new_column, new_row, inputs, new_g, hidden, unit, inverse, *gains,
):
    rows = tokens.shape[0]

    def second_of(pages):
        return sum(jnp.where(pages == p, map_ref[p], 0) for p in range(map_ref.shape[0])).astype(f32)

    column, row = second_of(page_column[...]), second_of(page_row[...])
    i = lax.broadcasted_iota(jnp.int32, (rows, rows), 0)
    j = lax.broadcasted_iota(jnp.int32, (rows, rows), 1)
    before_column = jnp.sum(jnp.where(j < i, row, 0.0), axis=1, keepdims=True)
    before_row = jnp.sum(jnp.where(i < j, column, 0.0), axis=0, keepdims=True)
    first = rows - jnp.sum(row)
    count[0] = first.astype(jnp.int32)
    at_column = lax.broadcasted_iota(jnp.int32, (rows, 1), 0).astype(f32)
    at_row = lax.broadcasted_iota(jnp.int32, (1, rows), 1).astype(f32)
    place_column = jnp.where(column > 0, first + before_column, at_column - before_column)
    place_row = jnp.where(row > 0, first + before_row, at_row - before_row)
    moved = i.astype(f32) == place_row
    order[...] = moved.astype(f32).astype(bf16)
    pages = page_row[...].astype(f32)
    new_column[...] = jnp.sum(jnp.where(moved, pages, 0.0), axis=1, keepdims=True).astype(jnp.int32)
    pages = page_column[...].astype(f32)
    back = place_column == j.astype(f32)
    new_row[...] = jnp.sum(jnp.where(back, pages, 0.0), axis=0, keepdims=True).astype(jnp.int32)
    new_g[...] = product(order[...], g[...]).astype(bf16)
    flat = columns[...].astype(f32).T
    for number, gain in enumerate(gains):
        gain[...] = flat[number : number + 1, :]
    inputs[...] = product(order[...], tokens[...])
    h, unit[...], inverse[...] = normed(inputs[...], gains[0][...])
    hidden[...] = h.astype(bf16)


def arrange(image_map, pages, tokens, g, weights, first):
    rows, width = tokens.shape

    def whole(*shape):
        return pl.BlockSpec(shape, lambda s: (0,) * len(shape))

    scalars = pl.BlockSpec(memory_space=pltpu.SMEM)
    kinds = [
        ((rows, rows), bf16), ((rows, 1), jnp.int32), ((1, rows), jnp.int32),
        ((rows, width), f32), ((rows, width), bf16), ((rows, width), bf16),
        ((rows, width), f32), ((rows, 1), f32), *[((1, width), f32)] * 3,
    ]
    return pl.pallas_call(
        arrange_kernel,
        grid=(1,),
        in_specs=[
            scalars, whole(rows, 1), whole(1, rows), whole(rows, width), whole(rows, width),
            pl.BlockSpec((width, 128), lambda s: (0, first)),
        ],
        out_specs=[scalars] + [whole(*shape) for shape, _ in kinds],
        out_shape=[jax.ShapeDtypeStruct((1,), jnp.int32)]
        + [jax.ShapeDtypeStruct(shape, dtype) for shape, dtype in kinds],
        compiler_params=params(1),
        name="arrange",
        cost_estimate=cost(6),
    )(image_map, pages[:, None], pages[None, :], tokens, g, weights)


def between_kernel(x_ref, mixed, w_out, w_query, gain, x_out, hidden, unit, inverse, query):
    x = x_ref[...] + product(mixed[...], w_out[...])
    x_out[...] = x
    h, unit[...], inverse[...] = normed(x, gain[...])
    hidden[...] = h.astype(bf16)
    query[...] = product(hidden[...], w_query[...]).astype(bf16)


def between(x, mixed, weights, gain):
    rows, width = x.shape
    tile = rows // 2

    def part(columns):
        return pl.BlockSpec((tile, columns), lambda s: (s, 0))

    kinds = ((width, f32), (width, bf16), (width, f32), (1, f32), (width, bf16))
    return pl.pallas_call(
        between_kernel,
        grid=(2,),
        in_specs=[
            part(width), part(width),
            pl.BlockSpec((width, width), lambda s: (0, 0)),
            pl.BlockSpec((width, width), lambda s: (0, 1)),
            pl.BlockSpec((1, width), lambda s: (0, 0)),
        ],
        out_specs=[part(columns) for columns, _ in kinds],
        out_shape=[jax.ShapeDtypeStruct((rows, columns), dtype) for columns, dtype in kinds],
        compiler_params=params(1),
        name="between",
        cost_estimate=cost(8),
    )(x, mixed, weights, weights, gain)


def key_range(tile):
    return max(0, tile * TILE - PAGE_MAX), (tile + 1) * TILE


def fill_bias(page_column, page_row, bias, tiles):
    for tile in range(tiles):
        low, high = key_range(tile)
        keys = low + lax.broadcasted_iota(jnp.int32, (high - low, TILE), 0)
        queries = tile * TILE + lax.broadcasted_iota(jnp.int32, (high - low, TILE), 1)
        same = page_column[low:high, :] == page_row[:, tile * TILE : (tile + 1) * TILE]
        bias[tile, : high - low, :] = jnp.where((keys <= queries) & same, 0.0, MASKED)


def self_forward_kernel(page_column, page_row, q, k, v, out, totals, bias):
    tiles = q.shape[0] // TILE
    scale = LOG2E * (q.shape[1] // 2) ** (-0.5)

    @pl.when(pl.program_id(0) == 0)
    def _():
        fill_bias(page_column, page_row, bias, tiles)

    for tile in range(tiles):
        low, high = key_range(tile)
        here = slice(tile * TILE, (tile + 1) * TILE)
        scores = product_t(k[low:high, :], two_heads(q[here, :])) * scale + twice(
            bias[tile, : high - low, :]
        )
        highest = jnp.max(scores, axis=0, keepdims=True)
        weights = jnp.exp2(scores - highest)
        total = jnp.sum(weights, axis=0, keepdims=True)
        mixed = product_rows(v[low:high, :], weights.astype(bf16)) * (1.0 / total)
        out[here, :] = join_heads(mixed).astype(bf16)
        level = highest + jnp.log2(total)
        totals[0, 0:1, here] = level[:, :TILE]
        totals[0, 1:2, here] = level[:, TILE:]


def self_forward(page_column, page_row, qkv):
    rows, width = qkv.shape[0], qkv.shape[1] // 3
    pairs = width // 128
    return pl.pallas_call(
        self_forward_kernel,
        grid=(pairs,),
        in_specs=[
            pl.BlockSpec((rows, 1), lambda j: (0, 0)),
            pl.BlockSpec((1, rows), lambda j: (0, 0)),
            pl.BlockSpec((rows, 128), lambda j: (0, j)),
            pl.BlockSpec((rows, 128), lambda j: (0, pairs + j)),
            pl.BlockSpec((rows, 128), lambda j: (0, 2 * pairs + j)),
        ],
        out_specs=[
            pl.BlockSpec((rows, 128), lambda j: (0, j)),
            pl.BlockSpec((1, 2, rows), lambda j: (j, 0, 0)),
        ],
        out_shape=[
            jax.ShapeDtypeStruct((rows, width), bf16),
            jax.ShapeDtypeStruct((pairs, 2, rows), f32),
        ],
        scratch_shapes=[pltpu.VMEM((rows // TILE, PAGE_MAX + TILE, TILE), f32)],
        compiler_params=params(1),
        name="self_forward",
        cost_estimate=cost(14),
    )(page_column, page_row, qkv, qkv, qkv)


def self_backward_kernel(page_column, page_row, q, k, v, g, totals, out, bias, dk, dv):
    tiles = q.shape[0] // TILE
    half_scale = (q.shape[1] // 2) ** (-0.5)
    scale = LOG2E * half_scale

    @pl.when(pl.program_id(0) == 0)
    def _():
        fill_bias(page_column, page_row, bias, tiles)

    dk[...] = jnp.zeros_like(dk)
    dv[...] = jnp.zeros_like(dv)
    for tile in range(tiles):
        low, high = key_range(tile)
        here = slice(tile * TILE, (tile + 1) * TILE)
        queries, grads = two_heads(q[here, :]), two_heads(g[here, :])
        keys, values = k[low:high, :], v[low:high, :]
        level = jnp.concatenate([totals[0, 0:1, here], totals[0, 1:2, here]], axis=1)
        weights = jnp.exp2(
            product_t(keys, queries) * scale + twice(bias[tile, : high - low, :]) - level
        )
        along = weights * product_t(values, grads)
        change = (along - weights * jnp.sum(along, axis=0, keepdims=True)).astype(bf16)
        dv[low:high, :] += product(weights.astype(bf16), grads)
        dk[low:high, :] += product(change, queries)
        out[0, here, :] = (join_heads(product_rows(keys, change)) * half_scale).astype(bf16)
    out[1] = (dk[...] * half_scale).astype(bf16)
    out[2] = dv[...].astype(bf16)


def self_backward(page_column, page_row, qkv, grads, totals):
    rows, width = qkv.shape[0], qkv.shape[1] // 3
    pairs = width // 128
    return pl.pallas_call(
        self_backward_kernel,
        grid=(pairs,),
        in_specs=[
            pl.BlockSpec((rows, 1), lambda j: (0, 0)),
            pl.BlockSpec((1, rows), lambda j: (0, 0)),
            pl.BlockSpec((rows, 128), lambda j: (0, j)),
            pl.BlockSpec((rows, 128), lambda j: (0, pairs + j)),
            pl.BlockSpec((rows, 128), lambda j: (0, 2 * pairs + j)),
            pl.BlockSpec((rows, 128), lambda j: (0, j)),
            pl.BlockSpec((1, 2, rows), lambda j: (j, 0, 0)),
        ],
        out_specs=pl.BlockSpec((3, rows, 128), lambda j: (0, 0, j)),
        out_shape=jax.ShapeDtypeStruct((3, rows, width), bf16),
        scratch_shapes=[
            pltpu.VMEM((rows // TILE, PAGE_MAX + TILE, TILE), f32),
            pltpu.VMEM((rows, 128), f32),
            pltpu.VMEM((rows, 128), f32),
        ],
        compiler_params=params(1),
        name="self_backward",
        cost_estimate=cost(15),
    )(page_column, page_row, qkv, qkv, qkv, grads, totals)


def cross_steps(count, tiles):
    first = (count + TILE - 1) // TILE
    skip = count // TILE
    return first, skip, first + tiles - skip


def cross_step(step, first, skip):
    image = jnp.where(step < first, 0, 1)
    tile = jnp.where(step < first, step, step - first + skip)
    return image, pl.multiple_of(tile * TILE, TILE)


def cross_forward_kernel(count_ref, q, k, v, out, totals):
    scale = LOG2E * (q.shape[1] // 2) ** (-0.5)
    count = count_ref[0]
    first, skip, steps = cross_steps(count, q.shape[0] // TILE)

    def one(step, carry):
        image, start = cross_step(step, first, skip)
        here = pl.ds(start, TILE)
        scores = product_t(k[image], two_heads(q[here, :])) * scale
        highest = jnp.max(scores, axis=0, keepdims=True)
        weights = jnp.exp2(scores - highest)
        total = jnp.sum(weights, axis=0, keepdims=True)
        mixed = product_rows(v[image], weights.astype(bf16)) * (1.0 / total)
        row = start + lax.broadcasted_iota(jnp.int32, (TILE, 128), 0)
        mine = (row >= count) == (image == 1)
        out[here, :] = jnp.where(mine, join_heads(mixed), out[here, :].astype(f32)).astype(bf16)
        level = highest + jnp.log2(total)
        lane = start + lax.broadcasted_iota(jnp.int32, (1, TILE), 1)
        mine = (lane >= count) == (image == 1)
        totals[0, 0:1, here] = jnp.where(mine, level[:, :TILE], totals[0, 0:1, here])
        totals[0, 1:2, here] = jnp.where(mine, level[:, TILE:], totals[0, 1:2, here])
        return carry

    lax.fori_loop(0, steps, one, 0)


def cross_forward(count, query, kv):
    rows, width = query.shape
    pairs = width // 128
    images, length = kv.shape[:2]
    return pl.pallas_call(
        cross_forward_kernel,
        grid_spec=pltpu.PrefetchScalarGridSpec(
            num_scalar_prefetch=1,
            grid=(pairs,),
            in_specs=[
                pl.BlockSpec((rows, 128), lambda j, c: (0, j)),
                pl.BlockSpec((images, length, 128), lambda j, c: (0, 0, j)),
                pl.BlockSpec((images, length, 128), lambda j, c: (0, 0, pairs + j)),
            ],
            out_specs=[
                pl.BlockSpec((rows, 128), lambda j, c: (0, j)),
                pl.BlockSpec((1, 2, rows), lambda j, c: (j, 0, 0)),
            ],
        ),
        out_shape=[
            jax.ShapeDtypeStruct((rows, width), bf16),
            jax.ShapeDtypeStruct((pairs, 2, rows), f32),
        ],
        compiler_params=params(1),
        name="cross_forward",
        cost_estimate=cost(24),
    )(count, query, kv, kv)


def cross_backward_kernel(count_ref, q, k, v, g, totals, dq_out, dkv_out, dq, dk, dv):
    half_scale = (q.shape[1] // 2) ** (-0.5)
    scale = LOG2E * half_scale
    count = count_ref[0]
    first, skip, steps = cross_steps(count, q.shape[0] // TILE)
    dq[...] = jnp.zeros_like(dq)
    dk[...] = jnp.zeros_like(dk)
    dv[...] = jnp.zeros_like(dv)

    def one(step, carry):
        image, start = cross_step(step, first, skip)
        here = pl.ds(start, TILE)
        queries, grads = two_heads(q[here, :]), two_heads(g[here, :])
        lane = start + lax.broadcasted_iota(jnp.int32, (1, TILE), 1)
        mine = (lane >= count) == (image == 1)
        level = jnp.concatenate(
            [
                jnp.where(mine, totals[0, 0:1, here], -MASKED),
                jnp.where(mine, totals[0, 1:2, here], -MASKED),
            ],
            axis=1,
        )
        weights = jnp.exp2(product_t(k[image], queries) * scale - level)
        along = weights * product_t(v[image], grads)
        change = (along - weights * jnp.sum(along, axis=0, keepdims=True)).astype(bf16)
        dv[image] += product(weights.astype(bf16), grads)
        dk[image] += product(change, queries)
        dq[here, :] += join_heads(product_rows(k[image], change))
        return carry

    lax.fori_loop(0, steps, one, 0)
    dq_out[...] = (dq[...] * half_scale).astype(bf16)
    dkv_out[0] = (dk[...] * half_scale).astype(bf16)
    dkv_out[1] = dv[...].astype(bf16)


def cross_backward(count, query, kv, grads, totals):
    rows, width = query.shape
    pairs = width // 128
    images, length = kv.shape[:2]
    return pl.pallas_call(
        cross_backward_kernel,
        grid_spec=pltpu.PrefetchScalarGridSpec(
            num_scalar_prefetch=1,
            grid=(pairs,),
            in_specs=[
                pl.BlockSpec((rows, 128), lambda j, c: (0, j)),
                pl.BlockSpec((images, length, 128), lambda j, c: (0, 0, j)),
                pl.BlockSpec((images, length, 128), lambda j, c: (0, 0, pairs + j)),
                pl.BlockSpec((rows, 128), lambda j, c: (0, j)),
                pl.BlockSpec((1, 2, rows), lambda j, c: (j, 0, 0)),
            ],
            out_specs=[
                pl.BlockSpec((rows, 128), lambda j, c: (0, j)),
                pl.BlockSpec((2, images, length, 128), lambda j, c: (0, 0, 0, j)),
            ],
            scratch_shapes=[
                pltpu.VMEM((rows, 128), f32),
                pltpu.VMEM((images, length, 128), f32),
                pltpu.VMEM((images, length, 128), f32),
            ],
        ),
        out_shape=[
            jax.ShapeDtypeStruct((rows, width), bf16),
            jax.ShapeDtypeStruct((2, images, length, width), bf16),
        ],
        compiler_params=params(1),
        name="cross_backward",
        cost_estimate=cost(28),
    )(count, query, kv, kv, grads, totals)


def here(lanes):
    return lax.axis_index("dp") * lanes + lax.axis_index("fsdp")


def bit_of(number, bit):
    return (number // (1 << bit)) % 2


def stages(devices, lanes, way):
    return list(way) + list(range(lanes.bit_length(), devices.bit_length() - 1))


def place_of(relative, devices, lanes, way):
    place = 0
    for bit in stages(devices, lanes, way)[1:]:
        place = place * 2 + bit_of(relative, bit)
    return place


def put_rows(me, devices, lanes, way, left, staged):
    flipped = left.astype(f32).T
    depth = flipped.shape[0] // devices
    for block in range(devices):
        relative = block ^ me
        quarter = 2 * (1 - bit_of(relative, lanes.bit_length() - 1)) + (1 - bit_of(relative, way[0]))
        place = quarter * (devices // 4) + place_of(relative, devices, lanes, way)
        start = pl.multiple_of(place * depth, depth)
        staged[pl.ds(start, depth), :] = flipped[block * depth : (block + 1) * depth, :]


def greet(partner):
    barrier = pltpu.get_barrier_semaphore()
    pl.semaphore_signal(barrier, inc=1, device_id=partner, device_id_type=pl.DeviceIdType.MESH)
    pl.semaphore_wait(barrier, 1)


def other_core(me, lanes):
    other = me ^ lanes
    return (other // lanes, lax.rem(other, lanes))


def to_core(partner, source, target, send_sem, recv_sem):
    return pltpu.make_async_remote_copy(
        src_ref=source,
        dst_ref=target,
        send_sem=send_sem,
        recv_sem=recv_sem,
        device_id=partner,
        device_id_type=pl.DeviceIdType.MESH,
    )


def put_halves(total, out, keep):
    half = total.shape[0] // 2
    out[...] = total[:half, :].astype(bf16).reshape(out.shape)
    keep[...] = total[half:, :].astype(bf16).reshape(keep.shape)


def weight_grad_kernel(devices, lanes, way, given, *refs):
    left, right = refs[:2]
    out, keep, staged, flipped, sent, own, came, send_sem, recv_sem = refs[2 + given :]
    step, steps = pl.program_id(0), pl.num_programs(0) - 1
    me = here(lanes)
    partner = other_core(me, lanes)
    half = flipped.shape[1] // 2

    @pl.when(step == 0)
    def _():
        greet(partner)
        for part in range(left.shape[0]):
            put_rows(me, devices, lanes, way, left[part], staged)
            flipped[part] = staged[...].astype(bf16)

    def copy(at):
        return to_core(partner, sent.at[at % 2], came.at[at], send_sem.at[at], recv_sem.at[at])

    @pl.when(step < steps)
    def _():
        def rows(low):
            total = product(flipped[0, low : low + half, :], right[0, 0])
            for part in range(1, left.shape[0]):
                total += product(flipped[part, low : low + half, :], right[0, part])
            return total

        sent[step % 2] = rows(0).astype(bf16)
        own[step % 2] = rows(half)
        copy(step).start()

    @pl.when(step > 0)
    def _():
        copy(step - 1).wait()
        put_halves(own[(step - 1) % 2] + came[step - 1].astype(f32), out, keep)


def weight_grad(number, devices, lanes, way, left, right, columns, first=0, into=(), only=None):
    parts, rows, depth = left.shape
    low, high = only or (0, right.shape[0])
    kinds, width = high - low, right.shape[3]
    wide = 512
    across = width // wide
    steps = kinds * across
    block = (devices // 4, depth // devices, wide)
    spec = pl.BlockSpec(block, lambda s: (0, 0, first // wide + jnp.maximum(s - 1, 0)))
    shape = jax.ShapeDtypeStruct((devices // 4, depth // devices, columns), bf16)

    def source(s):
        s = jnp.minimum(s, steps - 1)
        return (low + s // across, 0, 0, s % across)

    return pl.pallas_call(
        functools.partial(weight_grad_kernel, devices, lanes, way, len(into)),
        grid=(steps + 1,),
        in_specs=[
            pl.BlockSpec((parts, rows, depth), lambda s: (0, 0, 0)),
            pl.BlockSpec((1, parts, rows, wide), source),
        ]
        + [pl.BlockSpec(memory_space=pltpu.HBM)] * len(into),
        out_specs=[spec, spec],
        scratch_shapes=[
            pltpu.VMEM((depth, rows), f32),
            pltpu.VMEM((parts, depth, rows), bf16),
            pltpu.VMEM((2, depth // 2, wide), bf16),
            pltpu.VMEM((2, depth // 2, wide), f32),
            pltpu.VMEM((steps, depth // 2, wide), bf16),
            pltpu.SemaphoreType.DMA((steps,)),
            pltpu.SemaphoreType.DMA((steps,)),
        ],
        out_shape=[shape, shape],
        input_output_aliases={2 + i: i for i in range(len(into))},
        compiler_params=pltpu.CompilerParams(
            dimension_semantics=("arbitrary",),
            vmem_limit_bytes=VMEM,
            collective_id=number,
            has_side_effects=True,
        ),
        name="weight_grad",
        cost_estimate=cost(3 * kinds * parts),
    )(left, right, *into)


def norm_grad_kernel(d_ref, w_ref, unit, inverse, gain, g_ref, *refs):
    *then, total = refs
    then_w, out, low, gain_out, then_out = then if len(then) == 5 else (None, *then, None)
    step = pl.program_id(0)
    kinds, _, width = d_ref.shape
    part = product_t(d_ref[0], w_ref[:, :width])
    for kind in range(1, kinds):
        part += product_t(d_ref[kind], w_ref[:, kind * width : (kind + 1) * width])
    wide = part.shape[1]
    total[:, pl.ds(pl.multiple_of(step * wide, wide), wide)] = part

    @pl.when(step == pl.num_programs(0) - 1)
    def _():
        change, gain_grad = norm_back(unit[...], inverse[...], gain[...], total[...])
        result = g_ref[...] + change
        out[...] = result
        low[...] = result.astype(bf16)
        gain_out[...] = gain_grad[None, :]
        if then_w is not None:
            then_out[...] = product_t(low[...], then_w[...]).astype(bf16)


def norm_grad(grads, weights, first, unit, inverse, gain, g, then=False):
    kinds, rows, width = grads.shape
    wide = 256

    def whole(shape):
        return pl.BlockSpec(shape, lambda j: (0,) * len(shape))

    return pl.pallas_call(
        norm_grad_kernel,
        grid=(width // wide,),
        in_specs=[
            whole((kinds, rows, width)),
            pl.BlockSpec((wide, kinds * width), lambda j: (j, first)),
            whole((rows, width)), whole((rows, 1)), whole((1, width)), whole((rows, width)),
            *[whole((width, width))] * then,
        ],
        out_specs=[whole((rows, width)), whole((rows, width)), whole((1, width))]
        + [whole((rows, width))] * then,
        out_shape=[
            jax.ShapeDtypeStruct((rows, width), f32),
            jax.ShapeDtypeStruct((rows, width), bf16),
            jax.ShapeDtypeStruct((1, width), f32),
            *[jax.ShapeDtypeStruct((rows, width), bf16)] * then,
        ],
        scratch_shapes=[pltpu.VMEM((rows, width), f32)],
        compiler_params=params(1),
        name="norm_grad",
        cost_estimate=cost(4 * kinds),
    )(grads, weights, unit, inverse, gain, g, *[weights] * then)


def feed_kernel(
    devices, lanes, ways, x_ref, mixed_ref, w_ref, g_ref, gain_ref, up_ref, down_ref,
    out, gx, low_gx, grad_mixed, ggain, up_out, up_keep, down_out, down_keep,
    unit, inverse, hidden, staged, flipped, total, back,
    up_sent, up_own, up_came, down_sent, down_own, down_came,
    up_send_sem, up_recv_sem, down_send_sem, down_recv_sem,
):
    step, groups = pl.program_id(0), pl.num_programs(0) - 1
    me = here(lanes)
    partner = other_core(me, lanes)
    core, low, high = (me // lanes) % 2, me % lanes, me // (2 * lanes)

    @pl.when(step == 0)
    def _():
        greet(partner)
        x = x_ref[...] + product(mixed_ref[...], w_ref[...])
        h, u, i = normed(x, gain_ref[...])
        unit[...] = u
        inverse[...] = i
        hidden[...] = h.astype(bf16)
        put_rows(me, devices, lanes, ways[0], h, staged)
        flipped[...] = staged[...].astype(bf16)
        total[...] = x
        back[...] = jnp.zeros_like(back)

    def up_copy(at):
        return to_core(partner, up_sent.at[at % 2], up_came.at[at], up_send_sem.at[at], up_recv_sem.at[at])

    def down_copy(at):
        return to_core(partner, down_sent, down_came.at[at], down_send_sem.at[at], down_recv_sem.at[at])

    @pl.when(step < groups)
    def _():
        g = g_ref[...]
        up = up_ref[...].reshape(-1, up_ref.shape[-1])
        down = down_ref[...].reshape(-1, down_ref.shape[-1])
        inner = product(hidden[...], up)
        share = 0.5 + 0.5 * lax.erf(inner * (0.5**0.5))
        slope = share + inner * (jnp.exp(-0.5 * inner * inner) * 0.3989422804014327)
        active = (inner * share).astype(bf16)
        change = (product_t(g, down) * slope).astype(bf16)
        half = flipped.shape[0] // 2
        up_sent[step % 2] = product(flipped[:half, :], change).astype(bf16)
        grad_down = product_rows(active, g)

        @pl.when(step % 2 != core)
        def _():
            down_sent[...] = grad_down.astype(bf16)

        @pl.when(step % 2 == core)
        def _():
            down_own[...] = grad_down

        up_own[step % 2] = product(flipped[half:, :], change)
        total[...] += product(active, down)
        back[...] += product_t(change, up)
        up_copy(step).start()

        @pl.when(step % 2 != core)
        def _():
            down_copy(step // 2).start()

    @pl.when(step == groups)
    def _():
        out[...] = total[...].astype(bf16)
        gx_norm, gain_grad = norm_back(unit[...], inverse[...], gain_ref[...], back[...])
        result = g_ref[...].astype(f32) + gx_norm
        gx[...] = result
        low_gx[...] = result.astype(bf16)
        grad_mixed[...] = product_t(low_gx[...], w_ref[...]).astype(bf16)
        ggain[...] = gain_grad[None, :]

    @pl.when(step > 0)
    def _():
        before = step - 1
        up_copy(before).wait()
        put_halves(up_own[before % 2] + up_came[before].astype(f32), up_out, up_keep)

        @pl.when(before % 2 != core)
        def _():
            down_copy(before // 2).wait_send()

        @pl.when(before % 2 == core)
        def _():
            down_copy(before // 2).wait_recv()
            sums = down_own[...] + down_came[before // 2].astype(f32)
            depth = sums.shape[0] // lanes
            for block in range(lanes):
                relative = (block ^ low) + 2 * lanes * ((before // 2) ^ high)
                place = place_of(relative, devices, lanes, ways[1])
                piece = sums[block * depth : (block + 1) * depth, :].astype(bf16)
                goes = bit_of(relative, ways[1][0]) == 1

                @pl.when(goes)
                def _(place=place, piece=piece):
                    down_out[place] = piece

                @pl.when(jnp.logical_not(goes))
                def _(place=place, piece=piece):
                    down_keep[place] = piece


def feed(number, devices, lanes, ways, x, mixed, projection, g, gain, weights):
    rows, width = x.shape
    pieces, depth = weights.shape[2:4]
    hidden = pieces * width
    groups = devices // lanes
    tile = hidden // groups
    across = width // tile

    def group(s):
        return jnp.minimum(s, groups - 1)

    def whole(shape):
        return pl.BlockSpec(shape, lambda s: (0,) * len(shape), pipeline_mode=pl.Buffered(1))

    last = projection.shape[1] // width - 1
    up_block = pl.BlockSpec((devices // 4, depth, tile), lambda s: (0, 0, jnp.maximum(s - 1, 0)))
    up_shape = jax.ShapeDtypeStruct((devices // 4, depth, hidden), bf16)
    down_shape = jax.ShapeDtypeStruct((devices // 4, hidden // devices, width), bf16)
    return pl.pallas_call(
        functools.partial(feed_kernel, devices, lanes, ways),
        grid=(groups + 1,),
        in_specs=[
            whole((rows, width)),
            whole((rows, width)),
            pl.BlockSpec((width, width), lambda s: (0, last), pipeline_mode=pl.Buffered(1)),
            whole((rows, width)),
            whole((1, width)),
            pl.BlockSpec(
                (devices, None, None, depth, tile),
                lambda s: (0, 0, group(s) // across, 0, group(s) % across),
            ),
            pl.BlockSpec((lanes, None, pieces, depth, width), lambda s: (group(s), 1, 0, 0, 0)),
        ],
        out_specs=[
            *[whole((rows, width))] * 4, whole((1, width)),
            up_block, up_block, whole(down_shape.shape), whole(down_shape.shape),
        ],
        scratch_shapes=[
            pltpu.VMEM((rows, width), f32),
            pltpu.VMEM((rows, 1), f32),
            pltpu.VMEM((rows, width), bf16),
            pltpu.VMEM((width, rows), f32),
            pltpu.VMEM((width, rows), bf16),
            pltpu.VMEM((rows, width), f32),
            pltpu.VMEM((rows, width), f32),
            pltpu.VMEM((2, width // 2, tile), bf16),
            pltpu.VMEM((2, width // 2, tile), f32),
            pltpu.VMEM((groups, width // 2, tile), bf16),
            pltpu.VMEM((tile, width), bf16),
            pltpu.VMEM((tile, width), f32),
            pltpu.VMEM((groups // 2, tile, width), bf16),
            pltpu.SemaphoreType.DMA((groups,)),
            pltpu.SemaphoreType.DMA((groups,)),
            pltpu.SemaphoreType.DMA((groups // 2,)),
            pltpu.SemaphoreType.DMA((groups // 2,)),
        ],
        out_shape=[
            jax.ShapeDtypeStruct((rows, width), bf16),
            jax.ShapeDtypeStruct((rows, width), f32),
            jax.ShapeDtypeStruct((rows, width), bf16),
            jax.ShapeDtypeStruct((rows, width), bf16),
            jax.ShapeDtypeStruct((1, width), f32),
            up_shape, up_shape, down_shape, down_shape,
        ],
        compiler_params=pltpu.CompilerParams(
            dimension_semantics=("arbitrary",),
            vmem_limit_bytes=VMEM,
            collective_id=number,
            has_side_effects=True,
        ),
        name="feed",
        cost_estimate=cost(40),
    )(x, mixed, projection, g, gain, weights, weights)


def gather_kernel(devices, lanes, tracks, x_ref, out, own_sem, send_sem, recv_sem):
    me = lax.axis_index("dp") * lanes + lax.axis_index("fsdp")
    count = devices // 2

    def device(bit):
        other = me ^ bit
        return (other // lanes, lax.rem(other, lanes))

    barrier = pltpu.get_barrier_semaphore()
    every = [1 << b for b in range(devices.bit_length() - 1)]
    for bit in every:
        pl.semaphore_signal(
            barrier, inc=1, device_id=device(bit), device_id_type=pl.DeviceIdType.MESH
        )
    pl.semaphore_wait(barrier, len(every))
    own = pltpu.make_async_copy(x_ref, out.at[me], own_sem)
    own.start()
    sends = []

    def block(track, number, to_core):
        low, high, bits = tracks[track]
        owner = me ^ sum(b for p, b in enumerate(bits) if (number >> p) & 1)
        return out.at[owner ^ lanes if to_core else owner, :, low:high]

    def arrived(track, number):
        to_core = number >= count
        here = block(track, number - count if to_core else number, to_core)
        pltpu.make_async_remote_copy(
            src_ref=here,
            dst_ref=here,
            send_sem=send_sem.at[0],
            recv_sem=recv_sem.at[track, number],
            device_id=device(lanes),
            device_id_type=pl.DeviceIdType.MESH,
        ).wait_recv()
        return here

    for number in sorted(range(count), key=lambda k: (bin(k).count("1"), k)):
        for track, (low, high, bits) in enumerate(tracks):
            there = block(track, number, False)
            here = arrived(track, number) if number else x_ref.at[:, low:high]
            for place, bit in enumerate(bits + (lanes,)):
                if number >> place == 0 or bit == lanes:
                    copy = pltpu.make_async_remote_copy(
                        src_ref=here,
                        dst_ref=there,
                        send_sem=send_sem.at[len(sends)],
                        recv_sem=recv_sem.at[track, number + (1 << place)],
                        device_id=device(bit),
                        device_id_type=pl.DeviceIdType.MESH,
                    )
                    copy.start()
                    sends.append(copy)
    for number in range(count, devices):
        for track in range(len(tracks)):
            arrived(track, number)
    for copy in sends:
        copy.wait_send()
    own.wait()


def gather(number, devices, lanes, values):
    depth, columns = values.shape
    middle = (columns // 256) * 128
    high = tuple(2 * lanes << b for b in range((devices // (2 * lanes)).bit_length() - 1))
    links = [high + tuple(1 << b for b in way) for way in orders(lanes)]
    tracks = ((0, middle, links[0]), (middle, columns, links[1]))
    return pl.pallas_call(
        functools.partial(gather_kernel, devices, lanes, tracks),
        in_specs=[pl.BlockSpec(memory_space=pltpu.VMEM)],
        out_specs=pl.BlockSpec(memory_space=pltpu.HBM),
        out_shape=jax.ShapeDtypeStruct((devices, depth, columns), values.dtype),
        scratch_shapes=[
            pltpu.SemaphoreType.DMA,
            pltpu.SemaphoreType.DMA((len(tracks) * (devices - 1),)),
            pltpu.SemaphoreType.DMA((len(tracks), devices)),
        ],
        compiler_params=pltpu.CompilerParams(collective_id=number, has_side_effects=True),
        name="gather",
        cost_estimate=cost(40),
    )(values).reshape(-1, columns)


def swap(values, devices, bit):
    return lax.ppermute(values, AXES, [(i, i ^ bit) for i in range(devices)])


def plus(a, b):
    return (a.astype(f32) + b.astype(f32)).astype(bf16)


def owner_sums(halves, devices, lanes, way, late=None):
    bits = stages(devices, lanes, way)
    out, keep = halves
    for stage, bit in enumerate(bits):
        arrived = swap(out, devices, 1 << bit)
        if stage == len(bits) - 1:
            return keep[0].astype(f32) + arrived[0].astype(f32)
        half = keep.shape[0] // 2
        out, keep = plus(keep[half:], arrived[half:]), plus(keep[:half], arrived[:half])
        if stage == 0 and late is not None:
            late_out, late_keep = late
            late_arrived = swap(late_out, devices, 1 << bit)
            out = jnp.concatenate([out, plus(late_keep[half:], late_arrived[half:])], axis=-1)
            keep = jnp.concatenate([keep, plus(late_keep[:half], late_arrived[:half])], axis=-1)


def gain_halves(values, devices, lanes, way, me):
    kinds, depth = values.shape
    blocks = jnp.pad(values.T, ((0, 0), (0, 128 - kinds))).astype(bf16)
    every = range(devices)
    core = lanes.bit_length() - 1
    order = sorted(every, key=lambda r: (1 - bit_of(r, core), 1 - bit_of(r, way[0]), place_of(r, devices, lanes, way)))
    blocks = blocks.reshape(devices, depth // devices, 128)[jnp.array(order) ^ me]
    arrived = swap(blocks[: devices // 2], devices, lanes)
    sums = plus(blocks[devices // 2 :], arrived)
    return sums[: devices // 4], sums[devices // 4 :]


def after(values, first):
    return lax.optimization_barrier((values, first))[0]


def orders(lanes):
    low = list(range(lanes.bit_length() - 1))
    return low, low[::-1]


def shards(devices, lanes, tokens, images, segment_ids, image_map, out_grad, norm_self, attn_query,
           attn_key, attn_value, attn_out, norm_cross, cross_query, cross_key, cross_value, cross_out,
           norm_ffn, ffn_up, ffn_down):
    me = lax.axis_index("dp") * lanes + lax.axis_index("fsdp")
    me_ref = me.astype(jnp.int32)[None]
    depth, width = attn_query.shape
    gains = jnp.stack([norm_self, norm_cross, norm_ffn], axis=1)
    gains = jnp.pad(gains, ((0, 0), (0, 128 - 3)))
    first_set = jnp.concatenate([attn_query, attn_key, attn_value, cross_key, cross_value, gains], axis=1)
    second_set = jnp.concatenate([attn_out, cross_query, cross_out], axis=1)
    pieces = ffn_up.shape[1] // width
    feed_set = jnp.stack(
        [ffn_up.reshape(depth, pieces, width).transpose(1, 0, 2), ffn_down.reshape(pieces, depth, width)]
    )
    first_set = gather(0, devices, lanes, first_set)
    feed_set = lax.all_gather(after(feed_set, first_set), AXES, axis=0)
    w_qkv = first_set[:, : 3 * width]
    w_kv = first_set[:, 3 * width : 5 * width]
    (count, order, page_column, page_row, inputs, grad_out, hidden_one, unit_one, inverse_one, *gains) = arrange(
        image_map[0], segment_ids[0], tokens[0], out_grad[0], first_set, 5 * width // 128
    )
    qkv = product(hidden_one, w_qkv).astype(bf16)
    mixed_one, log_one = self_forward(page_column, page_row, qkv)
    kv = lax.dot_general(images, w_kv, (((2,), (0,)), ((), ())), preferred_element_type=f32).astype(bf16)
    second_set = gather(1, devices, lanes, after(second_set, (mixed_one, kv)))
    after_self, hidden_two, unit_two, inverse_two, query_two = between(inputs, mixed_one, second_set, gains[1])
    mixed_two, log_two = cross_forward(count, query_two, kv)

    one_way, other_way = orders(lanes)
    (output, grad_after_cross, branch_two, grad_mixed_two, grad_gain_ffn, *halves) = feed(
        2, devices, lanes, (one_way, other_way), after_self, mixed_two, second_set, grad_out, gains[2], feed_set
    )

    def sums(way, halves, late=None):
        return owner_sums(halves, devices, lanes, way, late)

    def halves_of(number, way, left, right, **options):
        return weight_grad(number, devices, lanes, way, left, right, 2 * width, **options)

    grad_up = sums(one_way, halves[:2])
    grad_down = sums(other_way, halves[2:])

    grad_query_two, grad_kv = cross_backward(count, query_two, kv, grad_mixed_two, log_two)
    halves = halves_of(3, one_way, mixed_two[None], after(branch_two, grad_kv)[None, None])
    halves = halves_of(4, one_way, hidden_two[None], grad_query_two[None, None], first=width, into=halves)
    grad_c = sums(one_way, halves)
    halves = halves_of(5, other_way, images, after(grad_kv, halves[0]))
    grad_d = sums(other_way, halves)
    grad_query_again = after(grad_query_two, halves[0])[None]
    grad_after_self, branch_one, grad_gain_cross, grad_mixed_one = norm_grad(
        grad_query_again, second_set, 1, unit_two, inverse_two, gains[1], grad_after_cross, then=True
    )
    grad_qkv = self_backward(page_column, page_row, qkv, grad_mixed_one, log_one)
    halves = halves_of(6, one_way, mixed_one[None], after(branch_one, grad_qkv)[None, None])
    options = dict(first=width, into=halves, only=(0, 1))
    halves = halves_of(7, one_way, hidden_one[None], grad_qkv[:, None], **options)
    grad_qkv_again = after(grad_qkv, halves[0])
    halves_kv = halves_of(8, one_way, hidden_one[None], grad_qkv_again[:, None], only=(1, 3))
    grad_qkv_again = after(grad_qkv, halves_kv[0])
    _, grad_inputs, grad_gain_self = norm_grad(
        grad_qkv_again, first_set, 0, unit_one, inverse_one, gains[0], grad_after_self
    )
    gain_grads = jnp.concatenate([grad_gain_self, grad_gain_cross, grad_gain_ffn])
    late = gain_halves(gain_grads, devices, lanes, one_way, me)
    grad_a = sums(one_way, halves)
    grad_b = sums(one_way, halves_kv, late)
    gain_sums = grad_b[:, 2 * width :]

    grad_kv = after(grad_kv, late[0])
    back = (((2,), (1,)), ((), ()))
    grad_images = lax.dot_general(grad_kv[0], w_kv[:, :width], back, preferred_element_type=f32)
    grad_images += lax.dot_general(grad_kv[1], w_kv[:, width:], back, preferred_element_type=f32)
    output = product_rows(order, output).astype(bf16)
    grad_inputs = product_rows(order, grad_inputs).astype(bf16)
    return (
        output[None],
        grad_inputs[None],
        grad_images.astype(bf16),
        gain_sums[:, 0],
        grad_a[:, width:],
        grad_b[:, :width],
        grad_b[:, width : 2 * width],
        grad_a[:, :width],
        gain_sums[:, 1],
        grad_c[:, width:],
        grad_d[:, :width],
        grad_d[:, width:],
        grad_c[:, :width],
        gain_sums[:, 2],
        grad_up,
        grad_down,
    )


def solution(mesh):
    rows = P(AXES)
    devices, lanes = mesh.shape["dp"] * mesh.shape["fsdp"], mesh.shape["fsdp"]
    return jax.shard_map(
        functools.partial(shards, devices, lanes),
        mesh=mesh,
        in_specs=(rows,) * 18,
        out_specs=(rows,) * 16,
        check_vma=False,
    )
```

```python
import functools

import jax
import jax.numpy as jnp
from jax import lax
from jax.experimental import pallas as pl
from jax.experimental.pallas import tpu as pltpu
from jax.sharding import PartitionSpec as P


AXES = ("dp", "fsdp")
LOG2E = 1.4426950408889634
EPSILON = 1e-05
MASKED = -1e30
TILE = 128
PAGE_MAX = 256
VMEM = 62 * 1024 * 1024

bf16 = jnp.bfloat16
f32 = jnp.float32


def product(left, right):
    return jnp.dot(left, right, preferred_element_type=f32)


def product_t(left, right):
    return lax.dot_general(left, right, (((1,), (1,)), ((), ())), preferred_element_type=f32)


def product_rows(left, right):
    return lax.dot_general(left, right, (((0,), (0,)), ((), ())), preferred_element_type=f32)


def normed(values, gain):
    centred = values - jnp.mean(values, axis=-1, keepdims=True)
    variance = jnp.mean(centred * centred, axis=-1, keepdims=True)
    inverse = lax.rsqrt(variance + EPSILON)
    unit = centred * inverse
    return unit * gain, unit, inverse


def norm_back(unit, inverse, gain, gradient):
    scaled = gradient * gain
    mean_scaled = jnp.mean(scaled, axis=-1, keepdims=True)
    mean_along = jnp.mean(scaled * unit, axis=-1, keepdims=True)
    return inverse * (scaled - mean_scaled - unit * mean_along), jnp.sum(gradient * unit, axis=0)


def params(count):
    return pltpu.CompilerParams(
        dimension_semantics=("arbitrary",) * count, vmem_limit_bytes=VMEM
    )


def cost(microseconds):
    return pl.CostEstimate(flops=int(microseconds * 1e9), bytes_accessed=0, transcendentals=0)


def two_heads(block):
    lane = lax.broadcasted_iota(jnp.int32, block.shape, 1)
    zero = jnp.zeros_like(block)
    half = block.shape[1] // 2
    return jnp.concatenate(
        [jnp.where(lane < half, block, zero), jnp.where(lane >= half, block, zero)], axis=0
    )


def join_heads(both):
    rows = both.shape[1] // 2
    feature = lax.broadcasted_iota(jnp.int32, (both.shape[0], rows), 0)
    return jnp.where(feature < both.shape[0] // 2, both[:, :rows], both[:, rows:]).T


def twice(row):
    return jnp.concatenate([row, row], axis=1)


def arrange_kernel(
    map_ref, page_column, page_row, tokens, g, columns,
    count, order, new_column, new_row, inputs, new_g, hidden, unit, inverse, *gains,
):
    rows = tokens.shape[0]

    def second_of(pages):
        return sum(jnp.where(pages == p, map_ref[p], 0) for p in range(map_ref.shape[0])).astype(f32)

    column, row = second_of(page_column[...]), second_of(page_row[...])
    i = lax.broadcasted_iota(jnp.int32, (rows, rows), 0)
    j = lax.broadcasted_iota(jnp.int32, (rows, rows), 1)
    before_column = jnp.sum(jnp.where(j < i, row, 0.0), axis=1, keepdims=True)
    before_row = jnp.sum(jnp.where(i < j, column, 0.0), axis=0, keepdims=True)
    first = rows - jnp.sum(row)
    count[0] = first.astype(jnp.int32)
    at_column = lax.broadcasted_iota(jnp.int32, (rows, 1), 0).astype(f32)
    at_row = lax.broadcasted_iota(jnp.int32, (1, rows), 1).astype(f32)
    place_column = jnp.where(column > 0, first + before_column, at_column - before_column)
    place_row = jnp.where(row > 0, first + before_row, at_row - before_row)
    moved = i.astype(f32) == place_row
    order[...] = moved.astype(f32).astype(bf16)
    pages = page_row[...].astype(f32)
    new_column[...] = jnp.sum(jnp.where(moved, pages, 0.0), axis=1, keepdims=True).astype(jnp.int32)
    pages = page_column[...].astype(f32)
    back = place_column == j.astype(f32)
    new_row[...] = jnp.sum(jnp.where(back, pages, 0.0), axis=0, keepdims=True).astype(jnp.int32)
    new_g[...] = product(order[...], g[...]).astype(bf16)
    flat = columns[...].astype(f32).T
    for number, gain in enumerate(gains):
        gain[...] = flat[number : number + 1, :]
    inputs[...] = product(order[...], tokens[...])
    h, unit[...], inverse[...] = normed(inputs[...], gains[0][...])
    hidden[...] = h.astype(bf16)


def arrange(image_map, pages, tokens, g, weights, first):
    rows, width = tokens.shape

    def whole(*shape):
        return pl.BlockSpec(shape, lambda s: (0,) * len(shape))

    scalars = pl.BlockSpec(memory_space=pltpu.SMEM)
    kinds = [
        ((rows, rows), bf16), ((rows, 1), jnp.int32), ((1, rows), jnp.int32),
        ((rows, width), f32), ((rows, width), bf16), ((rows, width), bf16),
        ((rows, width), f32), ((rows, 1), f32), *[((1, width), f32)] * 3,
    ]
    return pl.pallas_call(
        arrange_kernel,
        grid=(1,),
        in_specs=[
            scalars, whole(rows, 1), whole(1, rows), whole(rows, width), whole(rows, width),
            pl.BlockSpec((width, 128), lambda s: (0, first)),
        ],
        out_specs=[scalars] + [whole(*shape) for shape, _ in kinds],
        out_shape=[jax.ShapeDtypeStruct((1,), jnp.int32)]
        + [jax.ShapeDtypeStruct(shape, dtype) for shape, dtype in kinds],
        compiler_params=params(1),
        name="arrange",
        cost_estimate=cost(6),
    )(image_map, pages[:, None], pages[None, :], tokens, g, weights)


def between_kernel(x_ref, mixed, w_out, w_query, gain, x_out, hidden, unit, inverse, query):
    x = x_ref[...] + product(mixed[...], w_out[...])
    x_out[...] = x
    h, unit[...], inverse[...] = normed(x, gain[...])
    hidden[...] = h.astype(bf16)
    query[...] = product(hidden[...], w_query[...]).astype(bf16)


def between(x, mixed, weights, gain):
    rows, width = x.shape
    tile = rows // 2

    def part(columns):
        return pl.BlockSpec((tile, columns), lambda s: (s, 0))

    kinds = ((width, f32), (width, bf16), (width, f32), (1, f32), (width, bf16))
    return pl.pallas_call(
        between_kernel,
        grid=(2,),
        in_specs=[
            part(width), part(width),
            pl.BlockSpec((width, width), lambda s: (0, 0)),
            pl.BlockSpec((width, width), lambda s: (0, 1)),
            pl.BlockSpec((1, width), lambda s: (0, 0)),
        ],
        out_specs=[part(columns) for columns, _ in kinds],
        out_shape=[jax.ShapeDtypeStruct((rows, columns), dtype) for columns, dtype in kinds],
        compiler_params=params(1),
        name="between",
        cost_estimate=cost(8),
    )(x, mixed, weights, weights, gain)


def key_range(tile):
    return max(0, tile * TILE - PAGE_MAX), (tile + 1) * TILE


def fill_bias(page_column, page_row, bias, tiles):
    for tile in range(tiles):
        low, high = key_range(tile)
        keys = low + lax.broadcasted_iota(jnp.int32, (high - low, TILE), 0)
        queries = tile * TILE + lax.broadcasted_iota(jnp.int32, (high - low, TILE), 1)
        same = page_column[low:high, :] == page_row[:, tile * TILE : (tile + 1) * TILE]
        bias[tile, : high - low, :] = jnp.where((keys <= queries) & same, 0.0, MASKED)


def attend_pair(q, k, v, out, totals, bias):
    tiles = q.shape[0] // TILE
    scale = LOG2E * (q.shape[1] // 2) ** (-0.5)
    for tile in range(tiles):
        low, high = key_range(tile)
        at = slice(tile * TILE, (tile + 1) * TILE)
        scores = product_t(k[low:high, :], two_heads(q[at, :])) * scale + twice(
            bias[tile, : high - low, :]
        )
        highest = jnp.max(scores, axis=0, keepdims=True)
        weights = jnp.exp2(scores - highest)
        total = jnp.sum(weights, axis=0, keepdims=True)
        mixed = product_rows(v[low:high, :], weights.astype(bf16)) * (1.0 / total)
        out[at, :] = join_heads(mixed).astype(bf16)
        level = highest + jnp.log2(total)
        totals[0, 0:1, at] = level[:, :TILE]
        totals[0, 1:2, at] = level[:, TILE:]


def self_backward_kernel(page_column, page_row, q, k, v, g, totals, out, bias, dk, dv):
    tiles = q.shape[0] // TILE
    half_scale = (q.shape[1] // 2) ** (-0.5)
    scale = LOG2E * half_scale

    @pl.when(pl.program_id(0) == 0)
    def _():
        fill_bias(page_column, page_row, bias, tiles)

    dk[...] = jnp.zeros_like(dk)
    dv[...] = jnp.zeros_like(dv)
    for tile in range(tiles):
        low, high = key_range(tile)
        here = slice(tile * TILE, (tile + 1) * TILE)
        queries, grads = two_heads(q[here, :]), two_heads(g[here, :])
        keys, values = k[low:high, :], v[low:high, :]
        level = jnp.concatenate([totals[0, 0:1, here], totals[0, 1:2, here]], axis=1)
        weights = jnp.exp2(
            product_t(keys, queries) * scale + twice(bias[tile, : high - low, :]) - level
        )
        along = weights * product_t(values, grads)
        change = (along - weights * jnp.sum(along, axis=0, keepdims=True)).astype(bf16)
        dv[low:high, :] += product(weights.astype(bf16), grads)
        dk[low:high, :] += product(change, queries)
        out[0, here, :] = (join_heads(product_rows(keys, change)) * half_scale).astype(bf16)
    out[1] = (dk[...] * half_scale).astype(bf16)
    out[2] = dv[...].astype(bf16)


def self_backward(page_column, page_row, qkv, grads, totals):
    rows, width = grads.shape
    pairs = width // 128
    return pl.pallas_call(
        self_backward_kernel,
        grid=(pairs,),
        in_specs=[
            pl.BlockSpec((rows, 1), lambda j: (0, 0)),
            pl.BlockSpec((1, rows), lambda j: (0, 0)),
            *[pl.BlockSpec((rows, 128), lambda j: (0, j))] * 4,
            pl.BlockSpec((1, 2, rows), lambda j: (j, 0, 0)),
        ],
        out_specs=pl.BlockSpec((3, rows, 128), lambda j: (0, 0, j)),
        out_shape=jax.ShapeDtypeStruct((3, rows, width), bf16),
        scratch_shapes=[
            pltpu.VMEM((rows // TILE, PAGE_MAX + TILE, TILE), f32),
            pltpu.VMEM((rows, 128), f32),
            pltpu.VMEM((rows, 128), f32),
        ],
        compiler_params=params(1),
        name="self_backward",
        cost_estimate=cost(15),
    )(page_column, page_row, *qkv, grads, totals)


def cross_steps(count, tiles):
    first = (count + TILE - 1) // TILE
    skip = count // TILE
    return first, skip, first + tiles - skip


def cross_step(step, first, skip):
    image = jnp.where(step < first, 0, 1)
    tile = jnp.where(step < first, step, step - first + skip)
    return image, pl.multiple_of(tile * TILE, TILE)


def cross_forward_kernel(count_ref, q, k, v, out, totals):
    scale = LOG2E * (q.shape[1] // 2) ** (-0.5)
    count = count_ref[0]
    first, skip, steps = cross_steps(count, q.shape[0] // TILE)

    def one(step, carry):
        image, start = cross_step(step, first, skip)
        here = pl.ds(start, TILE)
        scores = product_t(k[image], two_heads(q[here, :])) * scale
        highest = jnp.max(scores, axis=0, keepdims=True)
        weights = jnp.exp2(scores - highest)
        total = jnp.sum(weights, axis=0, keepdims=True)
        mixed = product_rows(v[image], weights.astype(bf16)) * (1.0 / total)
        row = start + lax.broadcasted_iota(jnp.int32, (TILE, 128), 0)
        mine = (row >= count) == (image == 1)
        out[here, :] = jnp.where(mine, join_heads(mixed), out[here, :].astype(f32)).astype(bf16)
        level = highest + jnp.log2(total)
        lane = start + lax.broadcasted_iota(jnp.int32, (1, TILE), 1)
        mine = (lane >= count) == (image == 1)
        totals[0, 0:1, here] = jnp.where(mine, level[:, :TILE], totals[0, 0:1, here])
        totals[0, 1:2, here] = jnp.where(mine, level[:, TILE:], totals[0, 1:2, here])
        return carry

    lax.fori_loop(0, steps, one, 0)


def cross_forward(count, query, kv):
    rows, width = query.shape
    pairs = width // 128
    images, length = kv.shape[:2]
    return pl.pallas_call(
        cross_forward_kernel,
        grid_spec=pltpu.PrefetchScalarGridSpec(
            num_scalar_prefetch=1,
            grid=(pairs,),
            in_specs=[
                pl.BlockSpec((rows, 128), lambda j, c: (0, j)),
                pl.BlockSpec((images, length, 128), lambda j, c: (0, 0, j)),
                pl.BlockSpec((images, length, 128), lambda j, c: (0, 0, pairs + j)),
            ],
            out_specs=[
                pl.BlockSpec((rows, 128), lambda j, c: (0, j)),
                pl.BlockSpec((1, 2, rows), lambda j, c: (j, 0, 0)),
            ],
        ),
        out_shape=[
            jax.ShapeDtypeStruct((rows, width), bf16),
            jax.ShapeDtypeStruct((pairs, 2, rows), f32),
        ],
        compiler_params=params(1),
        name="cross_forward",
        cost_estimate=cost(24),
    )(count, query, kv, kv)


def cross_backward_kernel(count_ref, q, k, v, g, totals, dq_out, dkv_out, dq, dk, dv):
    half_scale = (q.shape[1] // 2) ** (-0.5)
    scale = LOG2E * half_scale
    count = count_ref[0]
    first, skip, steps = cross_steps(count, q.shape[0] // TILE)
    dq[...] = jnp.zeros_like(dq)
    dk[...] = jnp.zeros_like(dk)
    dv[...] = jnp.zeros_like(dv)

    def one(step, carry):
        image, start = cross_step(step, first, skip)
        here = pl.ds(start, TILE)
        queries, grads = two_heads(q[here, :]), two_heads(g[here, :])
        lane = start + lax.broadcasted_iota(jnp.int32, (1, TILE), 1)
        mine = (lane >= count) == (image == 1)
        level = jnp.concatenate(
            [
                jnp.where(mine, totals[0, 0:1, here], -MASKED),
                jnp.where(mine, totals[0, 1:2, here], -MASKED),
            ],
            axis=1,
        )
        weights = jnp.exp2(product_t(k[image], queries) * scale - level)
        along = weights * product_t(v[image], grads)
        change = (along - weights * jnp.sum(along, axis=0, keepdims=True)).astype(bf16)
        dv[image] += product(weights.astype(bf16), grads)
        dk[image] += product(change, queries)
        dq[here, :] += join_heads(product_rows(k[image], change))
        return carry

    lax.fori_loop(0, steps, one, 0)
    dq_out[...] = (dq[...] * half_scale).astype(bf16)
    dkv_out[0] = (dk[...] * half_scale).astype(bf16)
    dkv_out[1] = dv[...].astype(bf16)


def cross_backward(count, query, kv, grads, totals):
    rows, width = query.shape
    pairs = width // 128
    images, length = kv.shape[:2]
    return pl.pallas_call(
        cross_backward_kernel,
        grid_spec=pltpu.PrefetchScalarGridSpec(
            num_scalar_prefetch=1,
            grid=(pairs,),
            in_specs=[
                pl.BlockSpec((rows, 128), lambda j, c: (0, j)),
                pl.BlockSpec((images, length, 128), lambda j, c: (0, 0, j)),
                pl.BlockSpec((images, length, 128), lambda j, c: (0, 0, pairs + j)),
                pl.BlockSpec((rows, 128), lambda j, c: (0, j)),
                pl.BlockSpec((1, 2, rows), lambda j, c: (j, 0, 0)),
            ],
            out_specs=[
                pl.BlockSpec((rows, 128), lambda j, c: (0, j)),
                pl.BlockSpec((2, images, length, 128), lambda j, c: (0, 0, 0, j)),
            ],
            scratch_shapes=[
                pltpu.VMEM((rows, 128), f32),
                pltpu.VMEM((images, length, 128), f32),
                pltpu.VMEM((images, length, 128), f32),
            ],
        ),
        out_shape=[
            jax.ShapeDtypeStruct((rows, width), bf16),
            jax.ShapeDtypeStruct((2, images, length, width), bf16),
        ],
        compiler_params=params(1),
        name="cross_backward",
        cost_estimate=cost(28),
    )(count, query, kv, kv, grads, totals)


def here(lanes):
    return lax.axis_index("dp") * lanes + lax.axis_index("fsdp")


def bit_of(number, bit):
    return (number // (1 << bit)) % 2


def stages(devices, lanes, way):
    return list(way) + list(range(lanes.bit_length(), devices.bit_length() - 1))


def place_of(relative, devices, lanes, way):
    place = 0
    for bit in stages(devices, lanes, way)[1:]:
        place = place * 2 + bit_of(relative, bit)
    return place


def put_rows(me, devices, lanes, way, left, staged):
    flipped = left.astype(f32).T
    depth = flipped.shape[0] // devices
    for block in range(devices):
        relative = block ^ me
        quarter = 2 * (1 - bit_of(relative, lanes.bit_length() - 1)) + (1 - bit_of(relative, way[0]))
        place = quarter * (devices // 4) + place_of(relative, devices, lanes, way)
        start = pl.multiple_of(place * depth, depth)
        staged[pl.ds(start, depth), :] = flipped[block * depth : (block + 1) * depth, :]


def greet(partner):
    barrier = pltpu.get_barrier_semaphore()
    pl.semaphore_signal(barrier, inc=1, device_id=partner, device_id_type=pl.DeviceIdType.MESH)
    pl.semaphore_wait(barrier, 1)


def other_core(me, lanes):
    other = me ^ lanes
    return (other // lanes, lax.rem(other, lanes))


def to_core(partner, source, target, send_sem, recv_sem):
    return pltpu.make_async_remote_copy(
        src_ref=source,
        dst_ref=target,
        send_sem=send_sem,
        recv_sem=recv_sem,
        device_id=partner,
        device_id_type=pl.DeviceIdType.MESH,
    )


def put_halves(total, out, keep):
    half = total.shape[0] // 2
    out[...] = total[:half, :].astype(bf16).reshape(out.shape)
    keep[...] = total[half:, :].astype(bf16).reshape(keep.shape)


def weight_grad_kernel(devices, lanes, way, given, *refs):
    left, right = refs[:2]
    out, keep, staged, flipped, sent, own, came, send_sem, recv_sem = refs[2 + given :]
    step, steps = pl.program_id(0), pl.num_programs(0) - 1
    me = here(lanes)
    partner = other_core(me, lanes)
    half = flipped.shape[1] // 2

    @pl.when(step == 0)
    def _():
        greet(partner)
        for part in range(left.shape[0]):
            put_rows(me, devices, lanes, way, left[part], staged)
            flipped[part] = staged[...].astype(bf16)

    def copy(at):
        return to_core(partner, sent.at[at % 2], came.at[at], send_sem.at[at], recv_sem.at[at])

    @pl.when(step < steps)
    def _():
        def rows(low):
            total = product(flipped[0, low : low + half, :], right[0, 0])
            for part in range(1, left.shape[0]):
                total += product(flipped[part, low : low + half, :], right[0, part])
            return total

        sent[step % 2] = rows(0).astype(bf16)
        own[step % 2] = rows(half)
        copy(step).start()

    @pl.when(step > 0)
    def _():
        copy(step - 1).wait()
        put_halves(own[(step - 1) % 2] + came[step - 1].astype(f32), out, keep)


def weight_grad(number, devices, lanes, way, left, right, columns, first=0, into=(), only=None):
    parts, rows, depth = left.shape
    low, high = only or (0, right.shape[0])
    kinds, width = high - low, right.shape[3]
    wide = 512
    across = width // wide
    steps = kinds * across
    block = (devices // 4, depth // devices, wide)
    spec = pl.BlockSpec(block, lambda s: (0, 0, first // wide + jnp.maximum(s - 1, 0)))
    shape = jax.ShapeDtypeStruct((devices // 4, depth // devices, columns), bf16)

    def source(s):
        s = jnp.minimum(s, steps - 1)
        return (low + s // across, 0, 0, s % across)

    return pl.pallas_call(
        functools.partial(weight_grad_kernel, devices, lanes, way, len(into)),
        grid=(steps + 1,),
        in_specs=[
            pl.BlockSpec((parts, rows, depth), lambda s: (0, 0, 0)),
            pl.BlockSpec((1, parts, rows, wide), source),
        ]
        + [pl.BlockSpec(memory_space=pltpu.HBM)] * len(into),
        out_specs=[spec, spec],
        scratch_shapes=[
            pltpu.VMEM((depth, rows), f32),
            pltpu.VMEM((parts, depth, rows), bf16),
            pltpu.VMEM((2, depth // 2, wide), bf16),
            pltpu.VMEM((2, depth // 2, wide), f32),
            pltpu.VMEM((steps, depth // 2, wide), bf16),
            pltpu.SemaphoreType.DMA((steps,)),
            pltpu.SemaphoreType.DMA((steps,)),
        ],
        out_shape=[shape, shape],
        input_output_aliases={2 + i: i for i in range(len(into))},
        compiler_params=pltpu.CompilerParams(
            dimension_semantics=("arbitrary",),
            vmem_limit_bytes=VMEM,
            collective_id=number,
            has_side_effects=True,
        ),
        name="weight_grad",
        cost_estimate=cost(3 * kinds * parts),
    )(left, right, *into)


def norm_grad_kernel(d_ref, w_ref, unit, inverse, gain, g_ref, *refs):
    *then, total = refs
    then_w, out, low, gain_out, then_out = then if len(then) == 5 else (None, *then, None)
    step = pl.program_id(0)
    kinds, _, width = d_ref.shape
    part = product_t(d_ref[0], w_ref[:, :width])
    for kind in range(1, kinds):
        part += product_t(d_ref[kind], w_ref[:, kind * width : (kind + 1) * width])
    wide = part.shape[1]
    total[:, pl.ds(pl.multiple_of(step * wide, wide), wide)] = part

    @pl.when(step == pl.num_programs(0) - 1)
    def _():
        change, gain_grad = norm_back(unit[...], inverse[...], gain[...], total[...])
        result = g_ref[...] + change
        out[...] = result
        low[...] = result.astype(bf16)
        gain_out[...] = gain_grad[None, :]
        if then_w is not None:
            then_out[...] = product_t(low[...], then_w[...]).astype(bf16)


def norm_grad(grads, weights, first, unit, inverse, gain, g, then=False):
    kinds, rows, width = grads.shape
    wide = 256

    def whole(shape):
        return pl.BlockSpec(shape, lambda j: (0,) * len(shape))

    return pl.pallas_call(
        norm_grad_kernel,
        grid=(width // wide,),
        in_specs=[
            whole((kinds, rows, width)),
            pl.BlockSpec((wide, kinds * width), lambda j: (j, first)),
            whole((rows, width)), whole((rows, 1)), whole((1, width)), whole((rows, width)),
            *[whole((width, width))] * then,
        ],
        out_specs=[whole((rows, width)), whole((rows, width)), whole((1, width))]
        + [whole((rows, width))] * then,
        out_shape=[
            jax.ShapeDtypeStruct((rows, width), f32),
            jax.ShapeDtypeStruct((rows, width), bf16),
            jax.ShapeDtypeStruct((1, width), f32),
            *[jax.ShapeDtypeStruct((rows, width), bf16)] * then,
        ],
        scratch_shapes=[pltpu.VMEM((rows, width), f32)],
        compiler_params=params(1),
        name="norm_grad",
        cost_estimate=cost(4 * kinds),
    )(grads, weights, unit, inverse, gain, g, *[weights] * then)


def feed_kernel(
    devices, lanes, ways, x_ref, mixed_ref, w_ref, g_ref, gain_ref, up_ref, down_ref,
    out, gx, low_gx, grad_mixed, ggain, up_out, up_keep, down_out, down_keep,
    unit, inverse, hidden, staged, flipped, total, back,
    up_sent, up_own, up_came, down_sent, down_own, down_came,
    up_send_sem, up_recv_sem, down_send_sem, down_recv_sem,
):
    step, groups = pl.program_id(0), pl.num_programs(0) - 1
    me = here(lanes)
    partner = other_core(me, lanes)
    core, low, high = (me // lanes) % 2, me % lanes, me // (2 * lanes)

    @pl.when(step == 0)
    def _():
        greet(partner)
        x = x_ref[...] + product(mixed_ref[...], w_ref[...])
        h, u, i = normed(x, gain_ref[...])
        unit[...] = u
        inverse[...] = i
        hidden[...] = h.astype(bf16)
        put_rows(me, devices, lanes, ways[0], h, staged)
        flipped[...] = staged[...].astype(bf16)
        total[...] = x
        back[...] = jnp.zeros_like(back)

    def up_copy(at):
        return to_core(partner, up_sent.at[at % 2], up_came.at[at], up_send_sem.at[at], up_recv_sem.at[at])

    def down_copy(at):
        return to_core(partner, down_sent, down_came.at[at], down_send_sem.at[at], down_recv_sem.at[at])

    @pl.when(step < groups)
    def _():
        g = g_ref[...]
        up = up_ref[...].reshape(-1, up_ref.shape[-1])
        down = down_ref[...].reshape(-1, down_ref.shape[-1])
        inner = product(hidden[...], up)
        share = 0.5 + 0.5 * lax.erf(inner * (0.5**0.5))
        slope = share + inner * (jnp.exp(-0.5 * inner * inner) * 0.3989422804014327)
        active = (inner * share).astype(bf16)
        change = (product_t(g, down) * slope).astype(bf16)
        half = flipped.shape[0] // 2
        up_sent[step % 2] = product(flipped[:half, :], change).astype(bf16)
        grad_down = product_rows(active, g)

        @pl.when(step % 2 != core)
        def _():
            down_sent[...] = grad_down.astype(bf16)

        @pl.when(step % 2 == core)
        def _():
            down_own[...] = grad_down

        up_own[step % 2] = product(flipped[half:, :], change)
        total[...] += product(active, down)
        back[...] += product_t(change, up)
        up_copy(step).start()

        @pl.when(step % 2 != core)
        def _():
            down_copy(step // 2).start()

    @pl.when(step == groups)
    def _():
        out[...] = total[...].astype(bf16)
        gx_norm, gain_grad = norm_back(unit[...], inverse[...], gain_ref[...], back[...])
        result = g_ref[...].astype(f32) + gx_norm
        gx[...] = result
        low_gx[...] = result.astype(bf16)
        grad_mixed[...] = product_t(low_gx[...], w_ref[...]).astype(bf16)
        ggain[...] = gain_grad[None, :]

    @pl.when(step > 0)
    def _():
        before = step - 1
        up_copy(before).wait()
        put_halves(up_own[before % 2] + up_came[before].astype(f32), up_out, up_keep)

        @pl.when(before % 2 != core)
        def _():
            down_copy(before // 2).wait_send()

        @pl.when(before % 2 == core)
        def _():
            down_copy(before // 2).wait_recv()
            sums = down_own[...] + down_came[before // 2].astype(f32)
            depth = sums.shape[0] // lanes
            for block in range(lanes):
                relative = (block ^ low) + 2 * lanes * ((before // 2) ^ high)
                place = place_of(relative, devices, lanes, ways[1])
                piece = sums[block * depth : (block + 1) * depth, :].astype(bf16)
                goes = bit_of(relative, ways[1][0]) == 1

                @pl.when(goes)
                def _(place=place, piece=piece):
                    down_out[place] = piece

                @pl.when(jnp.logical_not(goes))
                def _(place=place, piece=piece):
                    down_keep[place] = piece


def feed(number, devices, lanes, ways, x, mixed, projection, g, gain, weights):
    rows, width = x.shape
    pieces, depth = weights.shape[2:4]
    hidden = pieces * width
    groups = devices // lanes
    tile = hidden // groups
    across = width // tile

    def group(s):
        return jnp.minimum(s, groups - 1)

    def whole(shape):
        return pl.BlockSpec(shape, lambda s: (0,) * len(shape), pipeline_mode=pl.Buffered(1))

    last = projection.shape[1] // width - 1
    up_block = pl.BlockSpec((devices // 4, depth, tile), lambda s: (0, 0, jnp.maximum(s - 1, 0)))
    up_shape = jax.ShapeDtypeStruct((devices // 4, depth, hidden), bf16)
    down_shape = jax.ShapeDtypeStruct((devices // 4, hidden // devices, width), bf16)
    return pl.pallas_call(
        functools.partial(feed_kernel, devices, lanes, ways),
        grid=(groups + 1,),
        in_specs=[
            whole((rows, width)),
            whole((rows, width)),
            pl.BlockSpec((width, width), lambda s: (0, last), pipeline_mode=pl.Buffered(1)),
            whole((rows, width)),
            whole((1, width)),
            pl.BlockSpec(
                (devices, None, None, depth, tile),
                lambda s: (0, 0, group(s) // across, 0, group(s) % across),
            ),
            pl.BlockSpec((lanes, None, pieces, depth, width), lambda s: (group(s), 1, 0, 0, 0)),
        ],
        out_specs=[
            *[whole((rows, width))] * 4, whole((1, width)),
            up_block, up_block, whole(down_shape.shape), whole(down_shape.shape),
        ],
        scratch_shapes=[
            pltpu.VMEM((rows, width), f32),
            pltpu.VMEM((rows, 1), f32),
            pltpu.VMEM((rows, width), bf16),
            pltpu.VMEM((width, rows), f32),
            pltpu.VMEM((width, rows), bf16),
            pltpu.VMEM((rows, width), f32),
            pltpu.VMEM((rows, width), f32),
            pltpu.VMEM((2, width // 2, tile), bf16),
            pltpu.VMEM((2, width // 2, tile), f32),
            pltpu.VMEM((groups, width // 2, tile), bf16),
            pltpu.VMEM((tile, width), bf16),
            pltpu.VMEM((tile, width), f32),
            pltpu.VMEM((groups // 2, tile, width), bf16),
            pltpu.SemaphoreType.DMA((groups,)),
            pltpu.SemaphoreType.DMA((groups,)),
            pltpu.SemaphoreType.DMA((groups // 2,)),
            pltpu.SemaphoreType.DMA((groups // 2,)),
        ],
        out_shape=[
            jax.ShapeDtypeStruct((rows, width), bf16),
            jax.ShapeDtypeStruct((rows, width), f32),
            jax.ShapeDtypeStruct((rows, width), bf16),
            jax.ShapeDtypeStruct((rows, width), bf16),
            jax.ShapeDtypeStruct((1, width), f32),
            up_shape, up_shape, down_shape, down_shape,
        ],
        compiler_params=pltpu.CompilerParams(
            dimension_semantics=("arbitrary",),
            vmem_limit_bytes=VMEM,
            collective_id=number,
            has_side_effects=True,
        ),
        name="feed",
        cost_estimate=cost(40),
    )(x, mixed, projection, g, gain, weights, weights)


class Spread:
    def __init__(self, devices, lanes, tracks, x_ref, out, own_sem, send_sem, recv_sem):
        self.devices, self.lanes, self.tracks = devices, lanes, tracks
        self.x_ref, self.out, self.own_sem = x_ref, out, own_sem
        self.send_sem, self.recv_sem = send_sem, recv_sem
        self.count, self.me = devices // 2, here(lanes)
        numbers = sorted(range(self.count), key=lambda k: (bin(k).count("1"), k))
        self.sends = [
            (track, number, place, bit)
            for number in numbers
            for track, (_, _, bits) in enumerate(tracks)
            for place, bit in enumerate(bits + (lanes,))
            if number >> place == 0 or bit == lanes
        ]
        self.numbers = numbers[1:]

    def device(self, bit):
        other = self.me ^ bit
        return (other // self.lanes, lax.rem(other, self.lanes))

    def block(self, track, number):
        low, high, bits = self.tracks[track]
        to_core = number >= self.count
        number -= self.count * to_core
        owner = self.me ^ sum(b for p, b in enumerate(bits) if (number >> p) & 1)
        return self.out.at[owner ^ self.lanes if to_core else owner, :, low:high]

    def copy(self, index):
        track, number, place, bit = self.sends[index]
        low, high, _ = self.tracks[track]
        target = self.block(track, number)
        return pltpu.make_async_remote_copy(
            src_ref=target if number else self.x_ref.at[:, low:high],
            dst_ref=target,
            send_sem=self.send_sem.at[index],
            recv_sem=self.recv_sem.at[track, number + (1 << place)],
            device_id=self.device(bit),
            device_id_type=pl.DeviceIdType.MESH,
        )

    def own(self):
        return pltpu.make_async_copy(self.x_ref, self.out.at[self.me], self.own_sem)

    def wait(self, track, number):
        target = self.block(track, number)
        pltpu.make_async_remote_copy(
            src_ref=target,
            dst_ref=target,
            send_sem=self.send_sem.at[0],
            recv_sem=self.recv_sem.at[track, number],
            device_id=self.device(self.lanes),
            device_id_type=pl.DeviceIdType.MESH,
        ).wait_recv()

    def send(self, number):
        for index, (_, sent, _, _) in enumerate(self.sends):
            if sent == number:
                self.copy(index).start()

    def start(self):
        barrier = pltpu.get_barrier_semaphore()
        every = [1 << b for b in range(self.devices.bit_length() - 1)]
        for bit in every:
            pl.semaphore_signal(
                barrier, inc=1, device_id=self.device(bit), device_id_type=pl.DeviceIdType.MESH
            )
        pl.semaphore_wait(barrier, len(every))
        self.own().start()
        self.send(0)

    def forward(self, numbers):
        for number in numbers:
            for track in range(len(self.tracks)):
                self.wait(track, number)
            self.send(number)

    def finish(self):
        for number in range(self.count, self.devices):
            for track in range(len(self.tracks)):
                self.wait(track, number)
        for index in range(len(self.sends)):
            self.copy(index).wait_send()
        self.own().wait()


def tracks_of(devices, lanes, columns):
    middle = (columns // 256) * 128
    high = tuple(2 * lanes << b for b in range((devices // (2 * lanes)).bit_length() - 1))
    links = [high + tuple(1 << b for b in way) for way in orders(lanes)]
    return ((0, middle, links[0]), (middle, columns, links[1]))


def spread_scratch(devices):
    return [
        pltpu.SemaphoreType.DMA,
        pltpu.SemaphoreType.DMA((2 * (devices - 1),)),
        pltpu.SemaphoreType.DMA((2, devices)),
    ]


def gather_kernel(devices, lanes, tracks, x_ref, out, own_sem, send_sem, recv_sem):
    spread = Spread(devices, lanes, tracks, x_ref, out, own_sem, send_sem, recv_sem)
    spread.start()
    spread.forward(spread.numbers)
    spread.finish()


def gather(number, devices, lanes, values):
    depth, columns = values.shape
    return pl.pallas_call(
        functools.partial(gather_kernel, devices, lanes, tracks_of(devices, lanes, columns)),
        in_specs=[pl.BlockSpec(memory_space=pltpu.VMEM)],
        out_specs=pl.BlockSpec(memory_space=pltpu.HBM),
        out_shape=jax.ShapeDtypeStruct((devices, depth, columns), values.dtype),
        scratch_shapes=spread_scratch(devices),
        compiler_params=pltpu.CompilerParams(collective_id=number, has_side_effects=True),
        name="gather",
        cost_estimate=cost(60),
    )(values).reshape(-1, columns)


def attend_kernel(
    devices, lanes, tracks, x_ref, page_column, page_row, hidden, w_q, w_k, w_v,
    gathered, q, k, v, out, totals, own_sem, send_sem, recv_sem, bias,
):
    step = pl.program_id(0)
    spread = Spread(devices, lanes, tracks, x_ref, gathered, own_sem, send_sem, recv_sem)

    @pl.when(step == 0)
    def _():
        spread.start()
        fill_bias(page_column, page_row, bias, hidden.shape[0] // TILE)

    for ref, weights in ((q, w_q), (k, w_k), (v, w_v)):
        ref[...] = product(hidden[...], weights[...]).astype(bf16)
    attend_pair(q, k, v, out, totals, bias)

    turns = hidden.shape[1] // 128
    for turn in range(1, turns):
        few = spread.numbers[
            len(spread.numbers) * (turn - 1) // (turns - 1) : len(spread.numbers) * turn // (turns - 1)
        ]

        @pl.when(step == turn)
        def _(few=few, last=turn == turns - 1):
            spread.forward(few)
            if last:
                spread.finish()


def attend(number, devices, lanes, values, page_column, page_row, hidden, weights):
    depth, columns = values.shape
    rows, width = hidden.shape
    pairs = width // 128

    def whole(*shape):
        return pl.BlockSpec(shape, lambda j: (0,) * len(shape))

    head = pl.BlockSpec((rows, 128), lambda j: (0, j))
    results = pl.pallas_call(
        functools.partial(attend_kernel, devices, lanes, tracks_of(devices, lanes, columns)),
        grid=(pairs,),
        in_specs=[
            whole(depth, columns), whole(rows, 1), whole(1, rows), whole(rows, width),
            pl.BlockSpec((width, 128), lambda j: (0, j)),
            pl.BlockSpec((width, 128), lambda j: (0, pairs + j)),
            pl.BlockSpec((width, 128), lambda j: (0, 2 * pairs + j)),
        ],
        out_specs=[
            pl.BlockSpec(memory_space=pltpu.HBM), head, head, head, head,
            pl.BlockSpec((1, 2, rows), lambda j: (j, 0, 0)),
        ],
        out_shape=[
            jax.ShapeDtypeStruct((devices, depth, columns), values.dtype),
            *[jax.ShapeDtypeStruct((rows, width), bf16)] * 4,
            jax.ShapeDtypeStruct((pairs, 2, rows), f32),
        ],
        scratch_shapes=spread_scratch(devices)
        + [pltpu.VMEM((rows // TILE, PAGE_MAX + TILE, TILE), f32)],
        compiler_params=pltpu.CompilerParams(
            dimension_semantics=("arbitrary",),
            vmem_limit_bytes=VMEM,
            collective_id=number,
            has_side_effects=True,
        ),
        name="attend",
        cost_estimate=cost(60),
    )(values, page_column, page_row, hidden, weights, weights, weights)
    gathered, q, k, v, *rest = results
    return gathered.reshape(-1, columns), (q, k, v), *rest


def image_kernel(images, weights, out):
    for image in range(images.shape[0]):
        out[image] = product(images[image], weights[...]).astype(bf16)


def image_keys(images, weights, first):
    count, length, width = images.shape
    wide = 512
    return pl.pallas_call(
        image_kernel,
        grid=(2 * width // wide,),
        in_specs=[
            pl.BlockSpec(images.shape, lambda j: (0, 0, 0)),
            pl.BlockSpec((width, wide), lambda j: (0, first * width // wide + j)),
        ],
        out_specs=pl.BlockSpec((count, length, wide), lambda j: (0, 0, j)),
        out_shape=jax.ShapeDtypeStruct((count, length, 2 * width), bf16),
        compiler_params=params(1),
        name="image_keys",
        cost_estimate=cost(8),
    )(images, weights)


def swap(values, devices, bit):
    return lax.ppermute(values, AXES, [(i, i ^ bit) for i in range(devices)])


def plus(a, b):
    return (a.astype(f32) + b.astype(f32)).astype(bf16)


def owner_sums(halves, devices, lanes, way, late=None):
    bits = stages(devices, lanes, way)
    out, keep = halves
    for stage, bit in enumerate(bits):
        arrived = swap(out, devices, 1 << bit)
        if stage == len(bits) - 1:
            return keep[0].astype(f32) + arrived[0].astype(f32)
        half = keep.shape[0] // 2
        out, keep = plus(keep[half:], arrived[half:]), plus(keep[:half], arrived[:half])
        if stage == 0 and late is not None:
            late_out, late_keep = late
            late_arrived = swap(late_out, devices, 1 << bit)
            out = jnp.concatenate([out, plus(late_keep[half:], late_arrived[half:])], axis=-1)
            keep = jnp.concatenate([keep, plus(late_keep[:half], late_arrived[:half])], axis=-1)


def gain_halves(values, devices, lanes, way, me):
    kinds, depth = values.shape
    blocks = jnp.pad(values.T, ((0, 0), (0, 128 - kinds))).astype(bf16)
    every = range(devices)
    core = lanes.bit_length() - 1
    order = sorted(every, key=lambda r: (1 - bit_of(r, core), 1 - bit_of(r, way[0]), place_of(r, devices, lanes, way)))
    blocks = blocks.reshape(devices, depth // devices, 128)[jnp.array(order) ^ me]
    arrived = swap(blocks[: devices // 2], devices, lanes)
    sums = plus(blocks[devices // 2 :], arrived)
    return sums[: devices // 4], sums[devices // 4 :]


def after(values, first):
    return lax.optimization_barrier((values, first))[0]


def orders(lanes):
    low = list(range(lanes.bit_length() - 1))
    return low, low[::-1]


def shards(devices, lanes, tokens, images, segment_ids, image_map, out_grad, norm_self, attn_query,
           attn_key, attn_value, attn_out, norm_cross, cross_query, cross_key, cross_value, cross_out,
           norm_ffn, ffn_up, ffn_down):
    me = lax.axis_index("dp") * lanes + lax.axis_index("fsdp")
    me_ref = me.astype(jnp.int32)[None]
    depth, width = attn_query.shape
    gains = jnp.stack([norm_self, norm_cross, norm_ffn], axis=1)
    gains = jnp.pad(gains, ((0, 0), (0, 128 - 3)))
    first_set = jnp.concatenate([attn_query, attn_key, attn_value, gains], axis=1)
    second_set = jnp.concatenate([attn_out, cross_query, cross_key, cross_value, cross_out], axis=1)
    pieces = ffn_up.shape[1] // width
    feed_set = jnp.stack(
        [ffn_up.reshape(depth, pieces, width).transpose(1, 0, 2), ffn_down.reshape(pieces, depth, width)]
    )
    first_set = gather(0, devices, lanes, first_set)
    feed_set = lax.all_gather(after(feed_set, first_set), AXES, axis=0)
    (count, order, page_column, page_row, inputs, grad_out, hidden_one, unit_one, inverse_one, *gains) = arrange(
        image_map[0], segment_ids[0], tokens[0], out_grad[0], first_set, 3 * width // 128
    )
    second_set, qkv, mixed_one, log_one = attend(
        1, devices, lanes, second_set, page_column, page_row, hidden_one, first_set
    )
    w_kv = second_set[:, 2 * width : 4 * width]
    kv = image_keys(images, second_set, 2)
    after_self, hidden_two, unit_two, inverse_two, query_two = between(inputs, mixed_one, second_set, gains[1])
    mixed_two, log_two = cross_forward(count, query_two, kv)

    one_way, other_way = orders(lanes)
    (output, grad_after_cross, branch_two, grad_mixed_two, grad_gain_ffn, *halves) = feed(
        2, devices, lanes, (one_way, other_way), after_self, mixed_two, second_set, grad_out, gains[2], feed_set
    )

    def sums(way, halves, late=None):
        return owner_sums(halves, devices, lanes, way, late)

    def halves_of(number, way, left, right, **options):
        return weight_grad(number, devices, lanes, way, left, right, 2 * width, **options)

    grad_up = sums(one_way, halves[:2])
    grad_down = sums(other_way, halves[2:])

    grad_query_two, grad_kv = cross_backward(count, query_two, kv, grad_mixed_two, log_two)
    halves = halves_of(3, one_way, mixed_two[None], after(branch_two, grad_kv)[None, None])
    halves = halves_of(4, one_way, hidden_two[None], grad_query_two[None, None], first=width, into=halves)
    grad_c = sums(one_way, halves)
    halves = halves_of(5, other_way, images, after(grad_kv, halves[0]))
    grad_d = sums(other_way, halves)
    grad_query_again = after(grad_query_two, halves[0])[None]
    grad_after_self, branch_one, grad_gain_cross, grad_mixed_one = norm_grad(
        grad_query_again, second_set, 1, unit_two, inverse_two, gains[1], grad_after_cross, then=True
    )
    grad_qkv = self_backward(page_column, page_row, qkv, grad_mixed_one, log_one)
    halves = halves_of(6, one_way, mixed_one[None], after(branch_one, grad_qkv)[None, None])
    options = dict(first=width, into=halves, only=(0, 1))
    halves = halves_of(7, one_way, hidden_one[None], grad_qkv[:, None], **options)
    grad_qkv_again = after(grad_qkv, halves[0])
    halves_kv = halves_of(8, one_way, hidden_one[None], grad_qkv_again[:, None], only=(1, 3))
    grad_qkv_again = after(grad_qkv, halves_kv[0])
    _, grad_inputs, grad_gain_self = norm_grad(
        grad_qkv_again, first_set, 0, unit_one, inverse_one, gains[0], grad_after_self
    )
    gain_grads = jnp.concatenate([grad_gain_self, grad_gain_cross, grad_gain_ffn])
    late = gain_halves(gain_grads, devices, lanes, one_way, me)
    grad_a = sums(one_way, halves)
    grad_b = sums(one_way, halves_kv, late)
    gain_sums = grad_b[:, 2 * width :]

    grad_kv = after(grad_kv, late[0])
    back = (((2,), (1,)), ((), ()))
    grad_images = lax.dot_general(grad_kv[0], w_kv[:, :width], back, preferred_element_type=f32)
    grad_images += lax.dot_general(grad_kv[1], w_kv[:, width:], back, preferred_element_type=f32)
    output = product_rows(order, output).astype(bf16)
    grad_inputs = product_rows(order, grad_inputs).astype(bf16)
    return (
        output[None],
        grad_inputs[None],
        grad_images.astype(bf16),
        gain_sums[:, 0],
        grad_a[:, width:],
        grad_b[:, :width],
        grad_b[:, width : 2 * width],
        grad_a[:, :width],
        gain_sums[:, 1],
        grad_c[:, width:],
        grad_d[:, :width],
        grad_d[:, width:],
        grad_c[:, :width],
        gain_sums[:, 2],
        grad_up,
        grad_down,
    )


def solution(mesh):
    rows = P(AXES)
    devices, lanes = mesh.shape["dp"] * mesh.shape["fsdp"], mesh.shape["fsdp"]
    return jax.shard_map(
        functools.partial(shards, devices, lanes),
        mesh=mesh,
        in_specs=(rows,) * 18,
        out_specs=(rows,) * 16,
        check_vma=False,
    )
```

```python
import functools

import jax
import jax.numpy as jnp
from jax import lax
from jax.experimental import pallas as pl
from jax.experimental.pallas import tpu as pltpu
from jax.sharding import PartitionSpec as P


AXES = ("dp", "fsdp")
LOG2E = 1.4426950408889634
EPSILON = 1e-05
MASKED = -1e30
TILE = 128
PAGE_MAX = 256
VMEM = 62 * 1024 * 1024

bf16 = jnp.bfloat16
f32 = jnp.float32


def product(left, right):
    return jnp.dot(left, right, preferred_element_type=f32)


def product_t(left, right):
    return lax.dot_general(left, right, (((1,), (1,)), ((), ())), preferred_element_type=f32)


def product_rows(left, right):
    return lax.dot_general(left, right, (((0,), (0,)), ((), ())), preferred_element_type=f32)


def normed(values, gain):
    centred = values - jnp.mean(values, axis=-1, keepdims=True)
    variance = jnp.mean(centred * centred, axis=-1, keepdims=True)
    inverse = lax.rsqrt(variance + EPSILON)
    unit = centred * inverse
    return unit * gain, unit, inverse


def norm_back(unit, inverse, gain, gradient):
    scaled = gradient * gain
    mean_scaled = jnp.mean(scaled, axis=-1, keepdims=True)
    mean_along = jnp.mean(scaled * unit, axis=-1, keepdims=True)
    return inverse * (scaled - mean_scaled - unit * mean_along), jnp.sum(gradient * unit, axis=0)


def params(count):
    return pltpu.CompilerParams(
        dimension_semantics=("arbitrary",) * count, vmem_limit_bytes=VMEM
    )


def cost(microseconds):
    return pl.CostEstimate(flops=int(microseconds * 1e9), bytes_accessed=0, transcendentals=0)


def two_heads(block):
    lane = lax.broadcasted_iota(jnp.int32, block.shape, 1)
    zero = jnp.zeros_like(block)
    half = block.shape[1] // 2
    return jnp.concatenate(
        [jnp.where(lane < half, block, zero), jnp.where(lane >= half, block, zero)], axis=0
    )


def join_heads(both):
    rows = both.shape[1] // 2
    feature = lax.broadcasted_iota(jnp.int32, (both.shape[0], rows), 0)
    return jnp.where(feature < both.shape[0] // 2, both[:, :rows], both[:, rows:]).T


def twice(row):
    return jnp.concatenate([row, row], axis=1)


def arrange_kernel(
    map_ref, page_column, page_row, tokens, g, columns,
    count, order, new_column, new_row, inputs, new_g, hidden, unit, inverse, *gains,
):
    rows = tokens.shape[0]

    def second_of(pages):
        return sum(jnp.where(pages == p, map_ref[p], 0) for p in range(map_ref.shape[0])).astype(f32)

    column, row = second_of(page_column[...]), second_of(page_row[...])
    i = lax.broadcasted_iota(jnp.int32, (rows, rows), 0)
    j = lax.broadcasted_iota(jnp.int32, (rows, rows), 1)
    before_column = jnp.sum(jnp.where(j < i, row, 0.0), axis=1, keepdims=True)
    before_row = jnp.sum(jnp.where(i < j, column, 0.0), axis=0, keepdims=True)
    first = rows - jnp.sum(row)
    count[0] = first.astype(jnp.int32)
    at_column = lax.broadcasted_iota(jnp.int32, (rows, 1), 0).astype(f32)
    at_row = lax.broadcasted_iota(jnp.int32, (1, rows), 1).astype(f32)
    place_column = jnp.where(column > 0, first + before_column, at_column - before_column)
    place_row = jnp.where(row > 0, first + before_row, at_row - before_row)
    moved = i.astype(f32) == place_row
    order[...] = moved.astype(f32).astype(bf16)
    pages = page_row[...].astype(f32)
    new_column[...] = jnp.sum(jnp.where(moved, pages, 0.0), axis=1, keepdims=True).astype(jnp.int32)
    pages = page_column[...].astype(f32)
    back = place_column == j.astype(f32)
    new_row[...] = jnp.sum(jnp.where(back, pages, 0.0), axis=0, keepdims=True).astype(jnp.int32)
    new_g[...] = product(order[...], g[...]).astype(bf16)
    flat = columns[...].astype(f32).T
    for number, gain in enumerate(gains):
        gain[...] = flat[number : number + 1, :]
    inputs[...] = product(order[...], tokens[...])
    h, unit[...], inverse[...] = normed(inputs[...], gains[0][...])
    hidden[...] = h.astype(bf16)


def arrange(image_map, pages, tokens, g, weights, first):
    rows, width = tokens.shape

    def whole(*shape):
        return pl.BlockSpec(shape, lambda s: (0,) * len(shape))

    scalars = pl.BlockSpec(memory_space=pltpu.SMEM)
    kinds = [
        ((rows, rows), bf16), ((rows, 1), jnp.int32), ((1, rows), jnp.int32),
        ((rows, width), f32), ((rows, width), bf16), ((rows, width), bf16),
        ((rows, width), f32), ((rows, 1), f32), *[((1, width), f32)] * 3,
    ]
    return pl.pallas_call(
        arrange_kernel,
        grid=(1,),
        in_specs=[
            scalars, whole(rows, 1), whole(1, rows), whole(rows, width), whole(rows, width),
            pl.BlockSpec((width, 128), lambda s: (0, first)),
        ],
        out_specs=[scalars] + [whole(*shape) for shape, _ in kinds],
        out_shape=[jax.ShapeDtypeStruct((1,), jnp.int32)]
        + [jax.ShapeDtypeStruct(shape, dtype) for shape, dtype in kinds],
        compiler_params=params(1),
        name="arrange",
        cost_estimate=cost(6),
    )(image_map, pages[:, None], pages[None, :], tokens, g, weights)


def between_kernel(x_ref, mixed, w_out, w_query, gain, x_out, hidden, unit, inverse, query):
    x = x_ref[...] + product(mixed[...], w_out[...])
    x_out[...] = x
    h, unit[...], inverse[...] = normed(x, gain[...])
    hidden[...] = h.astype(bf16)
    query[...] = product(hidden[...], w_query[...]).astype(bf16)


def between(x, mixed, weights, gain):
    rows, width = x.shape
    tile = rows // 2

    def part(columns):
        return pl.BlockSpec((tile, columns), lambda s: (s, 0))

    kinds = ((width, f32), (width, bf16), (width, f32), (1, f32), (width, bf16))
    return pl.pallas_call(
        between_kernel,
        grid=(2,),
        in_specs=[
            part(width), part(width),
            pl.BlockSpec((width, width), lambda s: (0, 0)),
            pl.BlockSpec((width, width), lambda s: (0, 1)),
            pl.BlockSpec((1, width), lambda s: (0, 0)),
        ],
        out_specs=[part(columns) for columns, _ in kinds],
        out_shape=[jax.ShapeDtypeStruct((rows, columns), dtype) for columns, dtype in kinds],
        compiler_params=params(1),
        name="between",
        cost_estimate=cost(8),
    )(x, mixed, weights, weights, gain)


def key_range(tile):
    return max(0, tile * TILE - PAGE_MAX), (tile + 1) * TILE


def fill_bias(page_column, page_row, bias, tiles):
    for tile in range(tiles):
        low, high = key_range(tile)
        keys = low + lax.broadcasted_iota(jnp.int32, (high - low, TILE), 0)
        queries = tile * TILE + lax.broadcasted_iota(jnp.int32, (high - low, TILE), 1)
        same = page_column[low:high, :] == page_row[:, tile * TILE : (tile + 1) * TILE]
        bias[tile, : high - low, :] = jnp.where((keys <= queries) & same, 0.0, MASKED)


def attend_pair(q, k, v, out, totals, bias):
    tiles = q.shape[0] // TILE
    scale = LOG2E * (q.shape[1] // 2) ** (-0.5)
    for tile in range(tiles):
        low, high = key_range(tile)
        at = slice(tile * TILE, (tile + 1) * TILE)
        scores = product_t(k[low:high, :], two_heads(q[at, :])) * scale + twice(
            bias[tile, : high - low, :]
        )
        highest = jnp.max(scores, axis=0, keepdims=True)
        weights = jnp.exp2(scores - highest)
        total = jnp.sum(weights, axis=0, keepdims=True)
        mixed = product_rows(v[low:high, :], weights.astype(bf16)) * (1.0 / total)
        out[at, :] = join_heads(mixed).astype(bf16)
        level = highest + jnp.log2(total)
        totals[0, 0:1, at] = level[:, :TILE]
        totals[0, 1:2, at] = level[:, TILE:]


def self_backward_kernel(page_column, page_row, q, k, v, g, totals, out, bias, dk, dv):
    tiles = q.shape[0] // TILE
    half_scale = (q.shape[1] // 2) ** (-0.5)
    scale = LOG2E * half_scale

    @pl.when(pl.program_id(0) == 0)
    def _():
        fill_bias(page_column, page_row, bias, tiles)

    dk[...] = jnp.zeros_like(dk)
    dv[...] = jnp.zeros_like(dv)
    for tile in range(tiles):
        low, high = key_range(tile)
        here = slice(tile * TILE, (tile + 1) * TILE)
        queries, grads = two_heads(q[here, :]), two_heads(g[here, :])
        keys, values = k[low:high, :], v[low:high, :]
        level = jnp.concatenate([totals[0, 0:1, here], totals[0, 1:2, here]], axis=1)
        weights = jnp.exp2(
            product_t(keys, queries) * scale + twice(bias[tile, : high - low, :]) - level
        )
        along = weights * product_t(values, grads)
        change = (along - weights * jnp.sum(along, axis=0, keepdims=True)).astype(bf16)
        dv[low:high, :] += product(weights.astype(bf16), grads)
        dk[low:high, :] += product(change, queries)
        out[0, here, :] = (join_heads(product_rows(keys, change)) * half_scale).astype(bf16)
    out[1] = (dk[...] * half_scale).astype(bf16)
    out[2] = dv[...].astype(bf16)


def self_backward(page_column, page_row, qkv, grads, totals):
    rows, width = grads.shape
    pairs = width // 128
    return pl.pallas_call(
        self_backward_kernel,
        grid=(pairs,),
        in_specs=[
            pl.BlockSpec((rows, 1), lambda j: (0, 0)),
            pl.BlockSpec((1, rows), lambda j: (0, 0)),
            *[pl.BlockSpec((rows, 128), lambda j: (0, j))] * 4,
            pl.BlockSpec((1, 2, rows), lambda j: (j, 0, 0)),
        ],
        out_specs=pl.BlockSpec((3, rows, 128), lambda j: (0, 0, j)),
        out_shape=jax.ShapeDtypeStruct((3, rows, width), bf16),
        scratch_shapes=[
            pltpu.VMEM((rows // TILE, PAGE_MAX + TILE, TILE), f32),
            pltpu.VMEM((rows, 128), f32),
            pltpu.VMEM((rows, 128), f32),
        ],
        compiler_params=params(1),
        name="self_backward",
        cost_estimate=cost(15),
    )(page_column, page_row, *qkv, grads, totals)


def cross_steps(count, tiles):
    first = (count + TILE - 1) // TILE
    skip = count // TILE
    return first, skip, first + tiles - skip


def cross_step(step, first, skip):
    image = jnp.where(step < first, 0, 1)
    tile = jnp.where(step < first, step, step - first + skip)
    return image, pl.multiple_of(tile * TILE, TILE)


PARTS = 2


def cross_forward_kernel(count_ref, q, k, v, out, totals):
    scale = LOG2E * (q.shape[1] // (2 * PARTS)) ** (-0.5)
    count = count_ref[0]
    first, skip, steps = cross_steps(count, q.shape[0] // TILE)

    def one(step, carry):
        image, start = cross_step(step, first, skip)
        at = pl.ds(start, TILE)
        row = start + lax.broadcasted_iota(jnp.int32, (TILE, 128), 0)
        lane = start + lax.broadcasted_iota(jnp.int32, (1, TILE), 1)
        here_row, here_lane = ((x >= count) == (image == 1) for x in (row, lane))
        lanes = [slice(128 * part, 128 * (part + 1)) for part in range(PARTS)]
        scores = [product_t(k[image, :, l], two_heads(q[at, l])) * scale for l in lanes]
        for part, l in enumerate(lanes):
            highest = jnp.max(scores[part], axis=0, keepdims=True)
            weights = jnp.exp2(scores[part] - highest)
            total = jnp.sum(weights, axis=0, keepdims=True)
            mixed = product_rows(v[image, :, l], weights.astype(bf16)) * (1.0 / total)
            old = out[at, l].astype(f32)
            out[at, l] = jnp.where(here_row, join_heads(mixed), old).astype(bf16)
            level = highest + jnp.log2(total)
            for head in range(2):
                index = slice(2 * part + head, 2 * part + head + 1)
                mine = level[:, head * TILE : (head + 1) * TILE]
                totals[0, index, at] = jnp.where(here_lane, mine, totals[0, index, at])
        return carry

    lax.fori_loop(0, steps, one, 0)


def cross_forward(count, query, kv):
    rows, width = query.shape
    wide = 128 * PARTS
    turns = width // wide
    images, length = kv.shape[:2]
    return pl.pallas_call(
        cross_forward_kernel,
        grid_spec=pltpu.PrefetchScalarGridSpec(
            num_scalar_prefetch=1,
            grid=(turns,),
            in_specs=[
                pl.BlockSpec((rows, wide), lambda j, c: (0, j)),
                pl.BlockSpec((images, length, wide), lambda j, c: (0, 0, j)),
                pl.BlockSpec((images, length, wide), lambda j, c: (0, 0, turns + j)),
            ],
            out_specs=[
                pl.BlockSpec((rows, wide), lambda j, c: (0, j)),
                pl.BlockSpec((1, 2 * PARTS, rows), lambda j, c: (j, 0, 0)),
            ],
        ),
        out_shape=[
            jax.ShapeDtypeStruct((rows, width), bf16),
            jax.ShapeDtypeStruct((turns, 2 * PARTS, rows), f32),
        ],
        compiler_params=params(1),
        name="cross_forward",
        cost_estimate=cost(24),
    )(count, query, kv, kv)


def cross_backward_kernel(count_ref, q, k, v, g, totals, dq_out, dkv_out, dq, dk, dv):
    half_scale = (q.shape[1] // (2 * PARTS)) ** (-0.5)
    scale = LOG2E * half_scale
    count = count_ref[0]
    first, skip, steps = cross_steps(count, q.shape[0] // TILE)
    dq[...] = jnp.zeros_like(dq)
    dk[...] = jnp.zeros_like(dk)
    dv[...] = jnp.zeros_like(dv)

    def one(step, carry):
        image, start = cross_step(step, first, skip)
        at = pl.ds(start, TILE)
        lane = start + lax.broadcasted_iota(jnp.int32, (1, TILE), 1)
        mine = (lane >= count) == (image == 1)
        lanes = [slice(128 * part, 128 * (part + 1)) for part in range(PARTS)]
        queries = [two_heads(q[at, l]) for l in lanes]
        grads = [two_heads(g[at, l]) for l in lanes]
        scores = [product_t(k[image, :, l], queries[part]) for part, l in enumerate(lanes)]
        along = [product_t(v[image, :, l], grads[part]) for part, l in enumerate(lanes)]
        for part, l in enumerate(lanes):
            level = jnp.concatenate(
                [
                    jnp.where(mine, totals[0, 2 * part + head : 2 * part + head + 1, at], -MASKED)
                    for head in range(2)
                ],
                axis=1,
            )
            weights = jnp.exp2(scores[part] * scale - level)
            dv[image, :, l] += product(weights.astype(bf16), grads[part])
            change = weights * along[part]
            change = (change - weights * jnp.sum(change, axis=0, keepdims=True)).astype(bf16)
            dk[image, :, l] += product(change, queries[part])
            dq[at, l] += join_heads(product_rows(k[image, :, l], change))
        return carry

    lax.fori_loop(0, steps, one, 0)
    dq_out[...] = (dq[...] * half_scale).astype(bf16)
    dkv_out[0] = (dk[...] * half_scale).astype(bf16)
    dkv_out[1] = dv[...].astype(bf16)


def cross_backward(count, query, kv, grads, totals):
    rows, width = query.shape
    wide = 128 * PARTS
    turns = width // wide
    images, length = kv.shape[:2]
    return pl.pallas_call(
        cross_backward_kernel,
        grid_spec=pltpu.PrefetchScalarGridSpec(
            num_scalar_prefetch=1,
            grid=(turns,),
            in_specs=[
                pl.BlockSpec((rows, wide), lambda j, c: (0, j)),
                pl.BlockSpec((images, length, wide), lambda j, c: (0, 0, j)),
                pl.BlockSpec((images, length, wide), lambda j, c: (0, 0, turns + j)),
                pl.BlockSpec((rows, wide), lambda j, c: (0, j)),
                pl.BlockSpec((1, 2 * PARTS, rows), lambda j, c: (j, 0, 0)),
            ],
            out_specs=[
                pl.BlockSpec((rows, wide), lambda j, c: (0, j)),
                pl.BlockSpec((2, images, length, wide), lambda j, c: (0, 0, 0, j)),
            ],
            scratch_shapes=[
                pltpu.VMEM((rows, wide), f32),
                pltpu.VMEM((images, length, wide), f32),
                pltpu.VMEM((images, length, wide), f32),
            ],
        ),
        out_shape=[
            jax.ShapeDtypeStruct((rows, width), bf16),
            jax.ShapeDtypeStruct((2, images, length, width), bf16),
        ],
        compiler_params=params(1),
        name="cross_backward",
        cost_estimate=cost(28),
    )(count, query, kv, kv, grads, totals)


def here(lanes):
    return lax.axis_index("dp") * lanes + lax.axis_index("fsdp")


def bit_of(number, bit):
    return (number // (1 << bit)) % 2


def stages(devices, lanes, way):
    return list(way) + list(range(lanes.bit_length(), devices.bit_length() - 1))


def place_of(relative, devices, lanes, way):
    place = 0
    for bit in stages(devices, lanes, way)[1:]:
        place = place * 2 + bit_of(relative, bit)
    return place


def put_rows(me, devices, lanes, way, left, staged):
    flipped = left.astype(f32).T
    depth = flipped.shape[0] // devices
    for block in range(devices):
        relative = block ^ me
        quarter = 2 * (1 - bit_of(relative, lanes.bit_length() - 1)) + (1 - bit_of(relative, way[0]))
        place = quarter * (devices // 4) + place_of(relative, devices, lanes, way)
        start = pl.multiple_of(place * depth, depth)
        staged[pl.ds(start, depth), :] = flipped[block * depth : (block + 1) * depth, :]


def greet(partner):
    barrier = pltpu.get_barrier_semaphore()
    pl.semaphore_signal(barrier, inc=1, device_id=partner, device_id_type=pl.DeviceIdType.MESH)
    pl.semaphore_wait(barrier, 1)


def other_core(me, lanes):
    other = me ^ lanes
    return (other // lanes, lax.rem(other, lanes))


def to_core(partner, source, target, send_sem, recv_sem):
    return pltpu.make_async_remote_copy(
        src_ref=source,
        dst_ref=target,
        send_sem=send_sem,
        recv_sem=recv_sem,
        device_id=partner,
        device_id_type=pl.DeviceIdType.MESH,
    )


def put_halves(total, out, keep):
    half = total.shape[0] // 2
    out[...] = total[:half, :].astype(bf16).reshape(out.shape)
    keep[...] = total[half:, :].astype(bf16).reshape(keep.shape)


def weight_grad_kernel(devices, lanes, way, given, *refs):
    left, right = refs[:2]
    out, keep, staged, flipped, sent, own, came, send_sem, recv_sem = refs[2 + given :]
    step, steps = pl.program_id(0), pl.num_programs(0) - 1
    me = here(lanes)
    partner = other_core(me, lanes)
    half = flipped.shape[1] // 2

    @pl.when(step == 0)
    def _():
        greet(partner)
        for part in range(left.shape[0]):
            put_rows(me, devices, lanes, way, left[part], staged)
            flipped[part] = staged[...].astype(bf16)

    def copy(at):
        return to_core(partner, sent.at[at % 2], came.at[at], send_sem.at[at], recv_sem.at[at])

    @pl.when(step < steps)
    def _():
        def rows(low):
            total = product(flipped[0, low : low + half, :], right[0, 0])
            for part in range(1, left.shape[0]):
                total += product(flipped[part, low : low + half, :], right[0, part])
            return total

        sent[step % 2] = rows(0).astype(bf16)
        own[step % 2] = rows(half)
        copy(step).start()

    @pl.when(step > 0)
    def _():
        copy(step - 1).wait()
        put_halves(own[(step - 1) % 2] + came[step - 1].astype(f32), out, keep)


def weight_grad(number, devices, lanes, way, left, right, columns, first=0, into=(), only=None):
    parts, rows, depth = left.shape
    low, high = only or (0, right.shape[0])
    kinds, width = high - low, right.shape[3]
    wide = 512
    across = width // wide
    steps = kinds * across
    block = (devices // 4, depth // devices, wide)
    spec = pl.BlockSpec(block, lambda s: (0, 0, first // wide + jnp.maximum(s - 1, 0)))
    shape = jax.ShapeDtypeStruct((devices // 4, depth // devices, columns), bf16)

    def source(s):
        s = jnp.minimum(s, steps - 1)
        return (low + s // across, 0, 0, s % across)

    return pl.pallas_call(
        functools.partial(weight_grad_kernel, devices, lanes, way, len(into)),
        grid=(steps + 1,),
        in_specs=[
            pl.BlockSpec((parts, rows, depth), lambda s: (0, 0, 0)),
            pl.BlockSpec((1, parts, rows, wide), source),
        ]
        + [pl.BlockSpec(memory_space=pltpu.HBM)] * len(into),
        out_specs=[spec, spec],
        scratch_shapes=[
            pltpu.VMEM((depth, rows), f32),
            pltpu.VMEM((parts, depth, rows), bf16),
            pltpu.VMEM((2, depth // 2, wide), bf16),
            pltpu.VMEM((2, depth // 2, wide), f32),
            pltpu.VMEM((steps, depth // 2, wide), bf16),
            pltpu.SemaphoreType.DMA((steps,)),
            pltpu.SemaphoreType.DMA((steps,)),
        ],
        out_shape=[shape, shape],
        input_output_aliases={2 + i: i for i in range(len(into))},
        compiler_params=pltpu.CompilerParams(
            dimension_semantics=("arbitrary",),
            vmem_limit_bytes=VMEM,
            collective_id=number,
            has_side_effects=True,
        ),
        name="weight_grad",
        cost_estimate=cost(3 * kinds * parts),
    )(left, right, *into)


def norm_grad_kernel(d_ref, w_ref, unit, inverse, gain, g_ref, *refs):
    *then, total = refs
    then_w, out, low, gain_out, then_out = then if len(then) == 5 else (None, *then, None)
    step = pl.program_id(0)
    kinds, _, width = d_ref.shape
    part = product_t(d_ref[0], w_ref[:, :width])
    for kind in range(1, kinds):
        part += product_t(d_ref[kind], w_ref[:, kind * width : (kind + 1) * width])
    wide = part.shape[1]
    total[:, pl.ds(pl.multiple_of(step * wide, wide), wide)] = part

    @pl.when(step == pl.num_programs(0) - 1)
    def _():
        change, gain_grad = norm_back(unit[...], inverse[...], gain[...], total[...])
        result = g_ref[...] + change
        out[...] = result
        low[...] = result.astype(bf16)
        gain_out[...] = gain_grad[None, :]
        if then_w is not None:
            then_out[...] = product_t(low[...], then_w[...]).astype(bf16)


def norm_grad(grads, weights, first, unit, inverse, gain, g, then=False):
    kinds, rows, width = grads.shape
    wide = 256

    def whole(shape):
        return pl.BlockSpec(shape, lambda j: (0,) * len(shape))

    return pl.pallas_call(
        norm_grad_kernel,
        grid=(width // wide,),
        in_specs=[
            whole((kinds, rows, width)),
            pl.BlockSpec((wide, kinds * width), lambda j: (j, first)),
            whole((rows, width)), whole((rows, 1)), whole((1, width)), whole((rows, width)),
            *[whole((width, width))] * then,
        ],
        out_specs=[whole((rows, width)), whole((rows, width)), whole((1, width))]
        + [whole((rows, width))] * then,
        out_shape=[
            jax.ShapeDtypeStruct((rows, width), f32),
            jax.ShapeDtypeStruct((rows, width), bf16),
            jax.ShapeDtypeStruct((1, width), f32),
            *[jax.ShapeDtypeStruct((rows, width), bf16)] * then,
        ],
        scratch_shapes=[pltpu.VMEM((rows, width), f32)],
        compiler_params=params(1),
        name="norm_grad",
        cost_estimate=cost(4 * kinds),
    )(grads, weights, unit, inverse, gain, g, *[weights] * then)


def feed_kernel(
    devices, lanes, ways, x_ref, mixed_ref, w_ref, g_ref, gain_ref, up_ref, down_ref,
    out, gx, low_gx, grad_mixed, ggain, up_out, up_keep, down_out, down_keep,
    unit, inverse, hidden, staged, flipped, total, back,
    up_sent, up_own, up_came, down_sent, down_own, down_came,
    up_send_sem, up_recv_sem, down_send_sem, down_recv_sem,
):
    step, groups = pl.program_id(0), pl.num_programs(0) - 1
    me = here(lanes)
    partner = other_core(me, lanes)
    core, low, high = (me // lanes) % 2, me % lanes, me // (2 * lanes)

    @pl.when(step == 0)
    def _():
        greet(partner)
        x = x_ref[...] + product(mixed_ref[...], w_ref[...])
        h, u, i = normed(x, gain_ref[...])
        unit[...] = u
        inverse[...] = i
        hidden[...] = h.astype(bf16)
        put_rows(me, devices, lanes, ways[0], h, staged)
        flipped[...] = staged[...].astype(bf16)
        total[...] = x
        back[...] = jnp.zeros_like(back)

    def up_copy(at):
        return to_core(partner, up_sent.at[at % 2], up_came.at[at], up_send_sem.at[at], up_recv_sem.at[at])

    def down_copy(at):
        return to_core(partner, down_sent, down_came.at[at], down_send_sem.at[at], down_recv_sem.at[at])

    @pl.when(step < groups)
    def _():
        g = g_ref[...]
        up = up_ref[...].reshape(-1, up_ref.shape[-1])
        down = down_ref[...].reshape(-1, down_ref.shape[-1])
        inner = product(hidden[...], up)
        share = 0.5 + 0.5 * lax.erf(inner * (0.5**0.5))
        slope = share + inner * (jnp.exp(-0.5 * inner * inner) * 0.3989422804014327)
        active = (inner * share).astype(bf16)
        change = (product_t(g, down) * slope).astype(bf16)
        half = flipped.shape[0] // 2
        up_sent[step % 2] = product(flipped[:half, :], change).astype(bf16)
        grad_down = product_rows(active, g)

        @pl.when(step % 2 != core)
        def _():
            down_sent[...] = grad_down.astype(bf16)

        @pl.when(step % 2 == core)
        def _():
            down_own[...] = grad_down

        up_own[step % 2] = product(flipped[half:, :], change)
        total[...] += product(active, down)
        back[...] += product_t(change, up)
        up_copy(step).start()

        @pl.when(step % 2 != core)
        def _():
            down_copy(step // 2).start()

    @pl.when(step == groups)
    def _():
        out[...] = total[...].astype(bf16)
        gx_norm, gain_grad = norm_back(unit[...], inverse[...], gain_ref[...], back[...])
        result = g_ref[...].astype(f32) + gx_norm
        gx[...] = result
        low_gx[...] = result.astype(bf16)
        grad_mixed[...] = product_t(low_gx[...], w_ref[...]).astype(bf16)
        ggain[...] = gain_grad[None, :]

    @pl.when(step > 0)
    def _():
        before = step - 1
        up_copy(before).wait()
        put_halves(up_own[before % 2] + up_came[before].astype(f32), up_out, up_keep)

        @pl.when(before % 2 != core)
        def _():
            down_copy(before // 2).wait_send()

        @pl.when(before % 2 == core)
        def _():
            down_copy(before // 2).wait_recv()
            sums = down_own[...] + down_came[before // 2].astype(f32)
            depth = sums.shape[0] // lanes
            for block in range(lanes):
                relative = (block ^ low) + 2 * lanes * ((before // 2) ^ high)
                place = place_of(relative, devices, lanes, ways[1])
                piece = sums[block * depth : (block + 1) * depth, :].astype(bf16)
                goes = bit_of(relative, ways[1][0]) == 1

                @pl.when(goes)
                def _(place=place, piece=piece):
                    down_out[place] = piece

                @pl.when(jnp.logical_not(goes))
                def _(place=place, piece=piece):
                    down_keep[place] = piece


def feed(number, devices, lanes, ways, x, mixed, projection, g, gain, weights):
    rows, width = x.shape
    pieces, depth = weights.shape[2:4]
    hidden = pieces * width
    groups = devices // lanes
    tile = hidden // groups
    across = width // tile

    def group(s):
        return jnp.minimum(s, groups - 1)

    def whole(shape):
        return pl.BlockSpec(shape, lambda s: (0,) * len(shape), pipeline_mode=pl.Buffered(1))

    last = projection.shape[1] // width - 1
    up_block = pl.BlockSpec((devices // 4, depth, tile), lambda s: (0, 0, jnp.maximum(s - 1, 0)))
    up_shape = jax.ShapeDtypeStruct((devices // 4, depth, hidden), bf16)
    down_shape = jax.ShapeDtypeStruct((devices // 4, hidden // devices, width), bf16)
    return pl.pallas_call(
        functools.partial(feed_kernel, devices, lanes, ways),
        grid=(groups + 1,),
        in_specs=[
            whole((rows, width)),
            whole((rows, width)),
            pl.BlockSpec((width, width), lambda s: (0, last), pipeline_mode=pl.Buffered(1)),
            whole((rows, width)),
            whole((1, width)),
            pl.BlockSpec(
                (devices, None, None, depth, tile),
                lambda s: (0, 0, group(s) // across, 0, group(s) % across),
            ),
            pl.BlockSpec((lanes, None, pieces, depth, width), lambda s: (group(s), 1, 0, 0, 0)),
        ],
        out_specs=[
            *[whole((rows, width))] * 4, whole((1, width)),
            up_block, up_block, whole(down_shape.shape), whole(down_shape.shape),
        ],
        scratch_shapes=[
            pltpu.VMEM((rows, width), f32),
            pltpu.VMEM((rows, 1), f32),
            pltpu.VMEM((rows, width), bf16),
            pltpu.VMEM((width, rows), f32),
            pltpu.VMEM((width, rows), bf16),
            pltpu.VMEM((rows, width), f32),
            pltpu.VMEM((rows, width), f32),
            pltpu.VMEM((2, width // 2, tile), bf16),
            pltpu.VMEM((2, width // 2, tile), f32),
            pltpu.VMEM((groups, width // 2, tile), bf16),
            pltpu.VMEM((tile, width), bf16),
            pltpu.VMEM((tile, width), f32),
            pltpu.VMEM((groups // 2, tile, width), bf16),
            pltpu.SemaphoreType.DMA((groups,)),
            pltpu.SemaphoreType.DMA((groups,)),
            pltpu.SemaphoreType.DMA((groups // 2,)),
            pltpu.SemaphoreType.DMA((groups // 2,)),
        ],
        out_shape=[
            jax.ShapeDtypeStruct((rows, width), bf16),
            jax.ShapeDtypeStruct((rows, width), f32),
            jax.ShapeDtypeStruct((rows, width), bf16),
            jax.ShapeDtypeStruct((rows, width), bf16),
            jax.ShapeDtypeStruct((1, width), f32),
            up_shape, up_shape, down_shape, down_shape,
        ],
        compiler_params=pltpu.CompilerParams(
            dimension_semantics=("arbitrary",),
            vmem_limit_bytes=VMEM,
            collective_id=number,
            has_side_effects=True,
        ),
        name="feed",
        cost_estimate=cost(40),
    )(x, mixed, projection, g, gain, weights, weights)


class Spread:
    def __init__(self, devices, lanes, tracks, x_ref, out, own_sem, send_sem, recv_sem):
        self.devices, self.lanes, self.tracks = devices, lanes, tracks
        self.x_ref, self.out, self.own_sem = x_ref, out, own_sem
        self.send_sem, self.recv_sem = send_sem, recv_sem
        self.count, self.me = devices // 2, here(lanes)
        numbers = sorted(range(self.count), key=lambda k: (bin(k).count("1"), k))
        self.sends = [
            (track, number, place, bit)
            for number in numbers
            for track, (_, _, bits) in enumerate(tracks)
            for place, bit in enumerate(bits + (lanes,))
            if number >> place == 0 or bit == lanes
        ]
        self.numbers = numbers[1:]

    def device(self, bit):
        other = self.me ^ bit
        return (other // self.lanes, lax.rem(other, self.lanes))

    def block(self, track, number):
        low, high, bits = self.tracks[track]
        to_core = number >= self.count
        number -= self.count * to_core
        owner = self.me ^ sum(b for p, b in enumerate(bits) if (number >> p) & 1)
        return self.out.at[owner ^ self.lanes if to_core else owner, :, low:high]

    def copy(self, index):
        track, number, place, bit = self.sends[index]
        low, high, _ = self.tracks[track]
        target = self.block(track, number)
        return pltpu.make_async_remote_copy(
            src_ref=target if number else self.x_ref.at[:, low:high],
            dst_ref=target,
            send_sem=self.send_sem.at[index],
            recv_sem=self.recv_sem.at[track, number + (1 << place)],
            device_id=self.device(bit),
            device_id_type=pl.DeviceIdType.MESH,
        )

    def own(self):
        return pltpu.make_async_copy(self.x_ref, self.out.at[self.me], self.own_sem)

    def wait(self, track, number):
        target = self.block(track, number)
        pltpu.make_async_remote_copy(
            src_ref=target,
            dst_ref=target,
            send_sem=self.send_sem.at[0],
            recv_sem=self.recv_sem.at[track, number],
            device_id=self.device(self.lanes),
            device_id_type=pl.DeviceIdType.MESH,
        ).wait_recv()

    def send(self, number):
        for index, (_, sent, _, _) in enumerate(self.sends):
            if sent == number:
                self.copy(index).start()

    def start(self):
        barrier = pltpu.get_barrier_semaphore()
        every = [1 << b for b in range(self.devices.bit_length() - 1)]
        for bit in every:
            pl.semaphore_signal(
                barrier, inc=1, device_id=self.device(bit), device_id_type=pl.DeviceIdType.MESH
            )
        pl.semaphore_wait(barrier, len(every))
        self.own().start()
        self.send(0)

    def forward(self, numbers):
        for number in numbers:
            for track in range(len(self.tracks)):
                self.wait(track, number)
            self.send(number)

    def finish(self):
        for number in range(self.count, self.devices):
            for track in range(len(self.tracks)):
                self.wait(track, number)
        for index in range(len(self.sends)):
            self.copy(index).wait_send()
        self.own().wait()


def tracks_of(devices, lanes, columns):
    middle = (columns // 256) * 128
    high = tuple(2 * lanes << b for b in range((devices // (2 * lanes)).bit_length() - 1))
    links = [high + tuple(1 << b for b in way) for way in orders(lanes)]
    return ((0, middle, links[0]), (middle, columns, links[1]))


def spread_scratch(devices):
    return [
        pltpu.SemaphoreType.DMA,
        pltpu.SemaphoreType.DMA((2 * (devices - 1),)),
        pltpu.SemaphoreType.DMA((2, devices)),
    ]


def gather_kernel(devices, lanes, tracks, x_ref, out, own_sem, send_sem, recv_sem):
    spread = Spread(devices, lanes, tracks, x_ref, out, own_sem, send_sem, recv_sem)
    spread.start()
    spread.forward(spread.numbers)
    spread.finish()


def gather(number, devices, lanes, values):
    depth, columns = values.shape
    return pl.pallas_call(
        functools.partial(gather_kernel, devices, lanes, tracks_of(devices, lanes, columns)),
        in_specs=[pl.BlockSpec(memory_space=pltpu.VMEM)],
        out_specs=pl.BlockSpec(memory_space=pltpu.HBM),
        out_shape=jax.ShapeDtypeStruct((devices, depth, columns), values.dtype),
        scratch_shapes=spread_scratch(devices),
        compiler_params=pltpu.CompilerParams(collective_id=number, has_side_effects=True),
        name="gather",
        cost_estimate=cost(60),
    )(values).reshape(-1, columns)


def attend_kernel(
    devices, lanes, tracks, x_ref, page_column, page_row, hidden, w_q, w_k, w_v,
    gathered, q, k, v, out, totals, own_sem, send_sem, recv_sem, bias,
):
    step = pl.program_id(0)
    spread = Spread(devices, lanes, tracks, x_ref, gathered, own_sem, send_sem, recv_sem)

    @pl.when(step == 0)
    def _():
        spread.start()
        fill_bias(page_column, page_row, bias, hidden.shape[0] // TILE)

    for ref, weights in ((q, w_q), (k, w_k), (v, w_v)):
        ref[...] = product(hidden[...], weights[...]).astype(bf16)
    attend_pair(q, k, v, out, totals, bias)

    turns = hidden.shape[1] // 128
    for turn in range(1, turns):
        few = spread.numbers[
            len(spread.numbers) * (turn - 1) // (turns - 1) : len(spread.numbers) * turn // (turns - 1)
        ]

        @pl.when(step == turn)
        def _(few=few, last=turn == turns - 1):
            spread.forward(few)
            if last:
                spread.finish()


def attend(number, devices, lanes, values, page_column, page_row, hidden, weights):
    depth, columns = values.shape
    rows, width = hidden.shape
    pairs = width // 128

    def whole(*shape):
        return pl.BlockSpec(shape, lambda j: (0,) * len(shape))

    head = pl.BlockSpec((rows, 128), lambda j: (0, j))
    results = pl.pallas_call(
        functools.partial(attend_kernel, devices, lanes, tracks_of(devices, lanes, columns)),
        grid=(pairs,),
        in_specs=[
            whole(depth, columns), whole(rows, 1), whole(1, rows), whole(rows, width),
            pl.BlockSpec((width, 128), lambda j: (0, j)),
            pl.BlockSpec((width, 128), lambda j: (0, pairs + j)),
            pl.BlockSpec((width, 128), lambda j: (0, 2 * pairs + j)),
        ],
        out_specs=[
            pl.BlockSpec(memory_space=pltpu.HBM), head, head, head, head,
            pl.BlockSpec((1, 2, rows), lambda j: (j, 0, 0)),
        ],
        out_shape=[
            jax.ShapeDtypeStruct((devices, depth, columns), values.dtype),
            *[jax.ShapeDtypeStruct((rows, width), bf16)] * 4,
            jax.ShapeDtypeStruct((pairs, 2, rows), f32),
        ],
        scratch_shapes=spread_scratch(devices)
        + [pltpu.VMEM((rows // TILE, PAGE_MAX + TILE, TILE), f32)],
        compiler_params=pltpu.CompilerParams(
            dimension_semantics=("arbitrary",),
            vmem_limit_bytes=VMEM,
            collective_id=number,
            has_side_effects=True,
        ),
        name="attend",
        cost_estimate=cost(60),
    )(values, page_column, page_row, hidden, weights, weights, weights)
    gathered, q, k, v, *rest = results
    return gathered.reshape(-1, columns), (q, k, v), *rest


def image_kernel(images, weights, out):
    for image in range(images.shape[0]):
        out[image] = product(images[image], weights[...]).astype(bf16)


def image_keys(images, weights, first):
    count, length, width = images.shape
    wide = 512
    return pl.pallas_call(
        image_kernel,
        grid=(2 * width // wide,),
        in_specs=[
            pl.BlockSpec(images.shape, lambda j: (0, 0, 0)),
            pl.BlockSpec((width, wide), lambda j: (0, first * width // wide + j)),
        ],
        out_specs=pl.BlockSpec((count, length, wide), lambda j: (0, 0, j)),
        out_shape=jax.ShapeDtypeStruct((count, length, 2 * width), bf16),
        compiler_params=params(1),
        name="image_keys",
        cost_estimate=cost(8),
    )(images, weights)


def swap(values, devices, bit):
    return lax.ppermute(values, AXES, [(i, i ^ bit) for i in range(devices)])


def plus(a, b):
    return (a.astype(f32) + b.astype(f32)).astype(bf16)


def owner_sums(halves, devices, lanes, way, late=None):
    bits = stages(devices, lanes, way)
    out, keep = halves
    for stage, bit in enumerate(bits):
        arrived = swap(out, devices, 1 << bit)
        if stage == len(bits) - 1:
            return keep[0].astype(f32) + arrived[0].astype(f32)
        half = keep.shape[0] // 2
        out, keep = plus(keep[half:], arrived[half:]), plus(keep[:half], arrived[:half])
        if stage == 0 and late is not None:
            late_out, late_keep = late
            late_arrived = swap(late_out, devices, 1 << bit)
            out = jnp.concatenate([out, plus(late_keep[half:], late_arrived[half:])], axis=-1)
            keep = jnp.concatenate([keep, plus(late_keep[:half], late_arrived[:half])], axis=-1)


def gain_halves(values, devices, lanes, way, me):
    kinds, depth = values.shape
    blocks = jnp.pad(values.T, ((0, 0), (0, 128 - kinds))).astype(bf16)
    every = range(devices)
    core = lanes.bit_length() - 1
    order = sorted(every, key=lambda r: (1 - bit_of(r, core), 1 - bit_of(r, way[0]), place_of(r, devices, lanes, way)))
    blocks = blocks.reshape(devices, depth // devices, 128)[jnp.array(order) ^ me]
    arrived = swap(blocks[: devices // 2], devices, lanes)
    sums = plus(blocks[devices // 2 :], arrived)
    return sums[: devices // 4], sums[devices // 4 :]


def after(values, first):
    return lax.optimization_barrier((values, first))[0]


def orders(lanes):
    low = list(range(lanes.bit_length() - 1))
    return low, low[::-1]


def shards(devices, lanes, tokens, images, segment_ids, image_map, out_grad, norm_self, attn_query,
           attn_key, attn_value, attn_out, norm_cross, cross_query, cross_key, cross_value, cross_out,
           norm_ffn, ffn_up, ffn_down):
    me = lax.axis_index("dp") * lanes + lax.axis_index("fsdp")
    me_ref = me.astype(jnp.int32)[None]
    depth, width = attn_query.shape
    gains = jnp.stack([norm_self, norm_cross, norm_ffn], axis=1)
    gains = jnp.pad(gains, ((0, 0), (0, 128 - 3)))
    first_set = jnp.concatenate([attn_query, attn_key, attn_value, gains], axis=1)
    second_set = jnp.concatenate([attn_out, cross_query, cross_key, cross_value, cross_out], axis=1)
    pieces = ffn_up.shape[1] // width
    feed_set = jnp.stack(
        [ffn_up.reshape(depth, pieces, width).transpose(1, 0, 2), ffn_down.reshape(pieces, depth, width)]
    )
    first_set = gather(0, devices, lanes, first_set)
    feed_set = lax.all_gather(after(feed_set, first_set), AXES, axis=0)
    (count, order, page_column, page_row, inputs, grad_out, hidden_one, unit_one, inverse_one, *gains) = arrange(
        image_map[0], segment_ids[0], tokens[0], out_grad[0], first_set, 3 * width // 128
    )
    second_set, qkv, mixed_one, log_one = attend(
        1, devices, lanes, second_set, page_column, page_row, hidden_one, first_set
    )
    w_kv = second_set[:, 2 * width : 4 * width]
    kv = image_keys(images, second_set, 2)
    after_self, hidden_two, unit_two, inverse_two, query_two = between(inputs, mixed_one, second_set, gains[1])
    mixed_two, log_two = cross_forward(count, query_two, kv)

    one_way, other_way = orders(lanes)
    (output, grad_after_cross, branch_two, grad_mixed_two, grad_gain_ffn, *halves) = feed(
        2, devices, lanes, (one_way, other_way), after_self, mixed_two, second_set, grad_out, gains[2], feed_set
    )

    def sums(way, halves, late=None):
        return owner_sums(halves, devices, lanes, way, late)

    def halves_of(number, way, left, right, **options):
        return weight_grad(number, devices, lanes, way, left, right, 2 * width, **options)

    grad_up = sums(one_way, halves[:2])
    grad_down = sums(other_way, halves[2:])

    grad_query_two, grad_kv = cross_backward(count, query_two, kv, grad_mixed_two, log_two)
    halves = halves_of(3, one_way, mixed_two[None], after(branch_two, grad_kv)[None, None])
    halves = halves_of(4, one_way, hidden_two[None], grad_query_two[None, None], first=width, into=halves)
    grad_c = sums(one_way, halves)
    halves = halves_of(5, other_way, images, after(grad_kv, halves[0]))
    grad_d = sums(other_way, halves)
    grad_query_again = after(grad_query_two, halves[0])[None]
    grad_after_self, branch_one, grad_gain_cross, grad_mixed_one = norm_grad(
        grad_query_again, second_set, 1, unit_two, inverse_two, gains[1], grad_after_cross, then=True
    )
    grad_qkv = self_backward(page_column, page_row, qkv, grad_mixed_one, log_one)
    halves_kv = halves_of(8, other_way, hidden_one[None], grad_qkv[:, None], only=(1, 3))
    branch_again = after(branch_one, halves_kv[0])[None, None]
    halves = halves_of(6, one_way, mixed_one[None], branch_again)
    options = dict(first=width, into=halves, only=(0, 1))
    halves = halves_of(7, one_way, hidden_one[None], grad_qkv[:, None], **options)
    grad_qkv_again = after(grad_qkv, halves[0])
    _, grad_inputs, grad_gain_self = norm_grad(
        grad_qkv_again, first_set, 0, unit_one, inverse_one, gains[0], grad_after_self
    )
    gain_grads = jnp.concatenate([grad_gain_self, grad_gain_cross, grad_gain_ffn])
    late = gain_halves(gain_grads, devices, lanes, other_way, me)
    grad_a = sums(one_way, halves)
    grad_b = sums(other_way, halves_kv, late)
    gain_sums = grad_b[:, 2 * width :]

    grad_kv = after(grad_kv, late[0])
    back = (((2,), (1,)), ((), ()))
    grad_images = lax.dot_general(grad_kv[0], w_kv[:, :width], back, preferred_element_type=f32)
    grad_images += lax.dot_general(grad_kv[1], w_kv[:, width:], back, preferred_element_type=f32)
    grad_images = grad_images.astype(bf16)
    output = product_rows(order, output).astype(bf16)
    grad_inputs = product_rows(order, grad_inputs).astype(bf16)
    return (
        output[None],
        grad_inputs[None],
        grad_images,
        gain_sums[:, 0],
        grad_a[:, width:],
        grad_b[:, :width],
        grad_b[:, width : 2 * width],
        grad_a[:, :width],
        gain_sums[:, 1],
        grad_c[:, width:],
        grad_d[:, :width],
        grad_d[:, width:],
        grad_c[:, :width],
        gain_sums[:, 2],
        grad_up,
        grad_down,
    )


def solution(mesh):
    rows = P(AXES)
    devices, lanes = mesh.shape["dp"] * mesh.shape["fsdp"], mesh.shape["fsdp"]
    return jax.shard_map(
        functools.partial(shards, devices, lanes),
        mesh=mesh,
        in_specs=(rows,) * 18,
        out_specs=(rows,) * 16,
        check_vma=False,
    )
```
